256 devices in a mesh: view: 4 (over x_hi, core), pencil: 64 (over x_lo, y, z).
Axes of the slice: x: 4 (x_hi: 2, x_lo: 2; x = x_hi * 2 + x_lo), y: 4, z: 8, core: 2. Of those that a mesh axis runs over, the one named last changes fastest.
Arguments:
- recorded: float32 [4, 256, 256, 256], P('view', 'pencil'), may hold values from 0.5 to 4
- spectral_weight: float32 [4, 256, 256, 256], P('view', None, 'pencil'), may hold values from 0.05 to 1
- psf_taps: float32 [4, 3, 9], replicated, may hold values from 0.1 to 1
Outputs:
- joined_volume: float32 [256, 256, 256], P('pencil', 'view')
- estimate: float32 [256, 256, 256], P('pencil', 'view')
The draws below stay inside these ranges and needn't reach their ends.
All inputs are finite; a program needn't handle non-finite values.
Results may differ from the reference program's by a relative error of at most 0.00029.
Values sent between devices are 32-bit elements; how exact they have to be, the bound alone decides.
A program may use at most 64 MiB of HBM per device.

```python
import math
import jax
import jax.numpy as jnp
from jax import lax

NZ = 256
NY = 256
NX = 256
TAPS = 9
ITERS = 2
VIEWS = 4


def level_of(own_key, shape, pieces, low, top_value):
    level = 1.0
    for axis_at, blocks in pieces:
        draws = jax.random.uniform(jax.random.fold_in(jax.random.fold_in(own_key, 6), axis_at), (blocks,), jnp.float32, low / len(pieces), top_value / len(pieces))
        level = level * jnp.repeat(jnp.exp(draws), shape[axis_at] // blocks).reshape((-1,) + (1,) * (len(shape) - 1 - axis_at))
    return level


def setup_inputs(seed: int = 0) -> dict:
    arg_keys = jax.random.split(jax.random.key(seed), 4)
    return {
        "recorded": jnp.clip(jnp.exp(math.log(4.0) - 2.0794415 * jax.random.uniform(arg_keys[0], (VIEWS, NZ, NY, NX), jnp.float32) ** level_of(arg_keys[0], (VIEWS, NZ, NY, NX), ((0, 4), (1, 64)), -0.2, 0.2)), 0.5, 4.0),
        "spectral_weight": jnp.clip(jnp.exp(math.log(1.0) - 2.9957323 * jax.random.uniform(arg_keys[1], (VIEWS, NZ, NY, NX), jnp.float32) ** level_of(arg_keys[1], (VIEWS, NZ, NY, NX), ((0, 4), (2, 64)), -0.2, 0.2)), 0.05, 1.0),
        "psf_taps": jnp.clip(jnp.exp(jax.random.uniform(arg_keys[2], (VIEWS, 3, TAPS), jnp.float32, math.log(0.1), math.log(1.0))), 0.1, 1.0),
    }


def conv_along(field, column, axis_dim, margin):
    padding = [(0, 0)] * field.ndim
    padding[axis_dim] = (margin, margin)
    padded = jnp.pad(field, padding)
    length = field.shape[axis_dim]
    running = column[0] * lax.slice_in_dim(padded, 0, length, axis=axis_dim)
    for offset in range(1, column.shape[0]):
        running = running + column[offset] * lax.slice_in_dim(padded, offset, offset + length, axis=axis_dim)
    return running


def blur_field(field, kernel, margin):
    for axis_dim in range(3):
        field = conv_along(field, kernel[axis_dim], axis_dim, margin)
    return field


def reference(recorded, spectral_weight, psf_taps):
    combined = spectral_weight[0] * jnp.fft.fftn(recorded[0])
    for viewer in range(1, VIEWS):
        combined = combined + spectral_weight[viewer] * jnp.fft.fftn(recorded[viewer])
    joined_volume = jnp.real(jnp.fft.ifftn(combined)).astype(jnp.float32)
    kernels = psf_taps / jnp.sum(psf_taps, axis=-1, keepdims=True)
    margin = TAPS // 2
    estimate = 0.1 + jax.nn.softplus(joined_volume)
    for repeat in range(ITERS):
        summed = jnp.zeros_like(estimate)
        for viewer in range(VIEWS):
            blurred = blur_field(estimate, kernels[viewer], margin)
            ratio = recorded[viewer] / blurred
            summed = summed + blur_field(ratio, kernels[viewer][:, ::-1], margin)
        estimate = estimate * summed / VIEWS
    return joined_volume, estimate
```

```python
import functools
import math

import jax
import jax.numpy as jnp
from jax import lax
from jax.experimental import pallas as pl
from jax.experimental.pallas import tpu as pltpu
from jax.sharding import PartitionSpec as P

NZ = 256
NY = 256
NX = 256
ITERS = 2
MESH_ID = pl.DeviceIdType.MESH
F32 = jnp.float32
BF16 = jnp.bfloat16
SIDES = [(dv, dp) for dp in (-1, 1, 0) for dv in (0, -1, 1) if (dv, dp) != (0, 0)]
SLOT = {side: k for k, side in enumerate(SIDES)}


def halves(value):
    high = value.astype(BF16)
    return high, (value - high.astype(F32)).astype(BF16)


def dot(left, right):
    return jnp.dot(left, right, preferred_element_type=F32)


def dot3(left, right_high, right_low):
    high, low = halves(left)
    return dot(high, right_high) + (dot(high, right_low) + dot(low, right_high))


def rl_kernel(views, pencils, taps, joined, stacked, out, est, zed, mid, spread, acc, rz, rs,
              th, tl, ah, al, send_sem, recv_sem):
    depth, rows, width = joined.shape
    frame = rows + 16
    v0, p0 = lax.axis_index("view"), lax.axis_index("pencil")

    def exists(side):
        v, p = v0 + side[0], p0 + side[1]
        return (v >= 0) & (v < views) & (p >= 0) & (p < pencils)

    def back(side):
        return (-side[0], -side[1])

    est[...] = jnp.zeros_like(est)
    mid[...] = jnp.zeros_like(mid)
    rz[...] = jnp.zeros_like(rz)
    rs[...] = jnp.zeros_like(rs)

    barrier = pltpu.get_barrier_semaphore()
    for side in SIDES:
        @pl.when(exists(side))
        def _(side=side):
            pl.semaphore_signal(barrier, inc=1, device_id=(v0 + side[0], p0 + side[1]), device_id_type=MESH_ID)

    planes_of = {-1: pl.ds(0, depth), 0: pl.ds(depth, depth), 1: pl.ds(2 * depth, depth)}

    def est_copy(side):
        dv, dp = side
        src_rows = {0: pl.ds(8, rows), 1: pl.ds(rows, 8), -1: pl.ds(8, 8)}[dv]
        dst_rows = {0: pl.ds(8, rows), 1: pl.ds(0, 8), -1: pl.ds(rows + 8, 8)}[dv]
        return pltpu.make_async_remote_copy(
            src_ref=est.at[planes_of[0], :, src_rows, :],
            dst_ref=est.at[planes_of[-dp], :, dst_rows, :],
            send_sem=send_sem.at[0, SLOT[side]],
            recv_sem=recv_sem.at[0, SLOT[back(side)]],
            device_id=(v0 + dv, p0 + dp),
            device_id_type=MESH_ID,
        )

    def acc_copy(side):
        dv, dp = side
        src_rows = {0: pl.ds(8, rows), 1: pl.ds(rows + 8, 8), -1: pl.ds(0, 8)}[dv]
        slot = SLOT[back(side)]
        landing = rz.at[0 if dp == 1 else 1] if dv == 0 else rs.at[slot]
        return pltpu.make_async_remote_copy(
            src_ref=acc.at[planes_of[dp], :, src_rows, :],
            dst_ref=landing,
            send_sem=send_sem.at[1, SLOT[side]],
            recv_sem=recv_sem.at[1, slot],
            device_id=(v0 + dv, p0 + dp),
            device_id_type=MESH_ID,
        )

    def each(sides, action):
        for side in sides:
            @pl.when(exists(side))
            def _(side=side):
                action(side)

    for h in range(2):
        s = joined[:, :, h * 128:(h + 1) * 128]
        est[pl.ds(depth, depth), h, pl.ds(8, rows), :] = 0.1 + (
            jnp.maximum(s, 0.0) + jnp.log1p(jnp.exp(-jnp.abs(s))))

    expected = sum(exists(side).astype(jnp.int32) for side in SIDES)
    pl.semaphore_wait(barrier, expected)
    each(SIDES, lambda side: est_copy(side).start())

    def band(v, carry):
        at = (lax.broadcasted_iota(jnp.int32, (width, width), 0)
              - lax.broadcasted_iota(jnp.int32, (width, width), 1))
        table, turned = jnp.zeros((width, width), F32), jnp.zeros((width, width), F32)
        for t in range(9):
            tap = taps[v, 2, t]
            table = jnp.where(at == t - 4, tap, table)
            turned = jnp.where(at == 4 - t, tap, turned)
        th[v], tl[v] = halves(table)
        ah[v], al[v] = halves(turned)
        return carry

    lax.fori_loop(0, views, band, 0)

    def view_step(v, carry):
        for z in range(depth):
            total = taps[v, 0, 0] * est[z]
            for t in range(1, 9):
                total = total + taps[v, 0, t] * est[z + t]
            zed[z] = total
        sides = []
        for h in range(2):
            planes = []
            for z in range(depth):
                total = taps[v, 1, 0] * zed[z, h, pl.ds(4, rows), :]
                for t in range(1, 9):
                    total = total + taps[v, 1, t] * zed[z, h, pl.ds(4 + t, rows), :]
                planes.append(total)
            sides.append(jnp.concatenate(planes, axis=0))
        blurred = dot3(jnp.concatenate(sides, axis=1), th[v], tl[v])
        ratio = stacked[v].reshape(depth * rows, width) / blurred
        turned = dot3(ratio, ah[v], al[v])
        for z in range(depth):
            for h in range(2):
                mid[z, h, pl.ds(16, rows), :] = turned[z * rows:(z + 1) * rows, h * 128:(h + 1) * 128]
        for z in range(depth):
            for h in range(2):
                total = taps[v, 1, 8] * mid[z, h, pl.ds(4, frame), :]
                for t in range(1, 9):
                    total = total + taps[v, 1, 8 - t] * mid[z, h, pl.ds(4 + t, frame), :]
                spread[v, z, h] = total
        return carry

    def gather_planes(planes):
        for zo in planes:
            total = None
            for v in range(views):
                for zs in range(depth):
                    if 0 <= zo - zs <= 8:
                        term = taps[v, 0, zo - zs] * spread[v, zs]
                        total = term if total is None else total + term
            acc[zo] = total

    def iteration(step, carry):
        each(SIDES, est_wait)
        lax.fori_loop(0, views, view_step, 0)
        gather_planes(list(range(0, depth)) + list(range(2 * depth, 3 * depth)))
        each([s for s in SIDES if s[1] != 0], lambda side: acc_copy(side).start())
        gather_planes(range(depth, 2 * depth))
        each([s for s in SIDES if s[1] == 0], lambda side: acc_copy(side).start())
        each(SIDES, lambda side: est_copy(side).wait_send())
        each(SIDES, acc_wait)
        for z in range(depth):
            for h in range(2):
                total = acc[depth + z, h, pl.ds(8, rows), :] + (rz[0, z, h] + rz[1, z, h])
                low = rs[SLOT[(-1, 0)], z, h] + (rs[SLOT[(-1, -1)], z, h] + rs[SLOT[(-1, 1)], z, h])
                high = rs[SLOT[(1, 0)], z, h] + (rs[SLOT[(1, -1)], z, h] + rs[SLOT[(1, 1)], z, h])
                total = jnp.concatenate(
                    [total[:8] + low, total[8:rows - 8], total[rows - 8:] + high], axis=0)
                fresh = est[depth + z, h, pl.ds(8, rows), :] * (total * (1.0 / views))
                est[depth + z, h, pl.ds(8, rows), :] = fresh
        each(SIDES, lambda side: acc_copy(side).wait_send())

        @pl.when(step < ITERS - 1)
        def _():
            each(SIDES, lambda side: est_copy(side).start())
        return carry

    def est_wait(side):
        dv, dp = side
        dst_rows = {0: pl.ds(8, rows), -1: pl.ds(0, 8), 1: pl.ds(rows + 8, 8)}[dv]
        landing = est.at[planes_of[dp], :, dst_rows, :]
        pltpu.make_async_remote_copy(
            src_ref=landing, dst_ref=landing, send_sem=send_sem.at[0, SLOT[side]],
            recv_sem=recv_sem.at[0, SLOT[side]], device_id=(v0 + dv, p0 + dp),
            device_id_type=MESH_ID).wait_recv()

    def acc_wait(side):
        dv, dp = side
        landing = rz.at[0 if dp == -1 else 1] if dv == 0 else rs.at[SLOT[side]]
        pltpu.make_async_remote_copy(
            src_ref=landing, dst_ref=landing, send_sem=send_sem.at[1, SLOT[side]],
            recv_sem=recv_sem.at[1, SLOT[side]], device_id=(v0 + dv, p0 + dp),
            device_id_type=MESH_ID).wait_recv()

    lax.fori_loop(0, ITERS, iteration, 0)
    for h in range(2):
        out[:, :, h * 128:(h + 1) * 128] = est[pl.ds(depth, depth), h, pl.ds(8, rows), :]


def richardson_lucy(joined, stacked, kernels):
    views, pencils = stacked.shape[0], lax.axis_size("pencil")
    depth, rows, width = joined.shape
    frame = rows + 16
    vmem = pl.BlockSpec(memory_space=pltpu.VMEM)
    return pl.pallas_call(
        functools.partial(rl_kernel, views, pencils),
        name="deconvolve",
        out_shape=jax.ShapeDtypeStruct(joined.shape, F32),
        in_specs=[pl.BlockSpec(memory_space=pltpu.SMEM), vmem, vmem],
        out_specs=vmem,
        scratch_shapes=[
            pltpu.VMEM((3 * depth, 2, frame, 128), F32),
            pltpu.VMEM((depth, 2, frame, 128), F32),
            pltpu.VMEM((depth, 2, frame + 16, 128), F32),
            pltpu.VMEM((views, depth, 2, frame, 128), F32),
            pltpu.VMEM((3 * depth, 2, frame, 128), F32),
            pltpu.VMEM((2, depth, 2, rows, 128), F32),
            pltpu.VMEM((8, depth, 2, 8, 128), F32),
            pltpu.VMEM((views, width, width), BF16),
            pltpu.VMEM((views, width, width), BF16),
            pltpu.VMEM((views, width, width), BF16),
            pltpu.VMEM((views, width, width), BF16),
            pltpu.SemaphoreType.DMA((2, 8)),
            pltpu.SemaphoreType.DMA((2, 8)),
        ],
        compiler_params=pltpu.CompilerParams(collective_id=1, has_side_effects=True,
                                             vmem_limit_bytes=24 * 1024 * 1024),
    )(kernels, joined, stacked)


def in_blocks(shard, dim, devices):
    shape = shard.shape
    parts = shard.reshape(*shape[:dim], devices, shape[dim] // devices, *shape[dim + 1 :])
    return jnp.moveaxis(parts, dim, 0)


def summed_on_arrival(shard, axis, dim):
    devices = lax.axis_size(axis)
    parts = lax.all_to_all(in_blocks(shard, dim, devices), axis, 0, 0, tiled=True)
    return jnp.sum(parts, axis=0)


def sent_together(arrays, axis, dim, along):
    both = jnp.concatenate(arrays, axis=along)
    whole, at, gathered = (summed_on_arrival(both, axis, dim), 0, [])
    for a in arrays:
        gathered.append(lax.slice_in_dim(whole, at, at + a.shape[along], axis=along))
        at += a.shape[along]
    return tuple(gathered)


def in_one_piece(arrays, axis, split_dim, concat_dim, along):
    widths = [a.shape[along] for a in arrays]
    both = jnp.concatenate(arrays, axis=along)
    whole = lax.all_to_all(both, axis, split_axis=split_dim, concat_axis=concat_dim, tiled=True)
    return tuple(jnp.split(whole, [sum(widths[:k]) for k in range(1, len(widths))], axis=along))


def tables(length):
    positions = jnp.arange(length, dtype=jnp.int32)
    product = positions[:, None] * positions[None, :] % length
    phases = product.astype(jnp.float32) * (2.0 * math.pi / length)
    return (jnp.cos(phases), jnp.sin(phases))


def mix(form, left, right):
    return jnp.einsum(form, left, right, precision=lax.Precision.HIGH)


def depth_forward(pieces):
    real_part, imag_part = pieces
    cosine, sine_part = tables(real_part.shape[0])
    out_real = mix("zyx,zk->kyx", real_part, cosine) + mix("zyx,zk->kyx", imag_part, sine_part)
    out_imag = mix("zyx,zk->kyx", imag_part, cosine) - mix("zyx,zk->kyx", real_part, sine_part)
    return (out_real, out_imag)


def depth_inverse(real_part, imag_part):
    cosine, sine_part = tables(real_part.shape[0])
    out_real = mix("kyx,kz->zyx", real_part, cosine) - mix("kyx,kz->zyx", imag_part, sine_part)
    out_imag = mix("kyx,kz->zyx", real_part, sine_part) + mix("kyx,kz->zyx", imag_part, cosine)
    return (out_real, out_imag)


def rows_inverse(pieces):
    real_part, imag_part = pieces
    cosine, sine_part = tables(real_part.shape[1])
    out_real = mix("zkx,ky->zyx", real_part, cosine) - mix("zkx,ky->zyx", imag_part, sine_part)
    out_imag = mix("zkx,ky->zyx", real_part, sine_part) + mix("zkx,ky->zyx", imag_part, cosine)
    return (out_real, out_imag)


def columns_inverse(real_part, imag_part):
    cosine, sine_part = tables(real_part.shape[2])
    total = mix("zyk,kx->zyx", real_part, cosine) - mix("zyk,kx->zyx", imag_part, sine_part)
    return total / float(NZ * NY * NX)


def body(recorded, spectral_weight, psf_taps):
    view_count = lax.axis_size("view")
    slab = recorded[0]
    cos_x, sin_x = tables(slab.shape[2])
    cos_y, sin_y = tables(slab.shape[1])
    first_real = mix("zyx,xk->zyk", slab, cos_x)
    first_imag = -mix("zyx,xk->zyk", slab, sin_x)
    second_real = mix("zyx,yk->zkx", first_real, cos_y) + mix("zyx,yk->zkx", first_imag, sin_y)
    second_imag = mix("zyx,yk->zkx", first_imag, cos_y) - mix("zyx,yk->zkx", first_real, sin_y)
    spec_real, spec_imag = depth_forward(
        (
            lax.all_to_all(second_real, "pencil", split_axis=1, concat_axis=0, tiled=True),
            lax.all_to_all(second_imag, "pencil", split_axis=1, concat_axis=0, tiled=True),
        )
    )
    weights = spectral_weight[0]
    weighted_real = spec_real * weights
    weighted_imag = spec_imag * weights
    quarter = slab.shape[1] // view_count
    share_real, share_imag = sent_together((weighted_real, weighted_imag), "view", 2, 0)
    part_real, part_imag = depth_inverse(share_real, share_imag)
    rows_real, rows_imag = rows_inverse(
        (
            lax.all_to_all(part_real, "pencil", split_axis=0, concat_axis=1, tiled=True),
            lax.all_to_all(part_imag, "pencil", split_axis=0, concat_axis=1, tiled=True),
        )
    )
    wide_real, wide_imag = in_one_piece((rows_real, rows_imag), "view", 1, 2, 0)
    joined_volume = columns_inverse(wide_real, wide_imag)
    kernels = psf_taps / jnp.sum(psf_taps, axis=-1, keepdims=True)
    stacked = lax.all_to_all(recorded, "view", split_axis=2, concat_axis=0, tiled=True)
    return (joined_volume, richardson_lucy(joined_volume, stacked, kernels))


def solution(mesh):
    return jax.shard_map(
        body,
        mesh=mesh,
        in_specs=(P("view", "pencil", None, None), P("view", None, "pencil", None), P()),
        out_specs=(P("pencil", "view", None), P("pencil", "view", None)),
        check_vma=False,
    )
```

```python
import functools

import jax
import jax.numpy as jnp
import numpy as np
from jax import lax
from jax.experimental import pallas as pl
from jax.experimental.pallas import tpu as pltpu
from jax.sharding import PartitionSpec as P

ITERS = 2
MESH_ID = pl.DeviceIdType.MESH
F32 = jnp.float32
BF16 = jnp.bfloat16
SIDES = [(dv, dp) for dp in (-1, 1, 0) for dv in (0, -1, 1) if (dv, dp) != (0, 0)]
SLOT = {side: k for k, side in enumerate(SIDES)}


def halves(value):
    high = value.astype(BF16)
    return high, (value - high.astype(F32)).astype(BF16)


def dot(left, right):
    return jnp.dot(left, right, preferred_element_type=F32)


def dot3(left, right_high, right_low):
    high, low = halves(left)
    return dot(high, right_high) + (dot(high, right_low) + dot(low, right_high))


def rl_kernel(views, pencils, taps, joined, stacked, out, est, zed, mid, spread, acc, rz, rs,
              th, tl, ah, al, send_sem, recv_sem):
    depth, rows, width = joined.shape
    frame = rows + 16
    v0, p0 = lax.axis_index("view"), lax.axis_index("pencil")

    def exists(side):
        v, p = v0 + side[0], p0 + side[1]
        return (v >= 0) & (v < views) & (p >= 0) & (p < pencils)

    def back(side):
        return (-side[0], -side[1])

    est[...] = jnp.zeros_like(est)
    mid[...] = jnp.zeros_like(mid)
    rz[...] = jnp.zeros_like(rz)
    rs[...] = jnp.zeros_like(rs)

    barrier = pltpu.get_barrier_semaphore()
    for side in SIDES:
        @pl.when(exists(side))
        def _(side=side):
            pl.semaphore_signal(barrier, inc=1, device_id=(v0 + side[0], p0 + side[1]), device_id_type=MESH_ID)

    planes_of = {-1: pl.ds(0, depth), 0: pl.ds(depth, depth), 1: pl.ds(2 * depth, depth)}

    def est_copy(side):
        dv, dp = side
        src_rows = {0: pl.ds(8, rows), 1: pl.ds(rows, 8), -1: pl.ds(8, 8)}[dv]
        dst_rows = {0: pl.ds(8, rows), 1: pl.ds(0, 8), -1: pl.ds(rows + 8, 8)}[dv]
        return pltpu.make_async_remote_copy(
            src_ref=est.at[planes_of[0], :, src_rows, :],
            dst_ref=est.at[planes_of[-dp], :, dst_rows, :],
            send_sem=send_sem.at[0, SLOT[side]],
            recv_sem=recv_sem.at[0, SLOT[back(side)]],
            device_id=(v0 + dv, p0 + dp),
            device_id_type=MESH_ID,
        )

    def acc_copy(side):
        dv, dp = side
        src_rows = {0: pl.ds(8, rows), 1: pl.ds(rows + 8, 8), -1: pl.ds(0, 8)}[dv]
        slot = SLOT[back(side)]
        landing = rz.at[0 if dp == 1 else 1] if dv == 0 else rs.at[slot]
        return pltpu.make_async_remote_copy(
            src_ref=acc.at[planes_of[dp], :, src_rows, :],
            dst_ref=landing,
            send_sem=send_sem.at[1, SLOT[side]],
            recv_sem=recv_sem.at[1, slot],
            device_id=(v0 + dv, p0 + dp),
            device_id_type=MESH_ID,
        )

    def each(sides, action):
        for side in sides:
            @pl.when(exists(side))
            def _(side=side):
                action(side)

    for h in range(2):
        s = joined[:, :, h * 128:(h + 1) * 128]
        est[pl.ds(depth, depth), h, pl.ds(8, rows), :] = 0.1 + (
            jnp.maximum(s, 0.0) + jnp.log1p(jnp.exp(-jnp.abs(s))))

    expected = sum(exists(side).astype(jnp.int32) for side in SIDES)
    pl.semaphore_wait(barrier, expected)
    each(SIDES, lambda side: est_copy(side).start())

    def band(v, carry):
        at = (lax.broadcasted_iota(jnp.int32, (width, width), 0)
              - lax.broadcasted_iota(jnp.int32, (width, width), 1))
        table, turned = jnp.zeros((width, width), F32), jnp.zeros((width, width), F32)
        for t in range(9):
            tap = taps[v, 2, t]
            table = jnp.where(at == t - 4, tap, table)
            turned = jnp.where(at == 4 - t, tap, turned)
        th[v], tl[v] = halves(table)
        ah[v], al[v] = halves(turned)
        return carry

    lax.fori_loop(0, views, band, 0)

    def view_step(v, carry):
        for z in range(depth):
            total = taps[v, 0, 0] * est[z]
            for t in range(1, 9):
                total = total + taps[v, 0, t] * est[z + t]
            zed[z] = total
        sides = []
        for h in range(2):
            planes = []
            for z in range(depth):
                total = taps[v, 1, 0] * zed[z, h, pl.ds(4, rows), :]
                for t in range(1, 9):
                    total = total + taps[v, 1, t] * zed[z, h, pl.ds(4 + t, rows), :]
                planes.append(total)
            sides.append(jnp.concatenate(planes, axis=0))
        blurred = dot3(jnp.concatenate(sides, axis=1), th[v], tl[v])
        ratio = stacked[v].reshape(depth * rows, width) / blurred
        turned = dot3(ratio, ah[v], al[v])
        for z in range(depth):
            for h in range(2):
                mid[z, h, pl.ds(16, rows), :] = turned[z * rows:(z + 1) * rows, h * 128:(h + 1) * 128]
        for z in range(depth):
            for h in range(2):
                total = taps[v, 1, 8] * mid[z, h, pl.ds(4, frame), :]
                for t in range(1, 9):
                    total = total + taps[v, 1, 8 - t] * mid[z, h, pl.ds(4 + t, frame), :]
                spread[v, z, h] = total
        return carry

    def gather_planes(planes):
        for zo in planes:
            total = None
            for v in range(views):
                for zs in range(depth):
                    if 0 <= zo - zs <= 8:
                        term = taps[v, 0, zo - zs] * spread[v, zs]
                        total = term if total is None else total + term
            acc[zo] = total

    def iteration(step, carry):
        each(SIDES, est_wait)
        lax.fori_loop(0, views, view_step, 0)
        gather_planes(list(range(0, depth)) + list(range(2 * depth, 3 * depth)))
        each([s for s in SIDES if s[1] != 0], lambda side: acc_copy(side).start())
        gather_planes(range(depth, 2 * depth))
        each([s for s in SIDES if s[1] == 0], lambda side: acc_copy(side).start())
        each(SIDES, lambda side: est_copy(side).wait_send())
        each(SIDES, acc_wait)
        for z in range(depth):
            for h in range(2):
                total = acc[depth + z, h, pl.ds(8, rows), :] + (rz[0, z, h] + rz[1, z, h])
                low = rs[SLOT[(-1, 0)], z, h] + (rs[SLOT[(-1, -1)], z, h] + rs[SLOT[(-1, 1)], z, h])
                high = rs[SLOT[(1, 0)], z, h] + (rs[SLOT[(1, -1)], z, h] + rs[SLOT[(1, 1)], z, h])
                total = jnp.concatenate(
                    [total[:8] + low, total[8:rows - 8], total[rows - 8:] + high], axis=0)
                fresh = est[depth + z, h, pl.ds(8, rows), :] * (total * (1.0 / views))
                est[depth + z, h, pl.ds(8, rows), :] = fresh
        each(SIDES, lambda side: acc_copy(side).wait_send())

        @pl.when(step < ITERS - 1)
        def _():
            each(SIDES, lambda side: est_copy(side).start())
        return carry

    def est_wait(side):
        dv, dp = side
        dst_rows = {0: pl.ds(8, rows), -1: pl.ds(0, 8), 1: pl.ds(rows + 8, 8)}[dv]
        landing = est.at[planes_of[dp], :, dst_rows, :]
        pltpu.make_async_remote_copy(
            src_ref=landing, dst_ref=landing, send_sem=send_sem.at[0, SLOT[side]],
            recv_sem=recv_sem.at[0, SLOT[side]], device_id=(v0 + dv, p0 + dp),
            device_id_type=MESH_ID).wait_recv()

    def acc_wait(side):
        dv, dp = side
        landing = rz.at[0 if dp == -1 else 1] if dv == 0 else rs.at[SLOT[side]]
        pltpu.make_async_remote_copy(
            src_ref=landing, dst_ref=landing, send_sem=send_sem.at[1, SLOT[side]],
            recv_sem=recv_sem.at[1, SLOT[side]], device_id=(v0 + dv, p0 + dp),
            device_id_type=MESH_ID).wait_recv()

    lax.fori_loop(0, ITERS, iteration, 0)
    for h in range(2):
        out[:, :, h * 128:(h + 1) * 128] = est[pl.ds(depth, depth), h, pl.ds(8, rows), :]


def richardson_lucy(joined, stacked, kernels):
    views, pencils = stacked.shape[0], lax.axis_size("pencil")
    depth, rows, width = joined.shape
    frame = rows + 16
    vmem = pl.BlockSpec(memory_space=pltpu.VMEM)
    return pl.pallas_call(
        functools.partial(rl_kernel, views, pencils),
        name="deconvolve",
        out_shape=jax.ShapeDtypeStruct(joined.shape, F32),
        in_specs=[pl.BlockSpec(memory_space=pltpu.SMEM), vmem, vmem],
        out_specs=vmem,
        scratch_shapes=[
            pltpu.VMEM((3 * depth, 2, frame, 128), F32),
            pltpu.VMEM((depth, 2, frame, 128), F32),
            pltpu.VMEM((depth, 2, frame + 16, 128), F32),
            pltpu.VMEM((views, depth, 2, frame, 128), F32),
            pltpu.VMEM((3 * depth, 2, frame, 128), F32),
            pltpu.VMEM((2, depth, 2, rows, 128), F32),
            pltpu.VMEM((8, depth, 2, 8, 128), F32),
            pltpu.VMEM((views, width, width), BF16),
            pltpu.VMEM((views, width, width), BF16),
            pltpu.VMEM((views, width, width), BF16),
            pltpu.VMEM((views, width, width), BF16),
            pltpu.SemaphoreType.DMA((2, 8)),
            pltpu.SemaphoreType.DMA((2, 8)),
        ],
        compiler_params=pltpu.CompilerParams(collective_id=1, has_side_effects=True,
                                             vmem_limit_bytes=24 * 1024 * 1024),
    )(kernels, joined, stacked)


def two_terms(table):
    high = table.astype(jnp.bfloat16)
    low = (table - high.astype(np.float64)).astype(jnp.bfloat16)
    return [high, low]


def transform_tables(n, nx):
    at = np.arange(n)
    phase = 2.0 * np.pi * (at[:, None] * at[None, :] % n) / n
    cosine, sine = np.cos(phase), np.sin(phase)
    q = n // 4
    rows = np.concatenate([cosine.reshape(4, q, n), sine.reshape(4, q, n)], axis=1)

    x, c = np.arange(nx)[:, None], np.arange(nx // 2)[None, :]
    wave = 2.0 * np.pi * (x * c % nx) / nx
    sign = np.where(x % 2 == 0, 1.0, -1.0)
    columns = np.concatenate([np.cos(wave), np.where(c == 0, sign, -np.sin(wave))], axis=1)
    scale = 1.0 / (float(n) * n * nx)
    back_re = np.where(c == 0, 1.0, 2.0 * np.cos(wave)).T
    back_im = np.where(c == 0, sign, -2.0 * np.sin(wave)).T
    columns_back = np.concatenate([back_re, back_im], axis=0) * scale

    index = np.arange(2 * n)
    part, depth = index % 8 // 4, index // 8 * 4 + index % 4
    c_z, s_z = cosine[:, depth], sine[:, depth]
    depth_table = np.concatenate(
        [np.where(part == 0, c_z, s_z), np.where(part == 0, -s_z, c_z)], axis=0)

    m = np.arange(n // 2)
    back = []
    for core in range(2):
        ky = m // 2 * 4 + 2 * core + m % 2
        back.append(np.concatenate([cosine[:, ky], sine[:, ky]], axis=1))
    return [t for table in (rows, columns, depth_table, np.stack(back), columns_back)
            for t in two_terms(table)]


def right3(high, low, right):
    r_high, r_low = halves(right)
    return dot(high, r_high) + (dot(high, r_low) + dot(low, r_high))


def left3(left, high, low):
    l_high, l_low = halves(left)
    return dot(l_high, high) + (dot(l_high, low) + dot(l_low, high))


def reversal(n):
    total = lax.broadcasted_iota(jnp.int32, (n, n), 0) + lax.broadcasted_iota(jnp.int32, (n, n), 1)
    return jnp.where((total == 0) | (total == n), 1.0, 0.0).astype(BF16)


def moved_right(value, table):
    high, low = halves(value)
    return dot(high, table) + dot(low, table)


def moved_left(table, value):
    high, low = halves(value)
    return dot(table, high) + dot(table, low)


def join_kernel(pencils, slab, weight, csh, csl, dxh, dxl, mh, ml, cyh, cyl, dih, dil, out,
                xh, xl, msg, got, wsend, wgot, we, wm, mth, mtl, g, gr, gm, fr, pj, r1, r2,
                ssem, rsem, lsem):
    n = 4 * pencils
    q = n // 4
    half = pencils // 2
    v, p = lax.axis_index("view"), lax.axis_index("pencil")
    core = lax.rem(v, 2)
    mate = v + 1 - 2 * core
    far = lax.rem(v + 2, 4)
    mirror = pencils - 1 - p
    mirror0 = lax.rem(pencils - p, pencils)
    own_mirror = (p == 0) | (p == half)

    barrier = pltpu.get_barrier_semaphore()

    def greet(i, carry):
        pl.semaphore_signal(barrier, inc=1, device_id=(v, lax.rem(p + i, pencils)), device_id_type=MESH_ID)
        return carry

    lax.fori_loop(1, pencils, greet, 0)
    pl.semaphore_signal(barrier, inc=1, device_id=(mate, p), device_id_type=MESH_ID)
    pl.semaphore_signal(barrier, inc=1, device_id=(far, p), device_id_type=MESH_ID)

    def remote(src, dst, k, device):
        return pltpu.make_async_remote_copy(
            src_ref=src, dst_ref=dst, send_sem=ssem.at[k], recv_sem=rsem.at[k],
            device_id=device, device_id_type=MESH_ID)

    lane0 = lax.broadcasted_iota(jnp.int32, (n, 128), 1) == 0

    for j in range(4):
        receiver = mirror0 if j == 0 else mirror
        pick = lane0 & (receiver < half)
        wsend[j] = jnp.where(pick, weight[0, j], weight[1, j])

    pl.semaphore_wait(barrier, pencils + 1)
    w_rest = remote(wsend.at[pl.ds(1, 3)], wgot.at[pl.ds(1, 3)], 1, (v, mirror))
    w_first = remote(wsend.at[0], wgot.at[0], 2, (v, mirror0))
    w_local = pltpu.make_async_copy(wsend.at[0], wgot.at[0], lsem.at[0])
    w_rest.start()

    @pl.when(jnp.logical_not(own_mirror))
    def _():
        w_first.start()

    @pl.when(own_mirror)
    def _():
        w_local.start()

    for z in range(4):
        xh[z], xl[z] = halves(left3(slab[z], dxh[...], dxl[...]))

    lane_q = lax.broadcasted_iota(jnp.int32, (q, 128), 1) == 0
    row_q = lax.broadcasted_iota(jnp.int32, (q, 128), 0)

    def send_chunk(i, carry):
        peer = carry + i
        at = pl.multiple_of(peer * 32, 32)

        @pl.when(peer != p)
        def _():
            remote(msg.at[pl.ds(at, 32)], got.at[p], 0, (v, peer)).start()
        return carry

    for b in range(4):
        for z in range(4):
            both = (dot(csh[b], xh[z]) + (dot(csh[b], xl[z]) + dot(csl[b], xh[z])))
            c_re, c_im = both[:q, :128], both[:q, 128:]
            s_re, s_im = both[q:, :128], both[q:, 128:]
            re, im = c_re + s_im, c_im - s_re
            re0 = c_re if b < 2 else c_im
            im0 = -s_re if b < 2 else -s_im
            if b == 0:
                im0 = jnp.where(row_q == 0, c_im, im0)
            if b == 2:
                im0 = jnp.where(row_q == 0, c_re, im0)
            msg[pl.ds(b * q * 8 + z, q, stride=8), :] = jnp.where(lane_q, re0, re)
            msg[pl.ds(b * q * 8 + 4 + z, q, stride=8), :] = jnp.where(lane_q, im0, im)
        lax.fori_loop(0, pencils // 4, send_chunk, b * (pencils // 4))

    own = pltpu.make_async_copy(msg.at[pl.ds(pl.multiple_of(p * 32, 32), 32)], got.at[p], lsem.at[1])
    own.start()

    mth[...] = mh[...].astype(F32).T.astype(BF16)
    mtl[...] = ml[...].astype(F32).T.astype(BF16)
    w_rest.wait_recv()

    @pl.when(jnp.logical_not(own_mirror))
    def _():
        w_first.wait()

    @pl.when(own_mirror)
    def _():
        w_local.wait()

    turn_z, turn_x = reversal(n), reversal(128)
    for j in range(4):
        mine = jnp.where(lane0 & (p >= half), weight[1, j], weight[0, j])
        turned = moved_left(turn_z, moved_right(wgot[(4 - j) % 4], turn_x))
        we[j] = 0.5 * (mine + turned)

    @pl.when(own_mirror)
    def _():
        first = (lax.broadcasted_iota(jnp.int32, (n, 128), 0) * 0 + p) == 0
        other = jnp.where(first, weight[1, 0], weight[0, 0])
        other = 0.5 * (other + moved_left(turn_z, other))
        main = we[0]
        we[0] = jnp.where(lane0, 0.5 * (main + other), main)
        wm[...] = jnp.where(lane0, 0.5 * (main - other), 0.0)

    own.wait()
    remote(got.at[pl.ds(0, pencils - 1)], got.at[pl.ds(0, pencils - 1)], 0, (v, mirror)).wait_recv()

    def tile_rows(j):
        return got[:, 8 * j:8 * j + 8, :].reshape(2 * n, 128)

    for pair in range(2):
        f = right3(mh[...], ml[...], jnp.concatenate([tile_rows(2 * pair), tile_rows(2 * pair + 1)], axis=1))
        for k in range(2):
            j = 2 * pair + k
            for part in range(2):
                g[j, part * n:(part + 1) * n, :] = (
                    f[part * n:(part + 1) * n, 128 * k:128 * k + 128] * we[j])

    @pl.when(own_mirror)
    def _():
        imag = lax.rem(lax.broadcasted_iota(jnp.int32, (2 * n, 128), 0), 8) >= 4
        rows = tile_rows(0)
        f = right3(mh[...], ml[...], jnp.where(imag, -rows, rows))
        for part in range(2):
            g[0, part * n:(part + 1) * n, :] = (
                g[0, part * n:(part + 1) * n, :] + f[part * n:(part + 1) * n, :] * wm[...])

    pair_sum = remote(g.at[pl.ds(2 - 2 * core, 2)], gr, 3, (mate, p))
    pair_sum.start()
    pair_sum.wait_recv()
    f = right3(mth[...], mtl[...], jnp.concatenate(
        [g[2 * core] + gr[0], g[2 * core + 1] + gr[1]], axis=1))
    gm[:, 0:8, :] = f[:, :128].reshape(pencils, 8, 128)
    gm[:, 8:16, :] = f[:, 128:].reshape(pencils, 8, 128)

    def here(peer):
        return fr.at[pl.ds(pl.multiple_of(peer * 16, 16), 16)]

    def send_back(i, carry):
        peer = lax.rem(p + i, pencils)
        remote(gm.at[peer], here(p), 4, (v, peer)).start()
        return carry

    lax.fori_loop(1, pencils, send_back, 0)
    own_back = pltpu.make_async_copy(gm.at[p], here(p), lsem.at[2])
    own_back.start()
    own_back.wait()
    most = fr.at[pl.ds(0, 16 * (pencils - 1))]
    remote(most, most, 4, (v, mirror)).wait_recv()

    m = lax.broadcasted_iota(jnp.int32, (n // 2, 128), 0)
    ky = m // 2 * 4 + 2 * core + lax.rem(m, 2)
    lane_m = lax.broadcasted_iota(jnp.int32, (n // 2, 128), 1) == 0
    low, high = (ky > 0) & (ky < n // 2), ky > n // 2
    for z in range(4):
        re = fr[pl.ds(z, n // 2, stride=8), :]
        im = fr[pl.ds(4 + z, n // 2, stride=8), :]
        zero = jnp.zeros_like(re)
        v1 = jnp.where(low, 2.0 * re, jnp.where(ky == 0, re, jnp.where(ky == n // 2, im, zero)))
        v2 = jnp.where(high, 2.0 * re, jnp.where(ky == 0, im, jnp.where(ky == n // 2, re, zero)))
        b1 = jnp.where(low, -2.0 * im, zero)
        b2 = jnp.where(high, -2.0 * im, zero)
        top = jnp.concatenate([jnp.where(lane_m, v1, re), jnp.where(lane_m, v2, im)], axis=1)
        bottom = jnp.concatenate([jnp.where(lane_m, b1, -im), jnp.where(lane_m, b2, re)], axis=1)
        u = right3(cyh[core], cyl[core], jnp.concatenate([top, bottom], axis=0))
        rows = left3(u, dih[...], dil[...])
        for quarter in range(4):
            pj[quarter // 2, quarter % 2, z] = rows[quarter * q:(quarter + 1) * q]

    near = remote(pj.at[:, 1 - core], r1, 5, (mate, p))
    near.start()
    near.wait_recv()
    away = lax.rem(v // 2 + 1, 2)
    kept = v // 2
    r1[...] = r1[...] + pj[:, core]
    long = remote(r1.at[away], r2, 6, (far, p))
    long.start()
    long.wait_recv()
    out[...] = r1[kept] + r2[...]

    w_rest.wait_send()
    sent = msg.at[pl.ds(0, 32 * (pencils - 1))]
    remote(sent, sent, 0, (v, mirror)).wait_send()
    pair_sum.wait_send()
    sent_back = gm.at[pl.ds(0, pencils - 1)]
    remote(sent_back, sent_back, 4, (v, mirror)).wait_send()
    near.wait_send()
    long.wait_send()


def spectral_join(slab, weight):
    pencils = lax.axis_size("pencil")
    n, nx = 4 * pencils, slab.shape[-1]
    q = n // 4
    vmem = pl.BlockSpec(memory_space=pltpu.VMEM)
    tables = [jnp.asarray(t) for t in transform_tables(n, nx)]
    return pl.pallas_call(
        functools.partial(join_kernel, pencils),
        name="join",
        out_shape=jax.ShapeDtypeStruct((4, q, nx), F32),
        in_specs=[vmem] * (2 + len(tables)),
        out_specs=vmem,
        scratch_shapes=[
            pltpu.VMEM((4, n, nx), BF16),
            pltpu.VMEM((4, n, nx), BF16),
            pltpu.VMEM((8 * n, 128), F32),
            pltpu.VMEM((pencils, 32, 128), F32),
            pltpu.VMEM((4, n, 128), F32),
            pltpu.VMEM((4, n, 128), F32),
            pltpu.VMEM((4, n, 128), F32),
            pltpu.VMEM((n, 128), F32),
            pltpu.VMEM((2 * n, 2 * n), BF16),
            pltpu.VMEM((2 * n, 2 * n), BF16),
            pltpu.VMEM((4, 2 * n, 128), F32),
            pltpu.VMEM((2, 2 * n, 128), F32),
            pltpu.VMEM((pencils, 16, 128), F32),
            pltpu.VMEM((pencils * 16, 128), F32),
            pltpu.VMEM((2, 2, 4, q, nx), F32),
            pltpu.VMEM((2, 4, q, nx), F32),
            pltpu.VMEM((4, q, nx), F32),
            pltpu.SemaphoreType.DMA((7,)),
            pltpu.SemaphoreType.DMA((7,)),
            pltpu.SemaphoreType.DMA((3,)),
        ],
        compiler_params=pltpu.CompilerParams(collective_id=2, has_side_effects=True,
                                             vmem_limit_bytes=40 * 1024 * 1024),
    )(slab, weight, *tables)


def weight_halves(block):
    n, chunk, nx = block.shape
    return jnp.transpose(block.reshape(n, chunk, 2, nx // 2), (2, 1, 0, 3))


def body(recorded, spectral_weight, psf_taps):
    kernels = psf_taps / jnp.sum(psf_taps, axis=-1, keepdims=True)
    stacked = lax.all_to_all(recorded, "view", split_axis=2, concat_axis=0, tiled=True)
    joined = spectral_join(recorded[0], weight_halves(spectral_weight[0]))
    return (joined, richardson_lucy(joined, stacked, kernels))


def solution(mesh):
    return jax.shard_map(
        body,
        mesh=mesh,
        in_specs=(P("view", "pencil", None, None), P("view", None, "pencil", None), P()),
        out_specs=(P("pencil", "view", None), P("pencil", "view", None)),
        check_vma=False,
    )
```

```python
import functools

import jax
import jax.numpy as jnp
import numpy as np
from jax import lax
from jax.experimental import pallas as pl
from jax.experimental.pallas import tpu as pltpu
from jax.sharding import PartitionSpec as P

ITERS = 2
MESH_ID = pl.DeviceIdType.MESH
F32 = jnp.float32
BF16 = jnp.bfloat16
SIDES = [(dv, dp) for dp in (-1, 1, 0) for dv in (0, -1, 1) if (dv, dp) != (0, 0)]
SLOT = {side: k for k, side in enumerate(SIDES)}


def halves(value):
    high = value.astype(BF16)
    return high, (value - high.astype(F32)).astype(BF16)


def dot(left, right):
    return jnp.dot(left, right, preferred_element_type=F32)


def two_terms(table):
    high = table.astype(jnp.bfloat16)
    low = (table - high.astype(np.float64)).astype(jnp.bfloat16)
    return [high, low]


def transform_tables(n, nx):
    at = np.arange(n)
    phase = 2.0 * np.pi * (at[:, None] * at[None, :] % n) / n
    cosine, sine = np.cos(phase), np.sin(phase)
    q = n // 4
    rows = np.concatenate([cosine.reshape(4, q, n), sine.reshape(4, q, n)], axis=1)

    x, c = np.arange(nx)[:, None], np.arange(nx // 2)[None, :]
    wave = 2.0 * np.pi * (x * c % nx) / nx
    sign = np.where(x % 2 == 0, 1.0, -1.0)
    columns = np.concatenate([np.cos(wave), np.where(c == 0, sign, -np.sin(wave))], axis=1)
    scale = 1.0 / (float(n) * n * nx)
    back_re = np.where(c == 0, 1.0, 2.0 * np.cos(wave)).T
    back_im = np.where(c == 0, sign, -2.0 * np.sin(wave)).T
    columns_back = np.concatenate([back_re, back_im], axis=0) * scale

    index = np.arange(2 * n)
    part, depth = index % 8 // 4, index // 8 * 4 + index % 4
    c_z, s_z = cosine[:, depth], sine[:, depth]
    depth_table = np.concatenate(
        [np.where(part == 0, c_z, s_z), np.where(part == 0, -s_z, c_z)], axis=0)

    m = np.arange(n // 2)
    back = []
    for core in range(2):
        ky = m // 2 * 4 + 2 * core + m % 2
        back.append(np.concatenate([cosine[:, ky], sine[:, ky]], axis=1))
    return [t for table in (rows, columns, depth_table, np.stack(back), columns_back)
            for t in two_terms(table)]


def right3(high, low, right):
    r_high, r_low = halves(right)
    return dot(high, r_high) + (dot(high, r_low) + dot(low, r_high))


def left3(left, high, low):
    l_high, l_low = halves(left)
    return dot(l_high, high) + (dot(l_high, low) + dot(l_low, high))


def reversal(n):
    total = lax.broadcasted_iota(jnp.int32, (n, n), 0) + lax.broadcasted_iota(jnp.int32, (n, n), 1)
    return jnp.where((total == 0) | (total == n), 1.0, 0.0).astype(BF16)


def moved_right(value, table):
    high, low = halves(value)
    return dot(high, table) + dot(low, table)


def moved_left(table, value):
    high, low = halves(value)
    return dot(table, high) + dot(table, low)


def dot3(left, right_high, right_low):
    high, low = halves(left)
    return dot(high, right_high) + (dot(high, right_low) + dot(low, right_high))


def kernel(views, pencils, taps, slab_ref, weight_ref, *refs):
    table_refs, refs = refs[:10], refs[10:]
    (out, out2, slab, weight, csh, csl, dxh, dxl, mh, ml, cyh, cyl, dih, dil,
     xh, xl, msg, got, wsend, wgot, we, wm, mth, mtl, g, gr, gm, fr, pj, r1, r2,
     stacked, est, zed, mid, spread, acc, rz, rs, th, tl, ah, al,
     ssem, rsem, lsem, load_sem, share_sem, send_sem, recv_sem) = refs
    n = 4 * pencils
    q = n // 4
    half = pencils // 2
    v, p = lax.axis_index("view"), lax.axis_index("pencil")
    core = lax.rem(v, 2)
    mate = v + 1 - 2 * core
    far = lax.rem(v + 2, 4)
    mirror = pencils - 1 - p
    mirror0 = lax.rem(pencils - p, pencils)
    own_mirror = (p == 0) | (p == half)

    tables = [csh, csl, dxh, dxl, mh, ml, cyh, cyl, dih, dil]
    loads = [pltpu.make_async_copy(src, dst, load_sem.at[k])
             for k, (src, dst) in enumerate(zip(table_refs, tables))]
    slab_load = pltpu.make_async_copy(slab_ref, slab, load_sem.at[10])
    weight_loads = [pltpu.make_async_copy(weight_ref.at[:, :, pl.ds(128 * h, 128)], weight.at[h], load_sem.at[11 + h])
                    for h in range(2)]
    slab_load.start()
    for load in loads[2:4] + weight_loads + loads[:2] + loads[4:]:
        load.start()
    flat = [weight.at[h].reshape(4 * n, 128) for h in range(2)]

    def weight_rows(h, j):
        return flat[h][pl.ds(j, n, stride=4), :]

    depth, rows, width = 4, q, slab.shape[-1]
    frame = rows + 16

    def exists(side):
        v1, p1 = v + side[0], p + side[1]
        return (v1 >= 0) & (v1 < views) & (p1 >= 0) & (p1 < pencils)

    def back(side):
        return (-side[0], -side[1])

    def each(sides, action):
        for side in sides:
            @pl.when(exists(side))
            def _(side=side):
                action(side)

    est[...] = jnp.zeros_like(est)
    rz[...] = jnp.zeros_like(rz)
    rs[...] = jnp.zeros_like(rs)

    barrier = pltpu.get_barrier_semaphore()

    def greet(i, carry):
        pl.semaphore_signal(barrier, inc=1, device_id=(v, lax.rem(p + i, pencils)), device_id_type=MESH_ID)
        return carry

    lax.fori_loop(1, pencils, greet, 0)
    for d in range(1, 4):
        pl.semaphore_signal(barrier, inc=1, device_id=(lax.rem(v + d, views), p), device_id_type=MESH_ID)
    corners = [side for side in SIDES if side[0] != 0 and side[1] != 0]

    def greet_corner(side):
        pl.semaphore_signal(barrier, inc=1, device_id=(v + side[0], p + side[1]), device_id_type=MESH_ID)

    each(corners, greet_corner)
    expected = pencils - 1 + 3 + sum(exists(side).astype(jnp.int32) for side in corners)

    slab_load.wait()
    loads[2].wait()
    loads[3].wait()
    for z in range(4):
        xh[z], xl[z] = halves(left3(slab[z], dxh[...], dxl[...]))
    mid[...] = jnp.zeros_like(mid)
    for load in weight_loads + loads[:2]:
        load.wait()

    def remote(src, dst, k, device):
        return pltpu.make_async_remote_copy(
            src_ref=src, dst_ref=dst, send_sem=ssem.at[k], recv_sem=rsem.at[k],
            device_id=device, device_id_type=MESH_ID)

    lane0 = lax.broadcasted_iota(jnp.int32, (n, 128), 1) == 0

    for j in range(4):
        receiver = mirror0 if j == 0 else mirror
        pick = lane0 & (receiver < half)
        wsend[j] = jnp.where(pick, weight_rows(0, j), weight_rows(1, j))

    pl.semaphore_wait(barrier, expected)
    w_rest = remote(wsend.at[pl.ds(1, 3)], wgot.at[pl.ds(1, 3)], 1, (v, mirror))
    w_first = remote(wsend.at[0], wgot.at[0], 2, (v, mirror0))
    w_local = pltpu.make_async_copy(wsend.at[0], wgot.at[0], lsem.at[0])
    w_rest.start()

    @pl.when(jnp.logical_not(own_mirror))
    def _():
        w_first.start()

    @pl.when(own_mirror)
    def _():
        w_local.start()

    lane_q = lax.broadcasted_iota(jnp.int32, (q, 128), 1) == 0
    row_q = lax.broadcasted_iota(jnp.int32, (q, 128), 0)

    group = pencils // 4
    for step in range(4):
        b = lax.rem(p // group + step, 4)
        first = b < 2
        for z in range(4):
            both = (dot(csh[b], xh[z]) + (dot(csh[b], xl[z]) + dot(csl[b], xh[z])))
            c_re, c_im = both[:q, :128], both[:q, 128:]
            s_re, s_im = both[q:, :128], both[q:, 128:]
            re, im = c_re + s_im, c_im - s_re
            re0 = jnp.where(first, c_re, c_im)
            im0 = jnp.where(first, -s_re, -s_im)
            im0 = jnp.where((row_q == 0) & (b == 0), c_im, im0)
            im0 = jnp.where((row_q == 0) & (b == 2), c_re, im0)
            at = pl.multiple_of(b * (q * 8), q * 8)
            msg[pl.ds(at + z, q, stride=8), :] = jnp.where(lane_q, re0, re)
            msg[pl.ds(at + 4 + z, q, stride=8), :] = jnp.where(lane_q, im0, im)

        def send_chunk(i, carry, b=b):
            peer = b * group + lax.rem(p + i, group)
            at = pl.multiple_of(peer * 32, 32)

            @pl.when(peer != p)
            def _():
                remote(msg.at[pl.ds(at, 32)], got.at[p], 0, (v, peer)).start()
            return carry

        lax.fori_loop(0, group, send_chunk, 0)

    own = pltpu.make_async_copy(msg.at[pl.ds(pl.multiple_of(p * 32, 32), 32)], got.at[p], lsem.at[1])
    own.start()

    def quarter_of(view):
        return slab.at[:, pl.ds(pl.multiple_of(view * q, q), q), :]

    shares = [pltpu.make_async_remote_copy(
        src_ref=quarter_of(lax.rem(v + d, views)), dst_ref=stacked.at[v],
        send_sem=share_sem.at[0, d - 1], recv_sem=share_sem.at[1, d - 1],
        device_id=(lax.rem(v + d, views), p), device_id_type=MESH_ID) for d in range(1, 4)]
    for share in shares:
        share.start()
    own_share = pltpu.make_async_copy(quarter_of(v), stacked.at[v], lsem.at[3])
    own_share.start()

    for load in loads[4:]:
        load.wait()
    mth[...] = mh[...].astype(F32).T.astype(BF16)
    mtl[...] = ml[...].astype(F32).T.astype(BF16)
    def band(v, carry):
        at = (lax.broadcasted_iota(jnp.int32, (width, width), 0)
              - lax.broadcasted_iota(jnp.int32, (width, width), 1))
        table, turned = jnp.zeros((width, width), F32), jnp.zeros((width, width), F32)
        for t in range(9):
            tap = taps[v, 2, t]
            table = jnp.where(at == t - 4, tap, table)
            turned = jnp.where(at == 4 - t, tap, turned)
        th[v], tl[v] = halves(table)
        ah[v], al[v] = halves(turned)
        return carry

    lax.fori_loop(0, views, band, 0)

    w_rest.wait_recv()

    @pl.when(jnp.logical_not(own_mirror))
    def _():
        w_first.wait_recv()

    @pl.when(own_mirror)
    def _():
        w_local.wait()

    turn_z, turn_x = reversal(n), reversal(128)
    for j in range(4):
        mine = jnp.where(lane0 & (p >= half), weight_rows(1, j), weight_rows(0, j))
        turned = moved_left(turn_z, moved_right(wgot[(4 - j) % 4], turn_x))
        we[j] = 0.5 * (mine + turned)

    @pl.when(own_mirror)
    def _():
        first = (lax.broadcasted_iota(jnp.int32, (n, 128), 0) * 0 + p) == 0
        other = jnp.where(first, weight_rows(1, 0), weight_rows(0, 0))
        other = 0.5 * (other + moved_left(turn_z, other))
        main = we[0]
        we[0] = jnp.where(lane0, 0.5 * (main + other), main)
        wm[...] = jnp.where(lane0, 0.5 * (main - other), 0.0)

    own.wait()
    remote(got.at[pl.ds(0, pencils - 1)], got.at[pl.ds(0, pencils - 1)], 0, (v, mirror)).wait_recv()

    def tile_rows(j):
        return got[:, 8 * j:8 * j + 8, :].reshape(2 * n, 128)

    for pair in range(2):
        f = right3(mh[...], ml[...], jnp.concatenate([tile_rows(2 * pair), tile_rows(2 * pair + 1)], axis=1))
        for k in range(2):
            j = 2 * pair + k
            for part in range(2):
                g[j, part * n:(part + 1) * n, :] = (
                    f[part * n:(part + 1) * n, 128 * k:128 * k + 128] * we[j])

    @pl.when(own_mirror)
    def _():
        imag = lax.rem(lax.broadcasted_iota(jnp.int32, (2 * n, 128), 0), 8) >= 4
        rows = tile_rows(0)
        f = right3(mh[...], ml[...], jnp.where(imag, -rows, rows))
        for part in range(2):
            g[0, part * n:(part + 1) * n, :] = (
                g[0, part * n:(part + 1) * n, :] + f[part * n:(part + 1) * n, :] * wm[...])

    pair_sum = remote(g.at[pl.ds(2 - 2 * core, 2)], gr, 3, (mate, p))
    pair_sum.start()
    pair_sum.wait_recv()
    f = right3(mth[...], mtl[...], jnp.concatenate(
        [g[2 * core] + gr[0], g[2 * core + 1] + gr[1]], axis=1))
    gm[:, 0:8, :] = f[:, :128].reshape(pencils, 8, 128)
    gm[:, 8:16, :] = f[:, 128:].reshape(pencils, 8, 128)

    def here(peer):
        return fr.at[pl.ds(pl.multiple_of(peer * 16, 16), 16)]

    def send_back(i, carry):
        peer = lax.rem(p + i, pencils)
        remote(gm.at[peer], here(p), 4, (v, peer)).start()
        return carry

    lax.fori_loop(1, pencils, send_back, 0)
    own_back = pltpu.make_async_copy(gm.at[p], here(p), lsem.at[2])
    own_back.start()
    own_back.wait()
    most = fr.at[pl.ds(0, 16 * (pencils - 1))]
    remote(most, most, 4, (v, mirror)).wait_recv()

    m = lax.broadcasted_iota(jnp.int32, (n // 2, 128), 0)
    ky = m // 2 * 4 + 2 * core + lax.rem(m, 2)
    lane_m = lax.broadcasted_iota(jnp.int32, (n // 2, 128), 1) == 0
    low, high = (ky > 0) & (ky < n // 2), ky > n // 2
    for z in range(4):
        re = fr[pl.ds(z, n // 2, stride=8), :]
        im = fr[pl.ds(4 + z, n // 2, stride=8), :]
        zero = jnp.zeros_like(re)
        v1 = jnp.where(low, 2.0 * re, jnp.where(ky == 0, re, jnp.where(ky == n // 2, im, zero)))
        v2 = jnp.where(high, 2.0 * re, jnp.where(ky == 0, im, jnp.where(ky == n // 2, re, zero)))
        b1 = jnp.where(low, -2.0 * im, zero)
        b2 = jnp.where(high, -2.0 * im, zero)
        top = jnp.concatenate([jnp.where(lane_m, v1, re), jnp.where(lane_m, v2, im)], axis=1)
        bottom = jnp.concatenate([jnp.where(lane_m, b1, -im), jnp.where(lane_m, b2, re)], axis=1)
        u = right3(cyh[core], cyl[core], jnp.concatenate([top, bottom], axis=0))
        field = left3(u, dih[...], dil[...])
        for quarter in range(4):
            pj[quarter // 2, quarter % 2, z] = field[quarter * q:(quarter + 1) * q]

    near = remote(pj.at[:, 1 - core], r1, 5, (mate, p))
    near.start()
    near.wait_recv()
    away = lax.rem(v // 2 + 1, 2)
    kept = v // 2
    r1[...] = r1[...] + pj[:, core]
    long = remote(r1.at[away], r2, 6, (far, p))
    long.start()
    long.wait_recv()
    out[...] = r1[kept] + r2[...]


    planes_of = {-1: pl.ds(0, depth), 0: pl.ds(depth, depth), 1: pl.ds(2 * depth, depth)}

    def est_copy(side):
        dv, dp = side
        src_rows = {0: pl.ds(8, rows), 1: pl.ds(rows, 8), -1: pl.ds(8, 8)}[dv]
        dst_rows = {0: pl.ds(8, rows), 1: pl.ds(0, 8), -1: pl.ds(rows + 8, 8)}[dv]
        return pltpu.make_async_remote_copy(
            src_ref=est.at[planes_of[0], :, src_rows, :],
            dst_ref=est.at[planes_of[-dp], :, dst_rows, :],
            send_sem=send_sem.at[0, SLOT[side]],
            recv_sem=recv_sem.at[0, SLOT[back(side)]],
            device_id=(v + dv, p + dp),
            device_id_type=MESH_ID,
        )

    def acc_copy(side):
        dv, dp = side
        src_rows = {0: pl.ds(8, rows), 1: pl.ds(rows + 8, 8), -1: pl.ds(0, 8)}[dv]
        slot = SLOT[back(side)]
        landing = rz.at[0 if dp == 1 else 1] if dv == 0 else rs.at[slot]
        return pltpu.make_async_remote_copy(
            src_ref=acc.at[planes_of[dp], :, src_rows, :],
            dst_ref=landing,
            send_sem=send_sem.at[1, SLOT[side]],
            recv_sem=recv_sem.at[1, slot],
            device_id=(v + dv, p + dp),
            device_id_type=MESH_ID,
        )

    def est_wait(side):
        dv, dp = side
        dst_rows = {0: pl.ds(8, rows), -1: pl.ds(0, 8), 1: pl.ds(rows + 8, 8)}[dv]
        landing = est.at[planes_of[dp], :, dst_rows, :]
        pltpu.make_async_remote_copy(
            src_ref=landing, dst_ref=landing, send_sem=send_sem.at[0, SLOT[side]],
            recv_sem=recv_sem.at[0, SLOT[side]], device_id=(v + dv, p + dp),
            device_id_type=MESH_ID).wait_recv()

    def acc_wait(side):
        dv, dp = side
        landing = rz.at[0 if dp == -1 else 1] if dv == 0 else rs.at[SLOT[side]]
        pltpu.make_async_remote_copy(
            src_ref=landing, dst_ref=landing, send_sem=send_sem.at[1, SLOT[side]],
            recv_sem=recv_sem.at[1, SLOT[side]], device_id=(v + dv, p + dp),
            device_id_type=MESH_ID).wait_recv()

    for h in range(2):
        s = out[:, :, h * 128:(h + 1) * 128]
        est[pl.ds(depth, depth), h, pl.ds(8, rows), :] = 0.1 + (
            jnp.maximum(s, 0.0) + jnp.log1p(jnp.exp(-jnp.abs(s))))

    each(SIDES, lambda side: est_copy(side).start())
    own_share.wait()
    for share in shares:
        share.wait_recv()

    def view_step(w, carry):
        for z in range(depth):
            total = taps[w, 0, 0] * est[z]
            for t in range(1, 9):
                total = total + taps[w, 0, t] * est[z + t]
            zed[z] = total
        sides = []
        for h in range(2):
            planes = []
            for z in range(depth):
                total = taps[w, 1, 0] * zed[z, h, pl.ds(4, rows), :]
                for t in range(1, 9):
                    total = total + taps[w, 1, t] * zed[z, h, pl.ds(4 + t, rows), :]
                planes.append(total)
            sides.append(jnp.concatenate(planes, axis=0))
        blurred = dot3(jnp.concatenate(sides, axis=1), th[w], tl[w])
        ratio = stacked[w].reshape(depth * rows, width) / blurred
        turned = dot3(ratio, ah[w], al[w])
        for z in range(depth):
            for h in range(2):
                mid[z, h, pl.ds(16, rows), :] = turned[z * rows:(z + 1) * rows, h * 128:(h + 1) * 128]
        for z in range(depth):
            for h in range(2):
                total = taps[w, 1, 8] * mid[z, h, pl.ds(4, frame), :]
                for t in range(1, 9):
                    total = total + taps[w, 1, 8 - t] * mid[z, h, pl.ds(4 + t, frame), :]
                spread[w, z, h] = total
        return carry

    def gather_planes(planes):
        for zo in planes:
            total = None
            for v in range(views):
                for zs in range(depth):
                    if 0 <= zo - zs <= 8:
                        term = taps[v, 0, zo - zs] * spread[v, zs]
                        total = term if total is None else total + term
            acc[zo] = total

    def iteration(step, carry):
        each(SIDES, est_wait)
        lax.fori_loop(0, views, view_step, 0)
        gather_planes(list(range(0, depth)) + list(range(2 * depth, 3 * depth)))
        each([s for s in SIDES if s[1] != 0], lambda side: acc_copy(side).start())
        gather_planes(range(depth, 2 * depth))
        each([s for s in SIDES if s[1] == 0], lambda side: acc_copy(side).start())
        each(SIDES, lambda side: est_copy(side).wait_send())
        each(SIDES, acc_wait)
        for z in range(depth):
            for h in range(2):
                total = acc[depth + z, h, pl.ds(8, rows), :] + (rz[0, z, h] + rz[1, z, h])
                low = rs[SLOT[(-1, 0)], z, h] + (rs[SLOT[(-1, -1)], z, h] + rs[SLOT[(-1, 1)], z, h])
                high = rs[SLOT[(1, 0)], z, h] + (rs[SLOT[(1, -1)], z, h] + rs[SLOT[(1, 1)], z, h])
                total = jnp.concatenate(
                    [total[:8] + low, total[8:rows - 8], total[rows - 8:] + high], axis=0)
                fresh = est[depth + z, h, pl.ds(8, rows), :] * (total * (1.0 / views))
                est[depth + z, h, pl.ds(8, rows), :] = fresh
        each(SIDES, lambda side: acc_copy(side).wait_send())

        @pl.when(step < ITERS - 1)
        def _():
            each(SIDES, lambda side: est_copy(side).start())
        return carry

    lax.fori_loop(0, ITERS, iteration, 0)
    for h in range(2):
        out2[:, :, h * 128:(h + 1) * 128] = est[pl.ds(depth, depth), h, pl.ds(8, rows), :]

    w_rest.wait_send()
    sent = msg.at[pl.ds(0, 32 * (pencils - 1))]
    remote(sent, sent, 0, (v, mirror)).wait_send()
    pair_sum.wait_send()
    sent_back = gm.at[pl.ds(0, pencils - 1)]
    remote(sent_back, sent_back, 4, (v, mirror)).wait_send()
    near.wait_send()
    long.wait_send()

    @pl.when(jnp.logical_not(own_mirror))
    def _():
        w_first.wait_send()
    for share in shares:
        share.wait_send()


def whole(recorded, weight, taps):
    views, pencils = lax.axis_size("view"), lax.axis_size("pencil")
    n, nx = 4 * pencils, recorded.shape[-1]
    q, depth = n // 4, 4
    frame = q + 16
    vmem, left = pl.BlockSpec(memory_space=pltpu.VMEM), pl.BlockSpec(memory_space=pl.ANY)
    tables = [jnp.asarray(t) for t in transform_tables(n, nx)]
    block = jax.ShapeDtypeStruct((depth, q, nx), F32)
    return pl.pallas_call(
        functools.partial(kernel, views, pencils),
        name="join_and_deconvolve",
        out_shape=(block, block),
        in_specs=[pl.BlockSpec(memory_space=pltpu.SMEM)] + [left] * (2 + len(tables)),
        out_specs=(vmem, vmem),
        scratch_shapes=[
            pltpu.VMEM((4, n, nx), F32),
            pltpu.VMEM((2, n, 4, 128), F32),
            *[pltpu.VMEM(t.shape, t.dtype) for t in tables],
            pltpu.VMEM((4, n, nx), BF16),
            pltpu.VMEM((4, n, nx), BF16),
            pltpu.VMEM((8 * n, 128), F32),
            pltpu.VMEM((pencils, 32, 128), F32),
            pltpu.VMEM((4, n, 128), F32),
            pltpu.VMEM((4, n, 128), F32),
            pltpu.VMEM((4, n, 128), F32),
            pltpu.VMEM((n, 128), F32),
            pltpu.VMEM((2 * n, 2 * n), BF16),
            pltpu.VMEM((2 * n, 2 * n), BF16),
            pltpu.VMEM((4, 2 * n, 128), F32),
            pltpu.VMEM((2, 2 * n, 128), F32),
            pltpu.VMEM((pencils, 16, 128), F32),
            pltpu.VMEM((pencils * 16, 128), F32),
            pltpu.VMEM((2, 2, 4, q, nx), F32),
            pltpu.VMEM((2, 4, q, nx), F32),
            pltpu.VMEM((4, q, nx), F32),
            pltpu.VMEM((views, depth, q, nx), F32),
            pltpu.VMEM((3 * depth, 2, frame, 128), F32),
            pltpu.VMEM((depth, 2, frame, 128), F32),
            pltpu.VMEM((depth, 2, frame + 16, 128), F32),
            pltpu.VMEM((views, depth, 2, frame, 128), F32),
            pltpu.VMEM((3 * depth, 2, frame, 128), F32),
            pltpu.VMEM((2, depth, 2, q, 128), F32),
            pltpu.VMEM((8, depth, 2, 8, 128), F32),
            *[pltpu.VMEM((views, nx, nx), BF16)] * 4,
            pltpu.SemaphoreType.DMA((7,)),
            pltpu.SemaphoreType.DMA((7,)),
            pltpu.SemaphoreType.DMA((4,)),
            pltpu.SemaphoreType.DMA((13,)),
            pltpu.SemaphoreType.DMA((2, 3)),
            pltpu.SemaphoreType.DMA((2, 8)),
            pltpu.SemaphoreType.DMA((2, 8)),
        ],
        compiler_params=pltpu.CompilerParams(collective_id=1, has_side_effects=True,
                                             vmem_limit_bytes=48 * 1024 * 1024),
    )(taps, recorded, weight, *tables)


def body(recorded, spectral_weight, psf_taps):
    kernels = psf_taps / jnp.sum(psf_taps, axis=-1, keepdims=True)
    return whole(recorded[0], spectral_weight[0], kernels)


def solution(mesh):
    return jax.shard_map(
        body,
        mesh=mesh,
        in_specs=(P("view", "pencil", None, None), P("view", None, "pencil", None), P()),
        out_specs=(P("pencil", "view", None), P("pencil", "view", None)),
        check_vma=False,
    )
```

```python
import functools

import jax
import jax.numpy as jnp
import numpy as np
from jax import lax
from jax.experimental import pallas as pl
from jax.experimental.pallas import tpu as pltpu
from jax.sharding import PartitionSpec as P

ITERS = 2
UNROLL = 4
MESH_ID = pl.DeviceIdType.MESH
F32 = jnp.float32
BF16 = jnp.bfloat16
SIDES = [(dv, dp) for dp in (-1, 1, 0) for dv in (0, -1, 1) if (dv, dp) != (0, 0)]
SLOT = {side: k for k, side in enumerate(SIDES)}


def halves(value):
    high = value.astype(BF16)
    return high, (value - high.astype(F32)).astype(BF16)


def dot(left, right):
    return jnp.dot(left, right, preferred_element_type=F32)


def two_terms(table):
    high = table.astype(jnp.bfloat16)
    low = (table - high.astype(np.float64)).astype(jnp.bfloat16)
    return [high, low]


def transform_tables(n, nx):
    at = np.arange(n)
    phase = 2.0 * np.pi * (at[:, None] * at[None, :] % n) / n
    cosine, sine = np.cos(phase), np.sin(phase)
    q = n // 4
    rows = np.concatenate([cosine.reshape(4, q, n), sine.reshape(4, q, n)], axis=1)

    x, c = np.arange(nx)[:, None], np.arange(nx // 2)[None, :]
    wave = 2.0 * np.pi * (x * c % nx) / nx
    sign = np.where(x % 2 == 0, 1.0, -1.0)
    columns = np.concatenate([np.cos(wave), np.where(c == 0, sign, -np.sin(wave))], axis=1)
    scale = 1.0 / (float(n) * n * nx)
    back_re = np.where(c == 0, 1.0, 2.0 * np.cos(wave)).T
    back_im = np.where(c == 0, sign, -2.0 * np.sin(wave)).T
    columns_back = np.concatenate([back_re, back_im], axis=0) * scale

    index = np.arange(2 * n)
    part, depth = index % 8 // 4, index // 8 * 4 + index % 4
    c_z, s_z = cosine[:, depth], sine[:, depth]
    depth_table = np.concatenate(
        [np.where(part == 0, c_z, s_z), np.where(part == 0, -s_z, c_z)], axis=0)

    m = np.arange(n // 2)
    back = []
    for core in range(2):
        ky = m // 2 * 4 + 2 * core + m % 2
        back.append(np.concatenate([cosine[:, ky], sine[:, ky]], axis=1))
    return [t for table in (rows, columns, depth_table, np.stack(back), columns_back)
            for t in two_terms(table)]


def right3(high, low, right):
    r_high, r_low = halves(right)
    return dot(high, r_high) + (dot(high, r_low) + dot(low, r_high))


def left3(left, high, low):
    l_high, l_low = halves(left)
    return dot(l_high, high) + (dot(l_high, low) + dot(l_low, high))


def reversal(n):
    total = lax.broadcasted_iota(jnp.int32, (n, n), 0) + lax.broadcasted_iota(jnp.int32, (n, n), 1)
    return jnp.where((total == 0) | (total == n), 1.0, 0.0).astype(BF16)


def moved_right(value, table):
    high, low = halves(value)
    return dot(high, table) + dot(low, table)


def moved_left(table, value):
    high, low = halves(value)
    return dot(table, high) + dot(table, low)


def dot3(left, right_high, right_low):
    high, low = halves(left)
    return dot(high, right_high) + (dot(high, right_low) + dot(low, right_high))


def kernel(views, pencils, taps, slab_ref, weight_ref, *refs):
    table_refs, refs = refs[:10], refs[10:]
    (out, out2, slab, weight, csh, csl, dxh, dxl, mh, ml, cyh, cyl, dih, dil,
     xh, xl, msg, got, wsend, wgot, we, wm, mth, mtl, g, gr, fs, gm, fr, pj, r1, r2,
     stacked, est, zed, mid, spread, acc, rz, rs, th, tl, ah, al,
     ssem, rsem, lsem, load_sem, share_sem, send_sem, recv_sem) = refs
    n = 4 * pencils
    q = n // 4
    half = pencils // 2
    v, p = lax.axis_index("view"), lax.axis_index("pencil")
    core = lax.rem(v, 2)
    mate = v + 1 - 2 * core
    far = lax.rem(v + 2, 4)
    mirror = pencils - 1 - p
    mirror0 = lax.rem(pencils - p, pencils)
    own_mirror = (p == 0) | (p == half)

    tables = [csh, csl, dxh, dxl, mh, ml, cyh, cyl, dih, dil]
    loads = [pltpu.make_async_copy(src, dst, load_sem.at[k])
             for k, (src, dst) in enumerate(zip(table_refs, tables))]
    slab_load = pltpu.make_async_copy(slab_ref, slab, load_sem.at[10])
    weight_loads = [pltpu.make_async_copy(weight_ref.at[:, :, pl.ds(128 * h, 128)], weight.at[h], load_sem.at[11 + h])
                    for h in range(2)]
    slab_load.start()
    for load in loads[2:4] + weight_loads + loads[:2] + loads[4:]:
        load.start()
    flat = [weight.at[h].reshape(4 * n, 128) for h in range(2)]

    def weight_rows(h, j):
        return flat[h][pl.ds(j, n, stride=4), :]

    depth, rows, width = 4, q, slab.shape[-1]
    frame = rows + 16

    def exists(side):
        v1, p1 = v + side[0], p + side[1]
        return (v1 >= 0) & (v1 < views) & (p1 >= 0) & (p1 < pencils)

    def back(side):
        return (-side[0], -side[1])

    def each(sides, action):
        for side in sides:
            @pl.when(exists(side))
            def _(side=side):
                action(side)

    est[...] = jnp.zeros_like(est)
    rz[...] = jnp.zeros_like(rz)
    rs[...] = jnp.zeros_like(rs)

    barrier = pltpu.get_barrier_semaphore()

    def greet(i, carry):
        pl.semaphore_signal(barrier, inc=1, device_id=(v, lax.rem(p + i, pencils)), device_id_type=MESH_ID)
        return carry

    lax.fori_loop(1, pencils, greet, 0)

    def greet_far(i, carry):
        pl.semaphore_signal(barrier, inc=1, device_id=(far, lax.rem(p + i, pencils)), device_id_type=MESH_ID)
        return carry

    lax.fori_loop(0, pencils, greet_far, 0)
    for other in (mate, lax.rem(mate + 2, 4)):
        pl.semaphore_signal(barrier, inc=1, device_id=(other, p), device_id_type=MESH_ID)
    corners = [side for side in SIDES if side[0] != 0 and side[1] != 0]

    def greet_corner(side):
        pl.semaphore_signal(barrier, inc=1, device_id=(v + side[0], p + side[1]), device_id_type=MESH_ID)

    each(corners, greet_corner)
    expected = 2 * pencils + 1 + sum(exists(side).astype(jnp.int32) for side in corners)

    slab_load.wait()
    loads[2].wait()
    loads[3].wait()
    for z in range(4):
        xh[z], xl[z] = halves(left3(slab[z], dxh[...], dxl[...]))
    mid[...] = jnp.zeros_like(mid)
    for load in weight_loads + loads[:2]:
        load.wait()

    def remote(src, dst, k, device):
        return pltpu.make_async_remote_copy(
            src_ref=src, dst_ref=dst, send_sem=ssem.at[k], recv_sem=rsem.at[k],
            device_id=device, device_id_type=MESH_ID)

    lane0 = lax.broadcasted_iota(jnp.int32, (n, 128), 1) == 0

    for j in range(4):
        receiver = mirror0 if j == 0 else mirror
        pick = lane0 & (receiver < half)
        wsend[j] = jnp.where(pick, weight_rows(0, j), weight_rows(1, j))

    pl.semaphore_wait(barrier, expected)
    w_rest = remote(wsend.at[pl.ds(1, 3)], wgot.at[pl.ds(1, 3)], 1, (v, mirror))
    w_first = remote(wsend.at[0], wgot.at[0], 2, (v, mirror0))
    w_local = pltpu.make_async_copy(wsend.at[0], wgot.at[0], lsem.at[0])
    w_rest.start()

    @pl.when(jnp.logical_not(own_mirror))
    def _():
        w_first.start()

    @pl.when(own_mirror)
    def _():
        w_local.start()

    lane_q = lax.broadcasted_iota(jnp.int32, (q, 128), 1) == 0
    row_q = lax.broadcasted_iota(jnp.int32, (q, 128), 0)

    group = pencils // 4
    for step in range(4):
        b = lax.rem(p // group + step, 4)
        first = b < 2
        for z in range(4):
            both = (dot(csh[b], xh[z]) + (dot(csh[b], xl[z]) + dot(csl[b], xh[z])))
            c_re, c_im = both[:q, :128], both[:q, 128:]
            s_re, s_im = both[q:, :128], both[q:, 128:]
            re, im = c_re + s_im, c_im - s_re
            re0 = jnp.where(first, c_re, c_im)
            im0 = jnp.where(first, -s_re, -s_im)
            im0 = jnp.where((row_q == 0) & (b == 0), c_im, im0)
            im0 = jnp.where((row_q == 0) & (b == 2), c_re, im0)
            at = pl.multiple_of(b * (q * 8), q * 8)
            msg[pl.ds(at + z, q, stride=8), :] = jnp.where(lane_q, re0, re)
            msg[pl.ds(at + 4 + z, q, stride=8), :] = jnp.where(lane_q, im0, im)

        def send_chunk(i, carry, b=b):
            peer = b * group + lax.rem(p + i, group)
            at = pl.multiple_of(peer * 32, 32)

            @pl.when(peer != p)
            def _():
                remote(msg.at[pl.ds(at, 32)], got.at[p], 0, (v, peer)).start()
            return carry

        lax.fori_loop(0, group, send_chunk, 0)

    own = pltpu.make_async_copy(msg.at[pl.ds(pl.multiple_of(p * 32, 32), 32)], got.at[p], lsem.at[1])
    own.start()

    def quarter_of(view):
        return slab.at[:, pl.ds(pl.multiple_of(view * q, q), q), :]

    shares = [pltpu.make_async_remote_copy(
        src_ref=quarter_of(lax.rem(v + d, views)), dst_ref=stacked.at[v],
        send_sem=share_sem.at[0, d - 1], recv_sem=share_sem.at[1, d - 1],
        device_id=(lax.rem(v + d, views), p), device_id_type=MESH_ID) for d in range(1, 4)]
    for share in shares:
        share.start()
    own_share = pltpu.make_async_copy(quarter_of(v), stacked.at[v], lsem.at[3])
    own_share.start()

    for load in loads[4:]:
        load.wait()
    mth[...] = mh[...].astype(F32).T.astype(BF16)
    mtl[...] = ml[...].astype(F32).T.astype(BF16)
    def band(v, carry):
        at = (lax.broadcasted_iota(jnp.int32, (width, width), 0)
              - lax.broadcasted_iota(jnp.int32, (width, width), 1))
        table, turned = jnp.zeros((width, width), F32), jnp.zeros((width, width), F32)
        for t in range(9):
            tap = taps[v, 2, t]
            table = jnp.where(at == t - 4, tap, table)
            turned = jnp.where(at == 4 - t, tap, turned)
        th[v], tl[v] = halves(table)
        ah[v], al[v] = halves(turned)
        return carry

    lax.fori_loop(0, views, band, 0)

    w_rest.wait_recv()

    @pl.when(jnp.logical_not(own_mirror))
    def _():
        w_first.wait_recv()

    @pl.when(own_mirror)
    def _():
        w_local.wait()

    turn_z, turn_x = reversal(n), reversal(128)
    for j in range(4):
        mine = jnp.where(lane0 & (p >= half), weight_rows(1, j), weight_rows(0, j))
        turned = moved_left(turn_z, moved_right(wgot[(4 - j) % 4], turn_x))
        we[j] = 0.5 * (mine + turned)

    @pl.when(own_mirror)
    def _():
        first = (lax.broadcasted_iota(jnp.int32, (n, 128), 0) * 0 + p) == 0
        other = jnp.where(first, weight_rows(1, 0), weight_rows(0, 0))
        other = 0.5 * (other + moved_left(turn_z, other))
        main = we[0]
        we[0] = jnp.where(lane0, 0.5 * (main + other), main)
        wm[...] = jnp.where(lane0, 0.5 * (main - other), 0.0)

    own.wait()
    remote(got.at[pl.ds(0, pencils - 1)], got.at[pl.ds(0, pencils - 1)], 0, (v, mirror)).wait_recv()

    def tile_rows(j):
        return got[:, 8 * j:8 * j + 8, :].reshape(2 * n, 128)

    for pair in range(2):
        f = right3(mh[...], ml[...], jnp.concatenate([tile_rows(2 * pair), tile_rows(2 * pair + 1)], axis=1))
        for k in range(2):
            j = 2 * pair + k
            for part in range(2):
                g[j, part * n:(part + 1) * n, :] = (
                    f[part * n:(part + 1) * n, 128 * k:128 * k + 128] * we[j])

    @pl.when(own_mirror)
    def _():
        imag = lax.rem(lax.broadcasted_iota(jnp.int32, (2 * n, 128), 0), 8) >= 4
        rows = tile_rows(0)
        f = right3(mh[...], ml[...], jnp.where(imag, -rows, rows))
        for part in range(2):
            g[0, part * n:(part + 1) * n, :] = (
                g[0, part * n:(part + 1) * n, :] + f[part * n:(part + 1) * n, :] * wm[...])

    pair_sum = remote(g.at[pl.ds(2 - 2 * core, 2)], gr, 3, (mate, p))
    pair_sum.start()
    pair_sum.wait_recv()
    f = right3(mth[...], mtl[...], jnp.concatenate(
        [g[2 * core] + gr[0], g[2 * core + 1] + gr[1]], axis=1))
    kept = v // 2
    away = 1 - kept
    for k in range(2):
        fs[k] = f[:, 128 * k:128 * k + 128]
    for x in range(2):
        for k in range(2):
            for part in range(2):
                for zz in range(2):
                    gm[x, pl.ds(4 * k + 2 * part + zz, pencils, stride=8), :] = (
                        fs[k, pl.ds(4 * part + 2 * x + zz, pencils, stride=8), :])

    def rows_of(peer):
        return pl.ds(pl.multiple_of(peer * 8, 8), 8)

    def send_back(i, carry):
        peer = lax.rem(p + i, pencils)

        @pl.when(i > 0)
        def _():
            remote(gm.at[kept, rows_of(peer)], fr.at[kept, rows_of(p)], 4, (v, peer)).start()

        remote(gm.at[away, rows_of(peer)], fr.at[kept, rows_of(p)], 7, (far, peer)).start()
        return carry

    lax.fori_loop(0, pencils, send_back, 0)
    own_back = pltpu.make_async_copy(gm.at[kept, rows_of(p)], fr.at[kept, rows_of(p)], lsem.at[2])
    own_back.start()
    own_back.wait()
    most = fr.at[kept, pl.ds(0, 8 * (pencils - 1))]
    remote(most, most, 4, (v, mirror)).wait_recv()
    remote(fr.at[away], fr.at[away], 7, (far, p)).wait_recv()

    m = lax.broadcasted_iota(jnp.int32, (n // 2, 128), 0)
    ky = m // 2 * 4 + 2 * core + lax.rem(m, 2)
    lane_m = lax.broadcasted_iota(jnp.int32, (n // 2, 128), 1) == 0
    low, high = (ky > 0) & (ky < n // 2), ky > n // 2
    for zz in range(2):
        re = fr[0, pl.ds(zz, n // 2, stride=4), :] + fr[1, pl.ds(zz, n // 2, stride=4), :]
        im = fr[0, pl.ds(2 + zz, n // 2, stride=4), :] + fr[1, pl.ds(2 + zz, n // 2, stride=4), :]
        zero = jnp.zeros_like(re)
        v1 = jnp.where(low, 2.0 * re, jnp.where(ky == 0, re, jnp.where(ky == n // 2, im, zero)))
        v2 = jnp.where(high, 2.0 * re, jnp.where(ky == 0, im, jnp.where(ky == n // 2, re, zero)))
        b1 = jnp.where(low, -2.0 * im, zero)
        b2 = jnp.where(high, -2.0 * im, zero)
        top = jnp.concatenate([jnp.where(lane_m, v1, re), jnp.where(lane_m, v2, im)], axis=1)
        bottom = jnp.concatenate([jnp.where(lane_m, b1, -im), jnp.where(lane_m, b2, re)], axis=1)
        u = right3(cyh[core], cyl[core], jnp.concatenate([top, bottom], axis=0))
        field = left3(u, dih[...], dil[...])
        for quarter in range(4):
            pj[quarter // 2, quarter % 2, zz] = field[quarter * q:(quarter + 1) * q]

    near = remote(pj.at[:, 1 - core], r1, 5, (mate, p))
    near.start()
    near.wait_recv()
    r1[...] = r1[...] + pj[:, core]
    long = remote(r1.at[away], r2, 6, (far, p))
    long.start()
    long.wait_recv()
    out[pl.ds(2 * kept, 2)] = r1[kept]
    out[pl.ds(2 * away, 2)] = r2[...]


    planes_of = {-1: pl.ds(0, depth), 0: pl.ds(depth, depth), 1: pl.ds(2 * depth, depth)}

    def est_copy(side):
        dv, dp = side
        src_rows = {0: pl.ds(8, rows), 1: pl.ds(rows, 8), -1: pl.ds(8, 8)}[dv]
        dst_rows = {0: pl.ds(8, rows), 1: pl.ds(0, 8), -1: pl.ds(rows + 8, 8)}[dv]
        return pltpu.make_async_remote_copy(
            src_ref=est.at[planes_of[0], :, src_rows, :],
            dst_ref=est.at[planes_of[-dp], :, dst_rows, :],
            send_sem=send_sem.at[0, SLOT[side]],
            recv_sem=recv_sem.at[0, SLOT[back(side)]],
            device_id=(v + dv, p + dp),
            device_id_type=MESH_ID,
        )

    def acc_copy(side):
        dv, dp = side
        src_rows = {0: pl.ds(8, rows), 1: pl.ds(rows + 8, 8), -1: pl.ds(0, 8)}[dv]
        slot = SLOT[back(side)]
        landing = rz.at[0 if dp == 1 else 1] if dv == 0 else rs.at[slot]
        return pltpu.make_async_remote_copy(
            src_ref=acc.at[planes_of[dp], :, src_rows, :],
            dst_ref=landing,
            send_sem=send_sem.at[1, SLOT[side]],
            recv_sem=recv_sem.at[1, slot],
            device_id=(v + dv, p + dp),
            device_id_type=MESH_ID,
        )

    def est_wait(side):
        dv, dp = side
        dst_rows = {0: pl.ds(8, rows), -1: pl.ds(0, 8), 1: pl.ds(rows + 8, 8)}[dv]
        landing = est.at[planes_of[dp], :, dst_rows, :]
        pltpu.make_async_remote_copy(
            src_ref=landing, dst_ref=landing, send_sem=send_sem.at[0, SLOT[side]],
            recv_sem=recv_sem.at[0, SLOT[side]], device_id=(v + dv, p + dp),
            device_id_type=MESH_ID).wait_recv()

    def acc_wait(side):
        dv, dp = side
        landing = rz.at[0 if dp == -1 else 1] if dv == 0 else rs.at[SLOT[side]]
        pltpu.make_async_remote_copy(
            src_ref=landing, dst_ref=landing, send_sem=send_sem.at[1, SLOT[side]],
            recv_sem=recv_sem.at[1, SLOT[side]], device_id=(v + dv, p + dp),
            device_id_type=MESH_ID).wait_recv()

    for h in range(2):
        s = out[:, :, h * 128:(h + 1) * 128]
        est[pl.ds(depth, depth), h, pl.ds(8, rows), :] = 0.1 + (
            jnp.maximum(s, 0.0) + jnp.log1p(jnp.exp(-jnp.abs(s))))

    each(SIDES, lambda side: est_copy(side).start())
    own_share.wait()
    for share in shares:
        share.wait_recv()

    def view_step(w, carry):
        for z in range(depth):
            total = taps[w, 0, 0] * est[z]
            for t in range(1, 9):
                total = total + taps[w, 0, t] * est[z + t]
            zed[w, z] = total
        sides = []
        for h in range(2):
            planes = []
            for z in range(depth):
                total = taps[w, 1, 0] * zed[w, z, h, pl.ds(4, rows), :]
                for t in range(1, 9):
                    total = total + taps[w, 1, t] * zed[w, z, h, pl.ds(4 + t, rows), :]
                planes.append(total)
            sides.append(jnp.concatenate(planes, axis=0))
        blurred = dot3(jnp.concatenate(sides, axis=1), th[w], tl[w])
        ratio = stacked[w].reshape(depth * rows, width) / blurred
        turned = dot3(ratio, ah[w], al[w])
        for z in range(depth):
            for h in range(2):
                mid[w, z, h, pl.ds(16, rows), :] = turned[z * rows:(z + 1) * rows, h * 128:(h + 1) * 128]
        for z in range(depth):
            for h in range(2):
                total = taps[w, 1, 8] * mid[w, z, h, pl.ds(4, frame), :]
                for t in range(1, 9):
                    total = total + taps[w, 1, 8 - t] * mid[w, z, h, pl.ds(4 + t, frame), :]
                spread[w, z, h] = total
        return carry

    def gather_planes(planes):
        for zo in planes:
            total = None
            for v in range(views):
                for zs in range(depth):
                    if 0 <= zo - zs <= 8:
                        term = taps[v, 0, zo - zs] * spread[v, zs]
                        total = term if total is None else total + term
            acc[zo] = total

    def iteration(step, carry):
        each(SIDES, est_wait)
        lax.fori_loop(0, views, view_step, 0, unroll=UNROLL)
        gather_planes(list(range(0, depth)) + list(range(2 * depth, 3 * depth)))
        each([s for s in SIDES if s[1] != 0], lambda side: acc_copy(side).start())
        gather_planes(range(depth, 2 * depth))
        each([s for s in SIDES if s[1] == 0], lambda side: acc_copy(side).start())
        each(SIDES, lambda side: est_copy(side).wait_send())
        each(SIDES, acc_wait)
        for z in range(depth):
            for h in range(2):
                total = acc[depth + z, h, pl.ds(8, rows), :] + (rz[0, z, h] + rz[1, z, h])
                low = rs[SLOT[(-1, 0)], z, h] + (rs[SLOT[(-1, -1)], z, h] + rs[SLOT[(-1, 1)], z, h])
                high = rs[SLOT[(1, 0)], z, h] + (rs[SLOT[(1, -1)], z, h] + rs[SLOT[(1, 1)], z, h])
                total = jnp.concatenate(
                    [total[:8] + low, total[8:rows - 8], total[rows - 8:] + high], axis=0)
                fresh = est[depth + z, h, pl.ds(8, rows), :] * (total * (1.0 / views))
                est[depth + z, h, pl.ds(8, rows), :] = fresh
        each(SIDES, lambda side: acc_copy(side).wait_send())

        @pl.when(step < ITERS - 1)
        def _():
            each(SIDES, lambda side: est_copy(side).start())
        return carry

    lax.fori_loop(0, ITERS, iteration, 0)
    for h in range(2):
        out2[:, :, h * 128:(h + 1) * 128] = est[pl.ds(depth, depth), h, pl.ds(8, rows), :]

    w_rest.wait_send()
    sent = msg.at[pl.ds(0, 32 * (pencils - 1))]
    remote(sent, sent, 0, (v, mirror)).wait_send()
    pair_sum.wait_send()
    sent_back = gm.at[kept, pl.ds(0, 8 * (pencils - 1))]
    remote(sent_back, sent_back, 4, (v, mirror)).wait_send()
    remote(gm.at[away], gm.at[away], 7, (far, p)).wait_send()
    near.wait_send()
    long.wait_send()

    @pl.when(jnp.logical_not(own_mirror))
    def _():
        w_first.wait_send()
    for share in shares:
        share.wait_send()


def whole(recorded, weight, taps):
    views, pencils = lax.axis_size("view"), lax.axis_size("pencil")
    n, nx = 4 * pencils, recorded.shape[-1]
    q, depth = n // 4, 4
    frame = q + 16
    vmem, left = pl.BlockSpec(memory_space=pltpu.VMEM), pl.BlockSpec(memory_space=pltpu.HBM)
    tables = [jnp.asarray(t) for t in transform_tables(n, nx)]
    block = jax.ShapeDtypeStruct((depth, q, nx), F32)
    return pl.pallas_call(
        functools.partial(kernel, views, pencils),
        name="join_and_deconvolve",
        out_shape=(block, block),
        in_specs=[pl.BlockSpec(memory_space=pltpu.SMEM)] + [left] * (2 + len(tables)),
        out_specs=(vmem, vmem),
        scratch_shapes=[
            pltpu.VMEM((4, n, nx), F32),
            pltpu.VMEM((2, n, 4, 128), F32),
            *[pltpu.VMEM(t.shape, t.dtype) for t in tables],
            pltpu.VMEM((4, n, nx), BF16),
            pltpu.VMEM((4, n, nx), BF16),
            pltpu.VMEM((8 * n, 128), F32),
            pltpu.VMEM((pencils, 32, 128), F32),
            pltpu.VMEM((4, n, 128), F32),
            pltpu.VMEM((4, n, 128), F32),
            pltpu.VMEM((4, n, 128), F32),
            pltpu.VMEM((n, 128), F32),
            pltpu.VMEM((2 * n, 2 * n), BF16),
            pltpu.VMEM((2 * n, 2 * n), BF16),
            pltpu.VMEM((4, 2 * n, 128), F32),
            pltpu.VMEM((2, 2 * n, 128), F32),
            pltpu.VMEM((2, 2 * n, 128), F32),
            pltpu.VMEM((2, 8 * pencils, 128), F32),
            pltpu.VMEM((2, 8 * pencils, 128), F32),
            pltpu.VMEM((2, 2, 2, q, nx), F32),
            pltpu.VMEM((2, 2, q, nx), F32),
            pltpu.VMEM((2, q, nx), F32),
            pltpu.VMEM((views, depth, q, nx), F32),
            pltpu.VMEM((3 * depth, 2, frame, 128), F32),
            pltpu.VMEM((views, depth, 2, frame, 128), F32),
            pltpu.VMEM((views, depth, 2, frame + 16, 128), F32),
            pltpu.VMEM((views, depth, 2, frame, 128), F32),
            pltpu.VMEM((3 * depth, 2, frame, 128), F32),
            pltpu.VMEM((2, depth, 2, q, 128), F32),
            pltpu.VMEM((8, depth, 2, 8, 128), F32),
            *[pltpu.VMEM((views, nx, nx), BF16)] * 4,
            pltpu.SemaphoreType.DMA((8,)),
            pltpu.SemaphoreType.DMA((8,)),
            pltpu.SemaphoreType.DMA((4,)),
            pltpu.SemaphoreType.DMA((13,)),
            pltpu.SemaphoreType.DMA((2, 3)),
            pltpu.SemaphoreType.DMA((2, 8)),
            pltpu.SemaphoreType.DMA((2, 8)),
        ],
        compiler_params=pltpu.CompilerParams(collective_id=1, has_side_effects=True,
                                             vmem_limit_bytes=60 * 1024 * 1024),
    )(taps, recorded, weight, *tables)


def body(recorded, spectral_weight, psf_taps):
    kernels = psf_taps / jnp.sum(psf_taps, axis=-1, keepdims=True)
    return whole(recorded[0], spectral_weight[0], kernels)


def solution(mesh):
    return jax.shard_map(
        body,
        mesh=mesh,
        in_specs=(P("view", "pencil", None, None), P("view", None, "pencil", None), P()),
        out_specs=(P("pencil", "view", None), P("pencil", "view", None)),
        check_vma=False,
    )
```

```python
import functools

import jax
import jax.numpy as jnp
import numpy as np
from jax import lax
from jax.experimental import pallas as pl
from jax.experimental.pallas import tpu as pltpu
from jax.sharding import PartitionSpec as P

ITERS = 2
UNROLL = 4
MESH_ID = pl.DeviceIdType.MESH
F32 = jnp.float32
BF16 = jnp.bfloat16
SIDES = [(dv, dp) for dp in (-1, 1, 0) for dv in (0, -1, 1) if (dv, dp) != (0, 0)]
SLOT = {side: k for k, side in enumerate(SIDES)}


def halves(value):
    high = value.astype(BF16)
    return high, (value - high.astype(F32)).astype(BF16)


def dot(left, right):
    return jnp.dot(left, right, preferred_element_type=F32)


def two_terms(table):
    high = table.astype(jnp.bfloat16)
    low = (table - high.astype(np.float64)).astype(jnp.bfloat16)
    return [high, low]


def transform_tables(n, nx):
    at = np.arange(n)
    phase = 2.0 * np.pi * (at[:, None] * at[None, :] % n) / n
    cosine, sine = np.cos(phase), np.sin(phase)
    q = n // 4
    rows = np.concatenate([cosine.reshape(4, q, n), sine.reshape(4, q, n)], axis=1)

    x, c = np.arange(nx)[:, None], np.arange(nx // 2)[None, :]
    wave = 2.0 * np.pi * (x * c % nx) / nx
    sign = np.where(x % 2 == 0, 1.0, -1.0)
    columns = np.concatenate([np.cos(wave), np.where(c == 0, sign, -np.sin(wave))], axis=1)
    scale = 1.0 / (float(n) * n * nx)
    back_re = np.where(c == 0, 1.0, 2.0 * np.cos(wave)).T
    back_im = np.where(c == 0, sign, -2.0 * np.sin(wave)).T
    columns_back = np.concatenate([back_re, back_im], axis=0) * scale

    index = np.arange(2 * n)
    part, depth = index % 8 // 4, index // 8 * 4 + index % 4
    c_z, s_z = cosine[:, depth], sine[:, depth]
    depth_table = np.concatenate(
        [np.where(part == 0, c_z, s_z), np.where(part == 0, -s_z, c_z)], axis=0)

    m = np.arange(n // 2)
    back = []
    for core in range(2):
        ky = m // 2 * 4 + 2 * core + m % 2
        back.append(np.concatenate([cosine[:, ky], sine[:, ky]], axis=1))
    return [t for table in (rows, columns, depth_table, np.stack(back), columns_back)
            for t in two_terms(table)]


def right3(high, low, right):
    r_high, r_low = halves(right)
    return dot(high, r_high) + (dot(high, r_low) + dot(low, r_high))


def left3(left, high, low):
    l_high, l_low = halves(left)
    return dot(l_high, high) + (dot(l_high, low) + dot(l_low, high))


def reversal(n):
    total = lax.broadcasted_iota(jnp.int32, (n, n), 0) + lax.broadcasted_iota(jnp.int32, (n, n), 1)
    return jnp.where((total == 0) | (total == n), 1.0, 0.0).astype(BF16)


def moved_right(value, table):
    high, low = halves(value)
    return dot(high, table) + dot(low, table)


def moved_left(table, value):
    high, low = halves(value)
    return dot(table, high) + dot(table, low)


def dot3(left, right_high, right_low):
    high, low = halves(left)
    return dot(high, right_high) + (dot(high, right_low) + dot(low, right_high))


def kernel(views, pencils, taps, slab_ref, weight_ref, *refs):
    table_refs, refs = refs[:10], refs[10:]
    (out, out2, slab, weight, csh, csl, dxh, dxl, mh, ml, cyh, cyl, dih, dil,
     xh, xl, msg, got, wsend, wgot, we, wm, mth, mtl, g, gr, gsh, gsl, fs, gm, fr, pj, r1, r2,
     stacked, est, zed, mid, spread, acc, rz, rs, th, tl, ah, al,
     ssem, rsem, lsem, load_sem, share_sem, send_sem, recv_sem) = refs
    n = 4 * pencils
    q = n // 4
    half = pencils // 2
    v, p = lax.axis_index("view"), lax.axis_index("pencil")
    core = lax.rem(v, 2)
    mate = v + 1 - 2 * core
    far = lax.rem(v + 2, 4)
    mirror = pencils - 1 - p
    mirror0 = lax.rem(pencils - p, pencils)
    own_mirror = (p == 0) | (p == half)

    tables = [csh, csl, dxh, dxl, mh, ml, cyh, cyl, dih, dil]
    loads = [pltpu.make_async_copy(src, dst, load_sem.at[k])
             for k, (src, dst) in enumerate(zip(table_refs, tables))]
    slab_load = pltpu.make_async_copy(slab_ref, slab, load_sem.at[10])
    weight_loads = [pltpu.make_async_copy(weight_ref.at[:, :, pl.ds(128 * h, 128)], weight.at[h], load_sem.at[11 + h])
                    for h in range(2)]
    slab_load.start()
    for load in loads[2:4] + weight_loads + loads[:2] + loads[4:]:
        load.start()
    flat = [weight.at[h].reshape(4 * n, 128) for h in range(2)]

    def weight_rows(h, j):
        return flat[h][pl.ds(j, n, stride=4), :]

    depth, rows, width = 4, q, slab.shape[-1]
    frame = rows + 16

    def exists(side):
        v1, p1 = v + side[0], p + side[1]
        return (v1 >= 0) & (v1 < views) & (p1 >= 0) & (p1 < pencils)

    def back(side):
        return (-side[0], -side[1])

    def each(sides, action):
        for side in sides:
            @pl.when(exists(side))
            def _(side=side):
                action(side)

    est[...] = jnp.zeros_like(est)
    rz[...] = jnp.zeros_like(rz)
    rs[...] = jnp.zeros_like(rs)

    barrier = pltpu.get_barrier_semaphore()

    def greet(i, carry):
        pl.semaphore_signal(barrier, inc=1, device_id=(v, lax.rem(p + i, pencils)), device_id_type=MESH_ID)
        return carry

    lax.fori_loop(1, pencils, greet, 0)

    def greet_far(i, carry):
        pl.semaphore_signal(barrier, inc=1, device_id=(far, lax.rem(p + i, pencils)), device_id_type=MESH_ID)
        return carry

    lax.fori_loop(0, pencils, greet_far, 0)
    for other in (mate, lax.rem(mate + 2, 4)):
        pl.semaphore_signal(barrier, inc=1, device_id=(other, p), device_id_type=MESH_ID)
    corners = [side for side in SIDES if side[0] != 0 and side[1] != 0]

    def greet_corner(side):
        pl.semaphore_signal(barrier, inc=1, device_id=(v + side[0], p + side[1]), device_id_type=MESH_ID)

    each(corners, greet_corner)
    expected = 2 * pencils + 1 + sum(exists(side).astype(jnp.int32) for side in corners)

    slab_load.wait()
    loads[2].wait()
    loads[3].wait()
    for z in range(4):
        xh[z], xl[z] = halves(left3(slab[z], dxh[...], dxl[...]))
    mid[...] = jnp.zeros_like(mid)
    for load in weight_loads + loads[:2]:
        load.wait()

    def remote(src, dst, k, device):
        return pltpu.make_async_remote_copy(
            src_ref=src, dst_ref=dst, send_sem=ssem.at[k], recv_sem=rsem.at[k],
            device_id=device, device_id_type=MESH_ID)

    lane0 = lax.broadcasted_iota(jnp.int32, (n, 128), 1) == 0

    for j in range(4):
        receiver = mirror0 if j == 0 else mirror
        pick = lane0 & (receiver < half)
        wsend[j] = jnp.where(pick, weight_rows(0, j), weight_rows(1, j))

    pl.semaphore_wait(barrier, expected)
    w_rest = remote(wsend.at[pl.ds(1, 3)], wgot.at[pl.ds(1, 3)], 1, (v, mirror))
    w_first = remote(wsend.at[0], wgot.at[0], 2, (v, mirror0))
    w_local = pltpu.make_async_copy(wsend.at[0], wgot.at[0], lsem.at[0])
    w_rest.start()

    @pl.when(jnp.logical_not(own_mirror))
    def _():
        w_first.start()

    @pl.when(own_mirror)
    def _():
        w_local.start()

    lane_q = lax.broadcasted_iota(jnp.int32, (q, 128), 1) == 0
    row_q = lax.broadcasted_iota(jnp.int32, (q, 128), 0)

    group = pencils // 4
    for step in range(4):
        b = lax.rem(p // group + step, 4)
        first = b < 2
        for z in range(4):
            both = (dot(csh[b], xh[z]) + (dot(csh[b], xl[z]) + dot(csl[b], xh[z])))
            c_re, c_im = both[:q, :128], both[:q, 128:]
            s_re, s_im = both[q:, :128], both[q:, 128:]
            re, im = c_re + s_im, c_im - s_re
            re0 = jnp.where(first, c_re, c_im)
            im0 = jnp.where(first, -s_re, -s_im)
            im0 = jnp.where((row_q == 0) & (b == 0), c_im, im0)
            im0 = jnp.where((row_q == 0) & (b == 2), c_re, im0)
            at = pl.multiple_of(b * (q * 8), q * 8)
            msg[pl.ds(at + z, q, stride=8), :] = jnp.where(lane_q, re0, re)
            msg[pl.ds(at + 4 + z, q, stride=8), :] = jnp.where(lane_q, im0, im)

        def send_chunk(i, carry, b=b):
            peer = b * group + lax.rem(p + i, group)
            at = pl.multiple_of(peer * 32, 32)

            @pl.when(peer != p)
            def _():
                remote(msg.at[pl.ds(at, 32)], got.at[p], 0, (v, peer)).start()
            return carry

        lax.fori_loop(0, group, send_chunk, 0)

    own = pltpu.make_async_copy(msg.at[pl.ds(pl.multiple_of(p * 32, 32), 32)], got.at[p], lsem.at[1])
    own.start()

    def quarter_of(view):
        return slab.at[:, pl.ds(pl.multiple_of(view * q, q), q), :]

    shares = [pltpu.make_async_remote_copy(
        src_ref=quarter_of(lax.rem(v + d, views)), dst_ref=stacked.at[v],
        send_sem=share_sem.at[0, d - 1], recv_sem=share_sem.at[1, d - 1],
        device_id=(lax.rem(v + d, views), p), device_id_type=MESH_ID) for d in range(1, 4)]
    for share in shares:
        share.start()
    own_share = pltpu.make_async_copy(quarter_of(v), stacked.at[v], lsem.at[3])
    own_share.start()

    for load in loads[4:]:
        load.wait()
    mth[...] = mh[...].astype(F32).T.astype(BF16)
    mtl[...] = ml[...].astype(F32).T.astype(BF16)
    def band(v, carry):
        at = (lax.broadcasted_iota(jnp.int32, (width, width), 0)
              - lax.broadcasted_iota(jnp.int32, (width, width), 1))
        table, turned = jnp.zeros((width, width), F32), jnp.zeros((width, width), F32)
        for t in range(9):
            tap = taps[v, 2, t]
            table = jnp.where(at == t - 4, tap, table)
            turned = jnp.where(at == 4 - t, tap, turned)
        whole_sum = 1.0
        for axis in range(3):
            axis_sum = taps[v, axis, 0]
            for t in range(1, 9):
                axis_sum = axis_sum + taps[v, axis, t]
            whole_sum = whole_sum * axis_sum
        th[v], tl[v] = halves(table / whole_sum)
        ah[v], al[v] = halves(turned / whole_sum)
        return carry

    lax.fori_loop(0, views, band, 0)

    w_rest.wait_recv()

    @pl.when(jnp.logical_not(own_mirror))
    def _():
        w_first.wait_recv()

    @pl.when(own_mirror)
    def _():
        w_local.wait()

    turn_z, turn_x = reversal(n), reversal(128)
    for j in range(4):
        mine = jnp.where(lane0 & (p >= half), weight_rows(1, j), weight_rows(0, j))
        turned = moved_left(turn_z, moved_right(wgot[(4 - j) % 4], turn_x))
        we[j] = 0.5 * (mine + turned)

    @pl.when(own_mirror)
    def _():
        first = (lax.broadcasted_iota(jnp.int32, (n, 128), 0) * 0 + p) == 0
        other = jnp.where(first, weight_rows(1, 0), weight_rows(0, 0))
        other = 0.5 * (other + moved_left(turn_z, other))
        main = we[0]
        we[0] = jnp.where(lane0, 0.5 * (main + other), main)
        wm[...] = jnp.where(lane0, 0.5 * (main - other), 0.0)

    own.wait()
    remote(got.at[pl.ds(0, pencils - 1)], got.at[pl.ds(0, pencils - 1)], 0, (v, mirror)).wait_recv()

    def pair_spectra(pair):
        block = got[:, pl.ds(pl.multiple_of(16 * pair, 16), 16), :]
        return [block[:, 8 * k:8 * k + 8, :].reshape(2 * n, 128) for k in range(2)]

    def weigh(pair):
        f = right3(mh[...], ml[...], jnp.concatenate(pair_spectra(pair), axis=1))
        for k in range(2):
            j = 2 * pair + k
            for part in range(2):
                g[j, part * n:(part + 1) * n, :] = (
                    f[part * n:(part + 1) * n, 128 * k:128 * k + 128] * we[j])

        @pl.when(own_mirror & (pair == 0))
        def _():
            imag = lax.rem(lax.broadcasted_iota(jnp.int32, (2 * n, 128), 0), 8) >= 4
            lines = got[:, 0:8, :].reshape(2 * n, 128)
            f = right3(mh[...], ml[...], jnp.where(imag, -lines, lines))
            for part in range(2):
                g[0, part * n:(part + 1) * n, :] = (
                    g[0, part * n:(part + 1) * n, :] + f[part * n:(part + 1) * n, :] * wm[...])

    weigh(1 - core)
    pair_sum = remote(g.at[pl.ds(2 - 2 * core, 2)], gr, 3, (mate, p))
    pair_sum.start()
    weigh(core)
    pair_sum.wait_recv()
    gsh[...], gsl[...] = halves(jnp.concatenate(
        [g[2 * core] + gr[0], g[2 * core + 1] + gr[1]], axis=1))

    kept = v // 2
    away = 1 - kept

    def rows_of(peer):
        return pl.ds(pl.multiple_of(peer * 8, 8), 8)

    for step in range(2):
        b = lax.rem(p // half + step, 2)
        at = pl.multiple_of(b * n, n)
        block = pl.ds(at, n)
        f = (dot(mth[block, :], gsh[...])
             + (dot(mth[block, :], gsl[...]) + dot(mtl[block, :], gsh[...])))
        for k in range(2):
            fs[k, block, :] = f[:, 128 * k:128 * k + 128]
        for x in range(2):
            for k in range(2):
                for part in range(2):
                    for zz in range(2):
                        gm[x, pl.ds(at + (4 * k + 2 * part + zz), half, stride=8), :] = (
                            fs[k, pl.ds(at + (4 * part + 2 * x + zz), half, stride=8), :])

        def send_back(i, carry, b=b):
            peer = b * half + lax.rem(p + i, half)

            @pl.when(peer != p)
            def _():
                remote(gm.at[kept, rows_of(peer)], fr.at[kept, rows_of(p)], 4, (v, peer)).start()

            remote(gm.at[away, rows_of(peer)], fr.at[kept, rows_of(p)], 7, (far, peer)).start()
            return carry

        lax.fori_loop(0, half, send_back, 0)

    own_back = pltpu.make_async_copy(gm.at[kept, rows_of(p)], fr.at[kept, rows_of(p)], lsem.at[2])
    own_back.start()
    own_back.wait()
    most = fr.at[kept, pl.ds(0, 8 * (pencils - 1))]
    remote(most, most, 4, (v, mirror)).wait_recv()
    remote(fr.at[away], fr.at[away], 7, (far, p)).wait_recv()

    m = lax.broadcasted_iota(jnp.int32, (n // 2, 128), 0)
    ky = m // 2 * 4 + 2 * core + lax.rem(m, 2)
    lane_m = lax.broadcasted_iota(jnp.int32, (n // 2, 128), 1) == 0
    low, high = (ky > 0) & (ky < n // 2), ky > n // 2
    for zz in range(2):
        re = fr[0, pl.ds(zz, n // 2, stride=4), :] + fr[1, pl.ds(zz, n // 2, stride=4), :]
        im = fr[0, pl.ds(2 + zz, n // 2, stride=4), :] + fr[1, pl.ds(2 + zz, n // 2, stride=4), :]
        zero = jnp.zeros_like(re)
        v1 = jnp.where(low, 2.0 * re, jnp.where(ky == 0, re, jnp.where(ky == n // 2, im, zero)))
        v2 = jnp.where(high, 2.0 * re, jnp.where(ky == 0, im, jnp.where(ky == n // 2, re, zero)))
        b1 = jnp.where(low, -2.0 * im, zero)
        b2 = jnp.where(high, -2.0 * im, zero)
        top = jnp.concatenate([jnp.where(lane_m, v1, re), jnp.where(lane_m, v2, im)], axis=1)
        bottom = jnp.concatenate([jnp.where(lane_m, b1, -im), jnp.where(lane_m, b2, re)], axis=1)
        u = right3(cyh[core], cyl[core], jnp.concatenate([top, bottom], axis=0))
        field = left3(u, dih[...], dil[...])
        for quarter in range(4):
            pj[quarter // 2, quarter % 2, zz] = field[quarter * q:(quarter + 1) * q]

    near = remote(pj.at[:, 1 - core], r1, 5, (mate, p))
    near.start()
    near.wait_recv()
    r1[...] = r1[...] + pj[:, core]
    long = remote(r1.at[away], r2, 6, (far, p))
    long.start()

    def est_copy(side, z):
        dv, dp = side
        src_rows = {0: pl.ds(8, rows), 1: pl.ds(rows, 8), -1: pl.ds(8, 8)}[dv]
        dst_rows = {0: pl.ds(8, rows), 1: pl.ds(0, 8), -1: pl.ds(rows + 8, 8)}[dv]
        return pltpu.make_async_remote_copy(
            src_ref=est.at[depth + z, :, src_rows, :],
            dst_ref=est.at[depth * (1 - dp) + z, :, dst_rows, :],
            send_sem=send_sem.at[0, SLOT[side], z],
            recv_sem=recv_sem.at[0, SLOT[back(side)], z],
            device_id=(v + dv, p + dp),
            device_id_type=MESH_ID,
        )

    def acc_copy(side, z):
        dv, dp = side
        src_rows = {0: pl.ds(8, rows), 1: pl.ds(rows + 8, 8), -1: pl.ds(0, 8)}[dv]
        slot = SLOT[back(side)]
        landing = rz.at[0 if dp == 1 else 1, z] if dv == 0 else rs.at[slot, z]
        return pltpu.make_async_remote_copy(
            src_ref=acc.at[depth * (1 + dp) + z, :, src_rows, :],
            dst_ref=landing,
            send_sem=send_sem.at[1, SLOT[side], z],
            recv_sem=recv_sem.at[1, slot, z],
            device_id=(v + dv, p + dp),
            device_id_type=MESH_ID,
        )

    def est_wait(side, z):
        dv, dp = side
        dst_rows = {0: pl.ds(8, rows), -1: pl.ds(0, 8), 1: pl.ds(rows + 8, 8)}[dv]
        landing = est.at[depth * (1 + dp) + z, :, dst_rows, :]
        pltpu.make_async_remote_copy(
            src_ref=landing, dst_ref=landing, send_sem=send_sem.at[0, SLOT[side], z],
            recv_sem=recv_sem.at[0, SLOT[side], z], device_id=(v + dv, p + dp),
            device_id_type=MESH_ID).wait_recv()

    def acc_wait(side, z):
        dv, dp = side
        landing = rz.at[0 if dp == -1 else 1, z] if dv == 0 else rs.at[SLOT[side], z]
        pltpu.make_async_remote_copy(
            src_ref=landing, dst_ref=landing, send_sem=send_sem.at[1, SLOT[side], z],
            recv_sem=recv_sem.at[1, SLOT[side], z], device_id=(v + dv, p + dp),
            device_id_type=MESH_ID).wait_recv()

    def every_plane(action):
        def at_plane(z, carry):
            each(SIDES, lambda side: action(side, z))
            return carry

        lax.fori_loop(0, depth, at_plane, 0)

    def start_estimate(first, planes):
        out[pl.ds(first, 2)] = planes
        for h in range(2):
            s = planes[:, :, h * 128:(h + 1) * 128]
            est[pl.ds(depth + first, 2), h, pl.ds(8, rows), :] = 0.1 + (
                jnp.maximum(s, 0.0) + jnp.log1p(jnp.exp(-jnp.abs(s))))
        for zz in range(2):
            each(SIDES, lambda side: est_copy(side, first + zz).start())

    start_estimate(2 * kept, r1[kept])
    long.wait_recv()
    start_estimate(2 * away, r2[...])
    own_share.wait()
    for share in shares:
        share.wait_recv()

    def view_step(w, carry):
        for z in range(depth):
            total = taps[w, 0, 0] * est[z]
            for t in range(1, 9):
                total = total + taps[w, 0, t] * est[z + t]
            zed[w, z] = total
        sides = []
        for h in range(2):
            planes = []
            for z in range(depth):
                total = taps[w, 1, 0] * zed[w, z, h, pl.ds(4, rows), :]
                for t in range(1, 9):
                    total = total + taps[w, 1, t] * zed[w, z, h, pl.ds(4 + t, rows), :]
                planes.append(total)
            sides.append(jnp.concatenate(planes, axis=0))
        blurred = dot3(jnp.concatenate(sides, axis=1), th[w], tl[w])
        ratio = stacked[w].reshape(depth * rows, width) / blurred
        turned = dot3(ratio, ah[w], al[w])
        for z in range(depth):
            for h in range(2):
                mid[w, z, h, pl.ds(16, rows), :] = turned[z * rows:(z + 1) * rows, h * 128:(h + 1) * 128]
        for z in range(depth):
            for h in range(2):
                total = taps[w, 1, 8] * mid[w, z, h, pl.ds(4, frame), :]
                for t in range(1, 9):
                    total = total + taps[w, 1, 8 - t] * mid[w, z, h, pl.ds(4 + t, frame), :]
                spread[w, z, h] = total
        return carry

    def gather_planes(planes):
        for zo in planes:
            total = None
            for v in range(views):
                for zs in range(depth):
                    if 0 <= zo - zs <= 8:
                        term = taps[v, 0, zo - zs] * spread[v, zs]
                        total = term if total is None else total + term
            acc[zo] = total

    def iteration(step, carry):
        every_plane(est_wait)
        lax.fori_loop(0, views, view_step, 0, unroll=UNROLL)
        for z in range(depth):
            gather_planes([z, 2 * depth + z, depth + z])
            each(SIDES, lambda side: acc_copy(side, z).start())

        def finish_plane(z, carry):
            each(SIDES, lambda side: acc_wait(side, z))
            each(SIDES, lambda side: est_copy(side, z).wait_send())
            for h in range(2):
                total = acc[depth + z, h, pl.ds(8, rows), :] + (rz[0, z, h] + rz[1, z, h])
                low = rs[SLOT[(-1, 0)], z, h] + (rs[SLOT[(-1, -1)], z, h] + rs[SLOT[(-1, 1)], z, h])
                high = rs[SLOT[(1, 0)], z, h] + (rs[SLOT[(1, -1)], z, h] + rs[SLOT[(1, 1)], z, h])
                total = jnp.concatenate(
                    [total[:8] + low, total[8:rows - 8], total[rows - 8:] + high], axis=0)
                est[depth + z, h, pl.ds(8, rows), :] = (
                    est[depth + z, h, pl.ds(8, rows), :] * (total * (1.0 / views)))

            @pl.when(step < ITERS - 1)
            def _():
                each(SIDES, lambda side: est_copy(side, z).start())
            return carry

        lax.fori_loop(0, depth, finish_plane, 0)
        every_plane(lambda side, z: acc_copy(side, z).wait_send())
        return carry

    lax.fori_loop(0, ITERS, iteration, 0)
    for h in range(2):
        out2[:, :, h * 128:(h + 1) * 128] = est[pl.ds(depth, depth), h, pl.ds(8, rows), :]

    w_rest.wait_send()
    sent = msg.at[pl.ds(0, 32 * (pencils - 1))]
    remote(sent, sent, 0, (v, mirror)).wait_send()
    pair_sum.wait_send()
    sent_back = gm.at[kept, pl.ds(0, 8 * (pencils - 1))]
    remote(sent_back, sent_back, 4, (v, mirror)).wait_send()
    remote(gm.at[away], gm.at[away], 7, (far, p)).wait_send()
    near.wait_send()
    long.wait_send()

    @pl.when(jnp.logical_not(own_mirror))
    def _():
        w_first.wait_send()
    for share in shares:
        share.wait_send()


def whole(recorded, weight, taps):
    views, pencils = lax.axis_size("view"), lax.axis_size("pencil")
    n, nx = 4 * pencils, recorded.shape[-1]
    q, depth = n // 4, 4
    frame = q + 16
    vmem, left = pl.BlockSpec(memory_space=pltpu.VMEM), pl.BlockSpec(memory_space=pltpu.HBM)
    tables = [jnp.asarray(t) for t in transform_tables(n, nx)]
    block = jax.ShapeDtypeStruct((depth, q, nx), F32)
    return pl.pallas_call(
        functools.partial(kernel, views, pencils),
        name="join_and_deconvolve",
        out_shape=(block, block),
        in_specs=[pl.BlockSpec(memory_space=pltpu.SMEM)] + [left] * (2 + len(tables)),
        out_specs=(vmem, vmem),
        scratch_shapes=[
            pltpu.VMEM((4, n, nx), F32),
            pltpu.VMEM((2, n, 4, 128), F32),
            *[pltpu.VMEM(t.shape, t.dtype) for t in tables],
            pltpu.VMEM((4, n, nx), BF16),
            pltpu.VMEM((4, n, nx), BF16),
            pltpu.VMEM((8 * n, 128), F32),
            pltpu.VMEM((pencils, 32, 128), F32),
            pltpu.VMEM((4, n, 128), F32),
            pltpu.VMEM((4, n, 128), F32),
            pltpu.VMEM((4, n, 128), F32),
            pltpu.VMEM((n, 128), F32),
            pltpu.VMEM((2 * n, 2 * n), BF16),
            pltpu.VMEM((2 * n, 2 * n), BF16),
            pltpu.VMEM((4, 2 * n, 128), F32),
            pltpu.VMEM((2, 2 * n, 128), F32),
            pltpu.VMEM((2 * n, 256), BF16),
            pltpu.VMEM((2 * n, 256), BF16),
            pltpu.VMEM((2, 2 * n, 128), F32),
            pltpu.VMEM((2, 8 * pencils, 128), F32),
            pltpu.VMEM((2, 8 * pencils, 128), F32),
            pltpu.VMEM((2, 2, 2, q, nx), F32),
            pltpu.VMEM((2, 2, q, nx), F32),
            pltpu.VMEM((2, q, nx), F32),
            pltpu.VMEM((views, depth, q, nx), F32),
            pltpu.VMEM((3 * depth, 2, frame, 128), F32),
            pltpu.VMEM((views, depth, 2, frame, 128), F32),
            pltpu.VMEM((views, depth, 2, frame + 16, 128), F32),
            pltpu.VMEM((views, depth, 2, frame, 128), F32),
            pltpu.VMEM((3 * depth, 2, frame, 128), F32),
            pltpu.VMEM((2, depth, 2, q, 128), F32),
            pltpu.VMEM((8, depth, 2, 8, 128), F32),
            *[pltpu.VMEM((views, nx, nx), BF16)] * 4,
            pltpu.SemaphoreType.DMA((8,)),
            pltpu.SemaphoreType.DMA((8,)),
            pltpu.SemaphoreType.DMA((4,)),
            pltpu.SemaphoreType.DMA((13,)),
            pltpu.SemaphoreType.DMA((2, 3)),
            pltpu.SemaphoreType.DMA((2, 8, 4)),
            pltpu.SemaphoreType.DMA((2, 8, 4)),
        ],
        compiler_params=pltpu.CompilerParams(collective_id=1, has_side_effects=True,
                                             vmem_limit_bytes=60 * 1024 * 1024),
    )(taps, recorded, weight, *tables)


def body(recorded, spectral_weight, psf_taps):
    return whole(recorded[0], spectral_weight[0], psf_taps)


def solution(mesh):
    return jax.shard_map(
        body,
        mesh=mesh,
        in_specs=(P("view", "pencil", None, None), P("view", None, "pencil", None), P()),
        out_specs=(P("pencil", "view", None), P("pencil", "view", None)),
        check_vma=False,
    )
```

```python
import functools

import jax
import jax.numpy as jnp
import numpy as np
from jax import lax
from jax.experimental import pallas as pl
from jax.experimental.pallas import tpu as pltpu
from jax.sharding import PartitionSpec as P

ITERS = 2
UNROLL = 4
MESH_ID = pl.DeviceIdType.MESH
F32 = jnp.float32
BF16 = jnp.bfloat16
SIDES = [(dv, dp) for dp in (-1, 1, 0) for dv in (0, -1, 1) if (dv, dp) != (0, 0)]
SLOT = {side: k for k, side in enumerate(SIDES)}


def halves(value):
    high = value.astype(BF16)
    return high, (value - high.astype(F32)).astype(BF16)


def dot(left, right):
    return jnp.dot(left, right, preferred_element_type=F32)


def two_terms(table):
    high = table.astype(jnp.bfloat16)
    low = (table - high.astype(np.float64)).astype(jnp.bfloat16)
    return [high, low]


def transform_tables(n, nx):
    at = np.arange(n)
    phase = 2.0 * np.pi * (at[:, None] * at[None, :] % n) / n
    cosine, sine = np.cos(phase), np.sin(phase)
    q = n // 4
    rows = np.concatenate([cosine.reshape(4, q, n), sine.reshape(4, q, n)], axis=1)

    x, c = np.arange(nx)[:, None], np.arange(nx // 2)[None, :]
    wave = 2.0 * np.pi * (x * c % nx) / nx
    sign = np.where(x % 2 == 0, 1.0, -1.0)
    columns = np.concatenate([np.cos(wave), np.where(c == 0, sign, -np.sin(wave))], axis=1)
    scale = 1.0 / (float(n) * n * nx)
    back_re = np.where(c == 0, 1.0, 2.0 * np.cos(wave)).T
    back_im = np.where(c == 0, sign, -2.0 * np.sin(wave)).T
    columns_back = np.concatenate([back_re, back_im], axis=0) * scale

    index = np.arange(2 * n)
    part, depth = index % 8 // 4, index // 8 * 4 + index % 4
    c_z, s_z = cosine[:, depth], sine[:, depth]
    depth_table = np.concatenate(
        [np.where(part == 0, c_z, s_z), np.where(part == 0, -s_z, c_z)], axis=0)

    m = np.arange(n // 2)
    back = []
    for core in range(2):
        ky = m // 2 * 4 + 2 * core + m % 2
        back.append(np.concatenate([cosine[:, ky], sine[:, ky]], axis=1))
    return [t for table in (rows, columns, depth_table, np.stack(back), columns_back)
            for t in two_terms(table)]


def right3(high, low, right):
    r_high, r_low = halves(right)
    return dot(high, r_high) + (dot(high, r_low) + dot(low, r_high))


def left3(left, high, low):
    l_high, l_low = halves(left)
    return dot(l_high, high) + (dot(l_high, low) + dot(l_low, high))


def reversal(n):
    total = lax.broadcasted_iota(jnp.int32, (n, n), 0) + lax.broadcasted_iota(jnp.int32, (n, n), 1)
    return jnp.where((total == 0) | (total == n), 1.0, 0.0).astype(BF16)


def moved_right(value, table):
    high, low = halves(value)
    return dot(high, table) + dot(low, table)


def moved_left(table, value):
    high, low = halves(value)
    return dot(table, high) + dot(table, low)


def dot3(left, right_high, right_low):
    high, low = halves(left)
    return dot(high, right_high) + (dot(high, right_low) + dot(low, right_high))


def kernel(views, pencils, taps, slab_ref, weight_ref, *refs):
    table_refs, refs = refs[:10], refs[10:]
    (out, out2, slab, weight, csh, csl, dxh, dxl, mh, ml, cyh, cyl, dih, dil,
     xh, xl, msg, got, wsend, wgot, we, wm, mth, mtl, g, gr, gsh, gsl, fs, gm, fr, pj, r1, r2,
     stacked, est, zed, mid, spread, acc, rz, rs, th, tl, ah, al,
     ssem, rsem, lsem, load_sem, share_sem, send_sem, recv_sem) = refs
    n = 4 * pencils
    q = n // 4
    half = pencils // 2
    v, p = lax.axis_index("view"), lax.axis_index("pencil")
    core = lax.rem(v, 2)
    mate = v + 1 - 2 * core
    far = lax.rem(v + 2, 4)
    mirror = pencils - 1 - p
    mirror0 = lax.rem(pencils - p, pencils)
    own_mirror = (p == 0) | (p == half)

    tables = [csh, csl, dxh, dxl, mh, ml, cyh, cyl, dih, dil]
    loads = [pltpu.make_async_copy(src, dst, load_sem.at[k])
             for k, (src, dst) in enumerate(zip(table_refs, tables))]
    slab_load = pltpu.make_async_copy(slab_ref, slab, load_sem.at[10])
    weight_loads = [pltpu.make_async_copy(weight_ref.at[:, :, pl.ds(128 * h, 128)], weight.at[h], load_sem.at[11 + h])
                    for h in range(2)]
    slab_load.start()
    for load in loads[2:4] + weight_loads + loads[:2] + loads[4:]:
        load.start()
    flat = [weight.at[h].reshape(4 * n, 128) for h in range(2)]

    def weight_rows(h, j):
        return flat[h][pl.ds(j, n, stride=4), :]

    depth, rows, width = 4, q, slab.shape[-1]
    frame = rows + 16

    def exists(side):
        v1, p1 = v + side[0], p + side[1]
        return (v1 >= 0) & (v1 < views) & (p1 >= 0) & (p1 < pencils)

    def back(side):
        return (-side[0], -side[1])

    def each(sides, action):
        for side in sides:
            @pl.when(exists(side))
            def _(side=side):
                action(side)

    est[...] = jnp.zeros_like(est)
    rz[...] = jnp.zeros_like(rz)
    rs[...] = jnp.zeros_like(rs)

    barrier = pltpu.get_barrier_semaphore()

    def greet(i, carry):
        pl.semaphore_signal(barrier, inc=1, device_id=(v, lax.rem(p + i, pencils)), device_id_type=MESH_ID)
        return carry

    lax.fori_loop(1, pencils, greet, 0, unroll=7)

    def greet_far(i, carry):
        pl.semaphore_signal(barrier, inc=1, device_id=(far, lax.rem(p + i, pencils)), device_id_type=MESH_ID)
        return carry

    lax.fori_loop(0, pencils, greet_far, 0, unroll=8)
    for other in (mate, lax.rem(mate + 2, 4)):
        pl.semaphore_signal(barrier, inc=1, device_id=(other, p), device_id_type=MESH_ID)
    corners = [side for side in SIDES if side[0] != 0 and side[1] != 0]

    def greet_corner(side):
        pl.semaphore_signal(barrier, inc=1, device_id=(v + side[0], p + side[1]), device_id_type=MESH_ID)

    each(corners, greet_corner)
    expected = 2 * pencils + 1 + sum(exists(side).astype(jnp.int32) for side in corners)

    slab_load.wait()
    loads[2].wait()
    loads[3].wait()
    for z in range(4):
        xh[z], xl[z] = halves(left3(slab[z], dxh[...], dxl[...]))
    mid[...] = jnp.zeros_like(mid)
    for load in weight_loads + loads[:2]:
        load.wait()

    def remote(src, dst, k, device):
        return pltpu.make_async_remote_copy(
            src_ref=src, dst_ref=dst, send_sem=ssem.at[k], recv_sem=rsem.at[k],
            device_id=device, device_id_type=MESH_ID)

    lane0 = lax.broadcasted_iota(jnp.int32, (n, 128), 1) == 0

    for j in range(4):
        receiver = mirror0 if j == 0 else mirror
        pick = lane0 & (receiver < half)
        wsend[j] = jnp.where(pick, weight_rows(0, j), weight_rows(1, j))

    pl.semaphore_wait(barrier, expected)
    w_rest = remote(wsend.at[pl.ds(1, 3)], wgot.at[pl.ds(1, 3)], 1, (v, mirror))
    w_first = remote(wsend.at[0], wgot.at[0], 2, (v, mirror0))
    w_local = pltpu.make_async_copy(wsend.at[0], wgot.at[0], lsem.at[0])
    w_rest.start()

    @pl.when(jnp.logical_not(own_mirror))
    def _():
        w_first.start()

    @pl.when(own_mirror)
    def _():
        w_local.start()

    lane_q = lax.broadcasted_iota(jnp.int32, (q, 128), 1) == 0
    row_q = lax.broadcasted_iota(jnp.int32, (q, 128), 0)

    group = pencils // 4
    for step in range(4):
        b = lax.rem(p // group + step, 4)
        first = b < 2
        for z in range(4):
            both = (dot(csh[b], xh[z]) + (dot(csh[b], xl[z]) + dot(csl[b], xh[z])))
            c_re, c_im = both[:q, :128], both[:q, 128:]
            s_re, s_im = both[q:, :128], both[q:, 128:]
            re, im = c_re + s_im, c_im - s_re
            re0 = jnp.where(first, c_re, c_im)
            im0 = jnp.where(first, -s_re, -s_im)
            im0 = jnp.where((row_q == 0) & (b == 0), c_im, im0)
            im0 = jnp.where((row_q == 0) & (b == 2), c_re, im0)
            at = pl.multiple_of(b * (q * 8), q * 8)
            msg[pl.ds(at + z, q, stride=8), :] = jnp.where(lane_q, re0, re)
            msg[pl.ds(at + 4 + z, q, stride=8), :] = jnp.where(lane_q, im0, im)

        def send_chunk(i, carry, b=b):
            peer = b * group + lax.rem(p + i, group)
            at = pl.multiple_of(peer * 32, 32)

            @pl.when(peer != p)
            def _():
                remote(msg.at[pl.ds(at, 32)], got.at[p], 0, (v, peer)).start()
            return carry

        lax.fori_loop(0, group, send_chunk, 0, unroll=2)

    own = pltpu.make_async_copy(msg.at[pl.ds(pl.multiple_of(p * 32, 32), 32)], got.at[p], lsem.at[1])
    own.start()

    def quarter_of(view):
        return slab.at[:, pl.ds(pl.multiple_of(view * q, q), q), :]

    shares = [pltpu.make_async_remote_copy(
        src_ref=quarter_of(lax.rem(v + d, views)), dst_ref=stacked.at[v],
        send_sem=share_sem.at[0, d - 1], recv_sem=share_sem.at[1, d - 1],
        device_id=(lax.rem(v + d, views), p), device_id_type=MESH_ID) for d in range(1, 4)]
    for share in shares:
        share.start()
    own_share = pltpu.make_async_copy(quarter_of(v), stacked.at[v], lsem.at[3])
    own_share.start()

    for load in loads[4:]:
        load.wait()
    mth[...] = mh[...].astype(F32).T.astype(BF16)
    mtl[...] = ml[...].astype(F32).T.astype(BF16)
    def band(v, carry):
        at = (lax.broadcasted_iota(jnp.int32, (width, width), 0)
              - lax.broadcasted_iota(jnp.int32, (width, width), 1))
        table, turned = jnp.zeros((width, width), F32), jnp.zeros((width, width), F32)
        for t in range(9):
            tap = taps[2, v, t]
            table = jnp.where(at == t - 4, tap, table)
            turned = jnp.where(at == 4 - t, tap, turned)
        whole_sum = 1.0
        for axis in range(3):
            axis_sum = taps[axis, v, 0]
            for t in range(1, 9):
                axis_sum = axis_sum + taps[axis, v, t]
            whole_sum = whole_sum * axis_sum
        th[v], tl[v] = halves(table / whole_sum)
        ah[v], al[v] = halves(turned / whole_sum)
        return carry

    lax.fori_loop(0, views, band, 0)

    w_rest.wait_recv()

    @pl.when(jnp.logical_not(own_mirror))
    def _():
        w_first.wait_recv()

    @pl.when(own_mirror)
    def _():
        w_local.wait()

    turn_z, turn_x = reversal(n), reversal(128)
    for j in range(4):
        mine = jnp.where(lane0 & (p >= half), weight_rows(1, j), weight_rows(0, j))
        turned = moved_left(turn_z, moved_right(wgot[(4 - j) % 4], turn_x))
        we[j] = 0.5 * (mine + turned)

    @pl.when(own_mirror)
    def _():
        first = (lax.broadcasted_iota(jnp.int32, (n, 128), 0) * 0 + p) == 0
        other = jnp.where(first, weight_rows(1, 0), weight_rows(0, 0))
        other = 0.5 * (other + moved_left(turn_z, other))
        main = we[0]
        we[0] = jnp.where(lane0, 0.5 * (main + other), main)
        wm[...] = jnp.where(lane0, 0.5 * (main - other), 0.0)

    own.wait()
    remote(got.at[pl.ds(0, pencils - 1)], got.at[pl.ds(0, pencils - 1)], 0, (v, mirror)).wait_recv()

    def pair_spectra(pair):
        block = got[:, pl.ds(pl.multiple_of(16 * pair, 16), 16), :]
        return [block[:, 8 * k:8 * k + 8, :].reshape(2 * n, 128) for k in range(2)]

    def weigh(pair):
        f = right3(mh[...], ml[...], jnp.concatenate(pair_spectra(pair), axis=1))
        for k in range(2):
            j = 2 * pair + k
            for part in range(2):
                g[j, part * n:(part + 1) * n, :] = (
                    f[part * n:(part + 1) * n, 128 * k:128 * k + 128] * we[j])

        @pl.when(own_mirror & (pair == 0))
        def _():
            imag = lax.rem(lax.broadcasted_iota(jnp.int32, (2 * n, 128), 0), 8) >= 4
            lines = got[:, 0:8, :].reshape(2 * n, 128)
            f = right3(mh[...], ml[...], jnp.where(imag, -lines, lines))
            for part in range(2):
                g[0, part * n:(part + 1) * n, :] = (
                    g[0, part * n:(part + 1) * n, :] + f[part * n:(part + 1) * n, :] * wm[...])

    weigh(1 - core)
    pair_sum = remote(g.at[pl.ds(2 - 2 * core, 2)], gr, 3, (mate, p))
    pair_sum.start()
    weigh(core)
    pair_sum.wait_recv()
    gsh[...], gsl[...] = halves(jnp.concatenate(
        [g[2 * core] + gr[0], g[2 * core + 1] + gr[1]], axis=1))

    kept = v // 2
    away = 1 - kept

    def rows_of(peer):
        return pl.ds(pl.multiple_of(peer * 8, 8), 8)

    for step in range(2):
        b = lax.rem(p // half + step, 2)
        at = pl.multiple_of(b * n, n)
        block = pl.ds(at, n)
        f = (dot(mth[block, :], gsh[...])
             + (dot(mth[block, :], gsl[...]) + dot(mtl[block, :], gsh[...])))
        for k in range(2):
            fs[k, block, :] = f[:, 128 * k:128 * k + 128]
        for x in range(2):
            for k in range(2):
                for part in range(2):
                    for zz in range(2):
                        gm[x, pl.ds(at + (4 * k + 2 * part + zz), half, stride=8), :] = (
                            fs[k, pl.ds(at + (4 * part + 2 * x + zz), half, stride=8), :])

        def send_back(i, carry, b=b):
            peer = b * half + lax.rem(p + i, half)

            @pl.when(peer != p)
            def _():
                remote(gm.at[kept, rows_of(peer)], fr.at[kept, rows_of(p)], 4, (v, peer)).start()

            remote(gm.at[away, rows_of(peer)], fr.at[kept, rows_of(p)], 7, (far, peer)).start()
            return carry

        lax.fori_loop(0, half, send_back, 0, unroll=2)

    own_back = pltpu.make_async_copy(gm.at[kept, rows_of(p)], fr.at[kept, rows_of(p)], lsem.at[2])
    own_back.start()
    own_back.wait()
    most = fr.at[kept, pl.ds(0, 8 * (pencils - 1))]
    remote(most, most, 4, (v, mirror)).wait_recv()
    remote(fr.at[away], fr.at[away], 7, (far, p)).wait_recv()

    m = lax.broadcasted_iota(jnp.int32, (n // 2, 128), 0)
    ky = m // 2 * 4 + 2 * core + lax.rem(m, 2)
    lane_m = lax.broadcasted_iota(jnp.int32, (n // 2, 128), 1) == 0
    low, high = (ky > 0) & (ky < n // 2), ky > n // 2
    for zz in range(2):
        re = fr[0, pl.ds(zz, n // 2, stride=4), :] + fr[1, pl.ds(zz, n // 2, stride=4), :]
        im = fr[0, pl.ds(2 + zz, n // 2, stride=4), :] + fr[1, pl.ds(2 + zz, n // 2, stride=4), :]
        zero = jnp.zeros_like(re)
        v1 = jnp.where(low, 2.0 * re, jnp.where(ky == 0, re, jnp.where(ky == n // 2, im, zero)))
        v2 = jnp.where(high, 2.0 * re, jnp.where(ky == 0, im, jnp.where(ky == n // 2, re, zero)))
        b1 = jnp.where(low, -2.0 * im, zero)
        b2 = jnp.where(high, -2.0 * im, zero)
        top = jnp.concatenate([jnp.where(lane_m, v1, re), jnp.where(lane_m, v2, im)], axis=1)
        bottom = jnp.concatenate([jnp.where(lane_m, b1, -im), jnp.where(lane_m, b2, re)], axis=1)
        u = right3(cyh[core], cyl[core], jnp.concatenate([top, bottom], axis=0))
        field = left3(u, dih[...], dil[...])
        for quarter in range(4):
            pj[quarter // 2, quarter % 2, zz] = field[quarter * q:(quarter + 1) * q]
        remote(pj.at[:, 1 - core, zz], r1.at[:, zz], 5 + 3 * zz, (mate, p)).start()

    def near(zz):
        return remote(pj.at[:, 1 - core, zz], r1.at[:, zz], 5 + 3 * zz, (mate, p))

    def long(zz):
        return remote(r1.at[away, zz], r2.at[zz], 6 + 3 * zz, (far, p))

    for zz in range(2):
        near(zz).wait_recv()
        r1[:, zz] = r1[:, zz] + pj[:, core, zz]
        long(zz).start()

    def est_copy(side, z):
        dv, dp = side
        src_rows = {0: pl.ds(8, rows), 1: pl.ds(rows, 8), -1: pl.ds(8, 8)}[dv]
        dst_rows = {0: pl.ds(8, rows), 1: pl.ds(0, 8), -1: pl.ds(rows + 8, 8)}[dv]
        return pltpu.make_async_remote_copy(
            src_ref=est.at[depth + z, :, src_rows, :],
            dst_ref=est.at[depth * (1 - dp) + z, :, dst_rows, :],
            send_sem=send_sem.at[0, SLOT[side], z],
            recv_sem=recv_sem.at[0, SLOT[back(side)], z],
            device_id=(v + dv, p + dp),
            device_id_type=MESH_ID,
        )

    def acc_copy(side, z):
        dv, dp = side
        src_rows = {0: pl.ds(8, rows), 1: pl.ds(rows + 8, 8), -1: pl.ds(0, 8)}[dv]
        slot = SLOT[back(side)]
        landing = rz.at[0 if dp == 1 else 1, z] if dv == 0 else rs.at[slot, z]
        return pltpu.make_async_remote_copy(
            src_ref=acc.at[depth * (1 + dp) + z, :, src_rows, :],
            dst_ref=landing,
            send_sem=send_sem.at[1, SLOT[side], z],
            recv_sem=recv_sem.at[1, slot, z],
            device_id=(v + dv, p + dp),
            device_id_type=MESH_ID,
        )

    def est_wait(side, z):
        dv, dp = side
        dst_rows = {0: pl.ds(8, rows), -1: pl.ds(0, 8), 1: pl.ds(rows + 8, 8)}[dv]
        landing = est.at[depth * (1 + dp) + z, :, dst_rows, :]
        pltpu.make_async_remote_copy(
            src_ref=landing, dst_ref=landing, send_sem=send_sem.at[0, SLOT[side], z],
            recv_sem=recv_sem.at[0, SLOT[side], z], device_id=(v + dv, p + dp),
            device_id_type=MESH_ID).wait_recv()

    def acc_wait(side, z):
        dv, dp = side
        landing = rz.at[0 if dp == -1 else 1, z] if dv == 0 else rs.at[SLOT[side], z]
        pltpu.make_async_remote_copy(
            src_ref=landing, dst_ref=landing, send_sem=send_sem.at[1, SLOT[side], z],
            recv_sem=recv_sem.at[1, SLOT[side], z], device_id=(v + dv, p + dp),
            device_id_type=MESH_ID).wait_recv()

    def every_plane(action):
        def at_plane(z, carry):
            each(SIDES, lambda side: action(side, z))
            return carry

        lax.fori_loop(0, depth, at_plane, 0)

    def start_estimate(z, plane):
        out[z] = plane
        for h in range(2):
            half_plane = plane[:, h * 128:(h + 1) * 128]
            est[depth + z, h, pl.ds(8, rows), :] = 0.1 + (
                jnp.maximum(half_plane, 0.0) + jnp.log1p(jnp.exp(-jnp.abs(half_plane))))
        each(SIDES, lambda side: est_copy(side, z).start())

    for zz in range(2):
        start_estimate(2 * kept + zz, r1[kept, zz])
    for zz in range(2):
        long(zz).wait_recv()
        start_estimate(2 * away + zz, r2[zz])
    own_share.wait()
    for share in shares:
        share.wait_recv()

    def view_step(w, carry):
        for z in range(depth):
            total = taps[0, w, 0] * est[z]
            for t in range(1, 9):
                total = total + taps[0, w, t] * est[z + t]
            zed[w, z] = total
        sides = []
        for h in range(2):
            planes = []
            for z in range(depth):
                total = taps[1, w, 0] * zed[w, z, h, pl.ds(4, rows), :]
                for t in range(1, 9):
                    total = total + taps[1, w, t] * zed[w, z, h, pl.ds(4 + t, rows), :]
                planes.append(total)
            sides.append(jnp.concatenate(planes, axis=0))
        blurred = dot3(jnp.concatenate(sides, axis=1), th[w], tl[w])
        ratio = stacked[w].reshape(depth * rows, width) / blurred
        turned = dot3(ratio, ah[w], al[w])
        for z in range(depth):
            for h in range(2):
                mid[w, z, h, pl.ds(16, rows), :] = turned[z * rows:(z + 1) * rows, h * 128:(h + 1) * 128]
        for z in range(depth):
            for h in range(2):
                total = taps[1, w, 8] * mid[w, z, h, pl.ds(4, frame), :]
                for t in range(1, 9):
                    total = total + taps[1, w, 8 - t] * mid[w, z, h, pl.ds(4 + t, frame), :]
                spread[w, z, h] = total
        return carry

    def gather_planes(planes):
        for zo in planes:
            total = None
            for v in range(views):
                for zs in range(depth):
                    if 0 <= zo - zs <= 8:
                        term = taps[0, v, zo - zs] * spread[v, zs]
                        total = term if total is None else total + term
            acc[zo] = total

    def iteration(step, carry):
        every_plane(est_wait)
        lax.fori_loop(0, views, view_step, 0, unroll=UNROLL)
        for z in range(depth):
            gather_planes([z, 2 * depth + z, depth + z])
            each(SIDES, lambda side: acc_copy(side, z).start())

        def finish_plane(z, carry):
            each(SIDES, lambda side: acc_wait(side, z))
            each(SIDES, lambda side: est_copy(side, z).wait_send())
            for h in range(2):
                total = acc[depth + z, h, pl.ds(8, rows), :] + (rz[0, z, h] + rz[1, z, h])
                low = rs[SLOT[(-1, 0)], z, h] + (rs[SLOT[(-1, -1)], z, h] + rs[SLOT[(-1, 1)], z, h])
                high = rs[SLOT[(1, 0)], z, h] + (rs[SLOT[(1, -1)], z, h] + rs[SLOT[(1, 1)], z, h])
                total = jnp.concatenate(
                    [total[:8] + low, total[8:rows - 8], total[rows - 8:] + high], axis=0)
                est[depth + z, h, pl.ds(8, rows), :] = (
                    est[depth + z, h, pl.ds(8, rows), :] * (total * (1.0 / views)))

            @pl.when(step < ITERS - 1)
            def _():
                each(SIDES, lambda side: est_copy(side, z).start())
            return carry

        lax.fori_loop(0, depth, finish_plane, 0)
        every_plane(lambda side, z: acc_copy(side, z).wait_send())
        return carry

    lax.fori_loop(0, ITERS, iteration, 0)
    for h in range(2):
        out2[:, :, h * 128:(h + 1) * 128] = est[pl.ds(depth, depth), h, pl.ds(8, rows), :]

    w_rest.wait_send()
    sent = msg.at[pl.ds(0, 32 * (pencils - 1))]
    remote(sent, sent, 0, (v, mirror)).wait_send()
    pair_sum.wait_send()
    sent_back = gm.at[kept, pl.ds(0, 8 * (pencils - 1))]
    remote(sent_back, sent_back, 4, (v, mirror)).wait_send()
    remote(gm.at[away], gm.at[away], 7, (far, p)).wait_send()
    for zz in range(2):
        near(zz).wait_send()
        long(zz).wait_send()

    @pl.when(jnp.logical_not(own_mirror))
    def _():
        w_first.wait_send()
    for share in shares:
        share.wait_send()


def whole(recorded, weight, taps):
    views, pencils = lax.axis_size("view"), lax.axis_size("pencil")
    n, nx = 4 * pencils, recorded.shape[-1]
    q, depth = n // 4, 4
    frame = q + 16
    vmem, left = pl.BlockSpec(memory_space=pltpu.VMEM), pl.BlockSpec(memory_space=pltpu.HBM)
    tables = [jnp.asarray(t) for t in transform_tables(n, nx)]
    block = pltpu.VMEM((depth, q, nx), F32)
    return pl.pallas_call(
        functools.partial(kernel, views, pencils),
        name="join_and_deconvolve",
        out_shape=(block, block),
        in_specs=[pl.BlockSpec(memory_space=pltpu.SMEM)] + [left] * (2 + len(tables)),
        out_specs=(vmem, vmem),
        scratch_shapes=[
            pltpu.VMEM((4, n, nx), F32),
            pltpu.VMEM((2, n, 4, 128), F32),
            *[pltpu.VMEM(t.shape, t.dtype) for t in tables],
            pltpu.VMEM((4, n, nx), BF16),
            pltpu.VMEM((4, n, nx), BF16),
            pltpu.VMEM((8 * n, 128), F32),
            pltpu.VMEM((pencils, 32, 128), F32),
            pltpu.VMEM((4, n, 128), F32),
            pltpu.VMEM((4, n, 128), F32),
            pltpu.VMEM((4, n, 128), F32),
            pltpu.VMEM((n, 128), F32),
            pltpu.VMEM((2 * n, 2 * n), BF16),
            pltpu.VMEM((2 * n, 2 * n), BF16),
            pltpu.VMEM((4, 2 * n, 128), F32),
            pltpu.VMEM((2, 2 * n, 128), F32),
            pltpu.VMEM((2 * n, 256), BF16),
            pltpu.VMEM((2 * n, 256), BF16),
            pltpu.VMEM((2, 2 * n, 128), F32),
            pltpu.VMEM((2, 8 * pencils, 128), F32),
            pltpu.VMEM((2, 8 * pencils, 128), F32),
            pltpu.VMEM((2, 2, 2, q, nx), F32),
            pltpu.VMEM((2, 2, q, nx), F32),
            pltpu.VMEM((2, q, nx), F32),
            pltpu.VMEM((views, depth, q, nx), F32),
            pltpu.VMEM((3 * depth, 2, frame, 128), F32),
            pltpu.VMEM((views, depth, 2, frame, 128), F32),
            pltpu.VMEM((views, depth, 2, frame + 16, 128), F32),
            pltpu.VMEM((views, depth, 2, frame, 128), F32),
            pltpu.VMEM((3 * depth, 2, frame, 128), F32),
            pltpu.VMEM((2, depth, 2, q, 128), F32),
            pltpu.VMEM((8, depth, 2, 8, 128), F32),
            *[pltpu.VMEM((views, nx, nx), BF16)] * 4,
            pltpu.SemaphoreType.DMA((10,)),
            pltpu.SemaphoreType.DMA((10,)),
            pltpu.SemaphoreType.DMA((4,)),
            pltpu.SemaphoreType.DMA((13,)),
            pltpu.SemaphoreType.DMA((2, 3)),
            pltpu.SemaphoreType.DMA((2, 8, 4)),
            pltpu.SemaphoreType.DMA((2, 8, 4)),
        ],
        compiler_params=pltpu.CompilerParams(collective_id=1, has_side_effects=True,
                                             vmem_limit_bytes=62 * 1024 * 1024),
    )(taps, recorded, weight, *tables)


def store(first, second, first_out, second_out, sem):
    copies = [pltpu.make_async_copy(src, dst, sem.at[k])
              for k, (src, dst) in enumerate(((first, first_out), (second, second_out)))]
    for copy in copies:
        copy.start()
    for copy in copies:
        copy.wait()


def stored(first, second):
    shape = jax.ShapeDtypeStruct(first.shape, F32)
    return pl.pallas_call(
        store,
        name="store",
        out_shape=(shape, shape),
        in_specs=[pl.BlockSpec(memory_space=pl.ANY)] * 2,
        out_specs=(pl.BlockSpec(memory_space=pltpu.HBM),) * 2,
        scratch_shapes=[pltpu.SemaphoreType.DMA((2,))],
        compiler_params=pltpu.CompilerParams(vmem_limit_bytes=2 * 1024 * 1024),
    )(first, second)


def body(recorded, spectral_weight, psf_taps):
    taps = jnp.transpose(psf_taps, (1, 0, 2))
    return stored(*whole(recorded[0], spectral_weight[0], taps))


def solution(mesh):
    return jax.shard_map(
        body,
        mesh=mesh,
        in_specs=(P("view", "pencil", None, None), P("view", None, "pencil", None), P()),
        out_specs=(P("pencil", "view", None), P("pencil", "view", None)),
        check_vma=False,
    )
```

```python
import functools

import jax
import jax.numpy as jnp
import numpy as np
from jax import lax
from jax.experimental import pallas as pl
from jax.experimental.pallas import tpu as pltpu
from jax.sharding import PartitionSpec as P

ITERS = 2
UNROLL = 4
LATE = (3, 7, 11)
MESH_ID = pl.DeviceIdType.MESH
F32 = jnp.float32
BF16 = jnp.bfloat16
SIDES = [(dv, dp) for dp in (-1, 1, 0) for dv in (0, -1, 1) if (dv, dp) != (0, 0)]
SLOT = {side: k for k, side in enumerate(SIDES)}


def halves(value):
    high = value.astype(BF16)
    return high, (value - high.astype(F32)).astype(BF16)


def dot(left, right):
    return jnp.dot(left, right, preferred_element_type=F32)


def two_terms(table):
    high = table.astype(jnp.bfloat16)
    low = (table - high.astype(np.float64)).astype(jnp.bfloat16)
    return [high, low]


def transform_tables(n, nx):
    at = np.arange(n)
    phase = 2.0 * np.pi * (at[:, None] * at[None, :] % n) / n
    cosine, sine = np.cos(phase), np.sin(phase)
    q = n // 4
    rows = np.concatenate([cosine.reshape(4, q, n), sine.reshape(4, q, n)], axis=1)

    x, c = np.arange(nx)[:, None], np.arange(nx // 2)[None, :]
    wave = 2.0 * np.pi * (x * c % nx) / nx
    sign = np.where(x % 2 == 0, 1.0, -1.0)
    columns = np.concatenate([np.cos(wave), np.where(c == 0, sign, -np.sin(wave))], axis=1)
    scale = 1.0 / (float(n) * n * nx)
    back_re = np.where(c == 0, 1.0, 2.0 * np.cos(wave)).T
    back_im = np.where(c == 0, sign, -2.0 * np.sin(wave)).T
    columns_back = np.concatenate([back_re, back_im], axis=0) * scale

    index = np.arange(2 * n)
    part, depth = index % 8 // 4, index // 8 * 4 + index % 4
    c_z, s_z = cosine[:, depth], sine[:, depth]
    depth_table = np.concatenate(
        [np.where(part == 0, c_z, s_z), np.where(part == 0, -s_z, c_z)], axis=0)

    m = np.arange(n // 2)
    back = []
    for core in range(2):
        ky = m // 2 * 4 + 2 * core + m % 2
        back.append(np.concatenate([cosine[:, ky], sine[:, ky]], axis=1))
    return [t for table in (rows, columns, depth_table, np.stack(back), columns_back)
            for t in two_terms(table)]


def right3(high, low, right):
    r_high, r_low = halves(right)
    return dot(high, r_high) + (dot(high, r_low) + dot(low, r_high))


def left3(left, high, low):
    l_high, l_low = halves(left)
    return dot(l_high, high) + (dot(l_high, low) + dot(l_low, high))


def reversal(n):
    total = lax.broadcasted_iota(jnp.int32, (n, n), 0) + lax.broadcasted_iota(jnp.int32, (n, n), 1)
    return jnp.where((total == 0) | (total == n), 1.0, 0.0).astype(BF16)


def moved_right(value, table):
    high, low = halves(value)
    return dot(high, table) + dot(low, table)


def moved_left(table, value):
    high, low = halves(value)
    return dot(table, high) + dot(table, low)


def dot3(left, right_high, right_low):
    high, low = halves(left)
    return dot(high, right_high) + (dot(high, right_low) + dot(low, right_high))


def kernel(views, pencils, taps, slab_ref, weight_ref, *refs):
    table_refs, refs = refs[:10], refs[10:]
    (out, out2, slab, weight, csh, csl, dxh, dxl, mh, ml, cyh, cyl, dih, dil,
     xh, xl, msg, got, wsend, wgot, we, wm, mth, mtl, g, gr, gsh, gsl, fs, gm, fr, pj, r1, r2,
     stacked, est, zed, mid, spread, acc, rz, rs, th, tl, ah, al,
     ssem, rsem, lsem, load_sem, share_sem, send_sem, recv_sem) = refs
    n = 4 * pencils
    q = n // 4
    half = pencils // 2
    v, p = lax.axis_index("view"), lax.axis_index("pencil")
    core = lax.rem(v, 2)
    mate = v + 1 - 2 * core
    far = lax.rem(v + 2, 4)
    mirror = pencils - 1 - p
    mirror0 = lax.rem(pencils - p, pencils)
    own_mirror = (p == 0) | (p == half)

    tables = [csh, csl, dxh, dxl, mh, ml, cyh, cyl, dih, dil]
    loads = [pltpu.make_async_copy(src, dst, load_sem.at[k])
             for k, (src, dst) in enumerate(zip(table_refs, tables))]
    slab_load = pltpu.make_async_copy(slab_ref, slab, load_sem.at[10])
    weight_loads = [pltpu.make_async_copy(weight_ref.at[:, :, pl.ds(128 * h, 128)], weight.at[h], load_sem.at[11 + h])
                    for h in range(2)]
    slab_load.start()
    for load in loads[2:4] + weight_loads + loads[:2] + loads[4:]:
        load.start()
    flat = [weight.at[h].reshape(4 * n, 128) for h in range(2)]

    def weight_rows(h, j):
        return flat[h][pl.ds(j, n, stride=4), :]

    depth, rows, width = 4, q, slab.shape[-1]
    frame = rows + 16

    def exists(side):
        v1, p1 = v + side[0], p + side[1]
        return (v1 >= 0) & (v1 < views) & (p1 >= 0) & (p1 < pencils)

    def back(side):
        return (-side[0], -side[1])

    def each(sides, action):
        for side in sides:
            @pl.when(exists(side))
            def _(side=side):
                action(side)

    est[...] = jnp.zeros_like(est)
    rz[...] = jnp.zeros_like(rz)
    rs[...] = jnp.zeros_like(rs)

    barrier = pltpu.get_barrier_semaphore()

    def greet(i, carry):
        pl.semaphore_signal(barrier, inc=1, device_id=(v, lax.rem(p + i, pencils)), device_id_type=MESH_ID)
        return carry

    lax.fori_loop(1, pencils, greet, 0, unroll=7)

    def greet_far(i, carry):
        pl.semaphore_signal(barrier, inc=1, device_id=(far, lax.rem(p + i, pencils)), device_id_type=MESH_ID)
        return carry

    lax.fori_loop(0, pencils, greet_far, 0, unroll=8)
    for other in (mate, lax.rem(mate + 2, 4)):
        pl.semaphore_signal(barrier, inc=1, device_id=(other, p), device_id_type=MESH_ID)
    corners = [side for side in SIDES if side[0] != 0 and side[1] != 0]

    def greet_corner(side):
        pl.semaphore_signal(barrier, inc=1, device_id=(v + side[0], p + side[1]), device_id_type=MESH_ID)

    each(corners, greet_corner)
    expected = 2 * pencils + 1 + sum(exists(side).astype(jnp.int32) for side in corners)

    slab_load.wait()
    loads[2].wait()
    loads[3].wait()
    for z in range(4):
        xh[z], xl[z] = halves(left3(slab[z], dxh[...], dxl[...]))
    mid[...] = jnp.zeros_like(mid)
    for load in weight_loads + loads[:2]:
        load.wait()

    def remote(src, dst, k, device):
        return pltpu.make_async_remote_copy(
            src_ref=src, dst_ref=dst, send_sem=ssem.at[k], recv_sem=rsem.at[k],
            device_id=device, device_id_type=MESH_ID)

    lane0 = lax.broadcasted_iota(jnp.int32, (n, 128), 1) == 0

    for j in range(4):
        receiver = mirror0 if j == 0 else mirror
        pick = lane0 & (receiver < half)
        wsend[j] = jnp.where(pick, weight_rows(0, j), weight_rows(1, j))

    pl.semaphore_wait(barrier, expected)
    w_rest = remote(wsend.at[pl.ds(1, 3)], wgot.at[pl.ds(1, 3)], 1, (v, mirror))
    w_first = remote(wsend.at[0], wgot.at[0], 2, (v, mirror0))
    w_local = pltpu.make_async_copy(wsend.at[0], wgot.at[0], lsem.at[0])
    w_rest.start()

    @pl.when(jnp.logical_not(own_mirror))
    def _():
        w_first.start()

    @pl.when(own_mirror)
    def _():
        w_local.start()

    lane_q = lax.broadcasted_iota(jnp.int32, (q, 128), 1) == 0
    row_q = lax.broadcasted_iota(jnp.int32, (q, 128), 0)

    group = pencils // 4
    for step in range(4):
        b = lax.rem(p // group + step, 4)
        first = b < 2
        for z in range(4):
            both = (dot(csh[b], xh[z]) + (dot(csh[b], xl[z]) + dot(csl[b], xh[z])))
            c_re, c_im = both[:q, :128], both[:q, 128:]
            s_re, s_im = both[q:, :128], both[q:, 128:]
            re, im = c_re + s_im, c_im - s_re
            re0 = jnp.where(first, c_re, c_im)
            im0 = jnp.where(first, -s_re, -s_im)
            im0 = jnp.where((row_q == 0) & (b == 0), c_im, im0)
            im0 = jnp.where((row_q == 0) & (b == 2), c_re, im0)
            at = pl.multiple_of(b * (q * 8), q * 8)
            msg[pl.ds(at + z, q, stride=8), :] = jnp.where(lane_q, re0, re)
            msg[pl.ds(at + 4 + z, q, stride=8), :] = jnp.where(lane_q, im0, im)

        def send_chunk(i, carry, b=b):
            peer = b * group + lax.rem(p + i, group)
            at = pl.multiple_of(peer * 32, 32)

            @pl.when(peer != p)
            def _():
                remote(msg.at[pl.ds(at, 32)], got.at[p], 0, (v, peer)).start()
            return carry

        lax.fori_loop(0, group, send_chunk, 0, unroll=2)

    own = pltpu.make_async_copy(msg.at[pl.ds(pl.multiple_of(p * 32, 32), 32)], got.at[p], lsem.at[1])
    own.start()

    def quarter_of(view):
        return slab.at[:, pl.ds(pl.multiple_of(view * q, q), q), :]

    shares = [pltpu.make_async_remote_copy(
        src_ref=quarter_of(lax.rem(v + d, views)), dst_ref=stacked.at[v],
        send_sem=share_sem.at[0, d - 1], recv_sem=share_sem.at[1, d - 1],
        device_id=(lax.rem(v + d, views), p), device_id_type=MESH_ID) for d in range(1, 4)]
    for share in shares:
        share.start()
    own_share = pltpu.make_async_copy(quarter_of(v), stacked.at[v], lsem.at[3])
    own_share.start()

    for load in loads[4:]:
        load.wait()
    mth[...] = mh[...].astype(F32).T.astype(BF16)
    mtl[...] = ml[...].astype(F32).T.astype(BF16)
    def band(v, carry):
        at = (lax.broadcasted_iota(jnp.int32, (width, width), 0)
              - lax.broadcasted_iota(jnp.int32, (width, width), 1))
        table, turned = jnp.zeros((width, width), F32), jnp.zeros((width, width), F32)
        for t in range(9):
            tap = taps[2, v, t]
            table = jnp.where(at == t - 4, tap, table)
            turned = jnp.where(at == 4 - t, tap, turned)
        whole_sum = 1.0
        for axis in range(3):
            axis_sum = taps[axis, v, 0]
            for t in range(1, 9):
                axis_sum = axis_sum + taps[axis, v, t]
            whole_sum = whole_sum * axis_sum
        th[v], tl[v] = halves(table / whole_sum)
        ah[v], al[v] = halves(turned / whole_sum)
        return carry

    lax.fori_loop(0, views, band, 0)

    w_rest.wait_recv()

    @pl.when(jnp.logical_not(own_mirror))
    def _():
        w_first.wait_recv()

    @pl.when(own_mirror)
    def _():
        w_local.wait()

    turn_z, turn_x = reversal(n), reversal(128)
    for j in range(4):
        mine = jnp.where(lane0 & (p >= half), weight_rows(1, j), weight_rows(0, j))
        turned = moved_left(turn_z, moved_right(wgot[(4 - j) % 4], turn_x))
        we[j] = 0.5 * (mine + turned)

    @pl.when(own_mirror)
    def _():
        first = (lax.broadcasted_iota(jnp.int32, (n, 128), 0) * 0 + p) == 0
        other = jnp.where(first, weight_rows(1, 0), weight_rows(0, 0))
        other = 0.5 * (other + moved_left(turn_z, other))
        main = we[0]
        we[0] = jnp.where(lane0, 0.5 * (main + other), main)
        wm[...] = jnp.where(lane0, 0.5 * (main - other), 0.0)

    own.wait()
    remote(got.at[pl.ds(0, pencils - 1)], got.at[pl.ds(0, pencils - 1)], 0, (v, mirror)).wait_recv()

    def pair_spectra(pair):
        block = got[:, pl.ds(pl.multiple_of(16 * pair, 16), 16), :]
        return [block[:, 8 * k:8 * k + 8, :].reshape(2 * n, 128) for k in range(2)]

    def weigh(pair):
        f = right3(mh[...], ml[...], jnp.concatenate(pair_spectra(pair), axis=1))
        for k in range(2):
            j = 2 * pair + k
            for part in range(2):
                g[j, part * n:(part + 1) * n, :] = (
                    f[part * n:(part + 1) * n, 128 * k:128 * k + 128] * we[j])

        @pl.when(own_mirror & (pair == 0))
        def _():
            imag = lax.rem(lax.broadcasted_iota(jnp.int32, (2 * n, 128), 0), 8) >= 4
            lines = got[:, 0:8, :].reshape(2 * n, 128)
            f = right3(mh[...], ml[...], jnp.where(imag, -lines, lines))
            for part in range(2):
                g[0, part * n:(part + 1) * n, :] = (
                    g[0, part * n:(part + 1) * n, :] + f[part * n:(part + 1) * n, :] * wm[...])

    weigh(1 - core)
    pair_sum = remote(g.at[pl.ds(2 - 2 * core, 2)], gr, 3, (mate, p))
    pair_sum.start()
    weigh(core)
    pair_sum.wait_recv()
    gsh[...], gsl[...] = halves(jnp.concatenate(
        [g[2 * core] + gr[0], g[2 * core + 1] + gr[1]], axis=1))

    kept = v // 2
    away = 1 - kept

    def rows_of(peer):
        return pl.ds(pl.multiple_of(peer * 8, 8), 8)

    for step in range(2):
        b = lax.rem(p // half + step, 2)
        at = pl.multiple_of(b * n, n)
        block = pl.ds(at, n)
        f = (dot(mth[block, :], gsh[...])
             + (dot(mth[block, :], gsl[...]) + dot(mtl[block, :], gsh[...])))
        for k in range(2):
            fs[k, block, :] = f[:, 128 * k:128 * k + 128]
        for x in range(2):
            for k in range(2):
                for part in range(2):
                    for zz in range(2):
                        gm[x, pl.ds(at + (4 * k + 2 * part + zz), half, stride=8), :] = (
                            fs[k, pl.ds(at + (4 * part + 2 * x + zz), half, stride=8), :])

        def send_back(i, carry, b=b):
            peer = b * half + lax.rem(p + i, half)

            @pl.when(peer != p)
            def _():
                remote(gm.at[kept, rows_of(peer)], fr.at[kept, rows_of(p)], 4, (v, peer)).start()

            remote(gm.at[away, rows_of(peer)], fr.at[kept, rows_of(p)], 7, (far, peer)).start()
            return carry

        lax.fori_loop(0, half, send_back, 0, unroll=2)

    own_back = pltpu.make_async_copy(gm.at[kept, rows_of(p)], fr.at[kept, rows_of(p)], lsem.at[2])
    own_back.start()
    own_back.wait()
    most = fr.at[kept, pl.ds(0, 8 * (pencils - 1))]
    remote(most, most, 4, (v, mirror)).wait_recv()
    remote(fr.at[away], fr.at[away], 7, (far, p)).wait_recv()

    m = lax.broadcasted_iota(jnp.int32, (n // 2, 128), 0)
    ky = m // 2 * 4 + 2 * core + lax.rem(m, 2)
    lane_m = lax.broadcasted_iota(jnp.int32, (n // 2, 128), 1) == 0
    low, high = (ky > 0) & (ky < n // 2), ky > n // 2
    for zz in range(2):
        re = fr[0, pl.ds(zz, n // 2, stride=4), :] + fr[1, pl.ds(zz, n // 2, stride=4), :]
        im = fr[0, pl.ds(2 + zz, n // 2, stride=4), :] + fr[1, pl.ds(2 + zz, n // 2, stride=4), :]
        zero = jnp.zeros_like(re)
        v1 = jnp.where(low, 2.0 * re, jnp.where(ky == 0, re, jnp.where(ky == n // 2, im, zero)))
        v2 = jnp.where(high, 2.0 * re, jnp.where(ky == 0, im, jnp.where(ky == n // 2, re, zero)))
        b1 = jnp.where(low, -2.0 * im, zero)
        b2 = jnp.where(high, -2.0 * im, zero)
        top = jnp.concatenate([jnp.where(lane_m, v1, re), jnp.where(lane_m, v2, im)], axis=1)
        bottom = jnp.concatenate([jnp.where(lane_m, b1, -im), jnp.where(lane_m, b2, re)], axis=1)
        u = right3(cyh[core], cyl[core], jnp.concatenate([top, bottom], axis=0))
        field = left3(u, dih[...], dil[...])
        for quarter in range(4):
            pj[quarter // 2, quarter % 2, zz] = field[quarter * q:(quarter + 1) * q]
        remote(pj.at[:, 1 - core, zz], r1.at[:, zz], 5 + 3 * zz, (mate, p)).start()

    def near(zz):
        return remote(pj.at[:, 1 - core, zz], r1.at[:, zz], 5 + 3 * zz, (mate, p))

    def long(zz):
        return remote(r1.at[away, zz], r2.at[zz], 6 + 3 * zz, (far, p))

    for zz in range(2):
        near(zz).wait_recv()
        r1[:, zz] = r1[:, zz] + pj[:, core, zz]
        long(zz).start()

    def est_copy(side, z):
        dv, dp = side
        src_rows = {0: pl.ds(8, rows), 1: pl.ds(rows, 8), -1: pl.ds(8, 8)}[dv]
        dst_rows = {0: pl.ds(8, rows), 1: pl.ds(0, 8), -1: pl.ds(rows + 8, 8)}[dv]
        return pltpu.make_async_remote_copy(
            src_ref=est.at[depth + z, :, src_rows, :],
            dst_ref=est.at[depth * (1 - dp) + z, :, dst_rows, :],
            send_sem=send_sem.at[0, SLOT[side], z],
            recv_sem=recv_sem.at[0, SLOT[back(side)], z],
            device_id=(v + dv, p + dp),
            device_id_type=MESH_ID,
        )

    def acc_copy(side, z):
        dv, dp = side
        src_rows = {0: pl.ds(8, rows), 1: pl.ds(rows + 8, 8), -1: pl.ds(0, 8)}[dv]
        slot = SLOT[back(side)]
        landing = rz.at[0 if dp == 1 else 1, z] if dv == 0 else rs.at[slot, z]
        return pltpu.make_async_remote_copy(
            src_ref=acc.at[depth * (1 + dp) + z, :, src_rows, :],
            dst_ref=landing,
            send_sem=send_sem.at[1, SLOT[side], z],
            recv_sem=recv_sem.at[1, slot, z],
            device_id=(v + dv, p + dp),
            device_id_type=MESH_ID,
        )

    def est_wait(side, z):
        dv, dp = side
        dst_rows = {0: pl.ds(8, rows), -1: pl.ds(0, 8), 1: pl.ds(rows + 8, 8)}[dv]
        landing = est.at[depth * (1 + dp) + z, :, dst_rows, :]
        pltpu.make_async_remote_copy(
            src_ref=landing, dst_ref=landing, send_sem=send_sem.at[0, SLOT[side], z],
            recv_sem=recv_sem.at[0, SLOT[side], z], device_id=(v + dv, p + dp),
            device_id_type=MESH_ID).wait_recv()

    def acc_wait(side, z):
        dv, dp = side
        landing = rz.at[0 if dp == -1 else 1, z] if dv == 0 else rs.at[SLOT[side], z]
        pltpu.make_async_remote_copy(
            src_ref=landing, dst_ref=landing, send_sem=send_sem.at[1, SLOT[side], z],
            recv_sem=recv_sem.at[1, SLOT[side], z], device_id=(v + dv, p + dp),
            device_id_type=MESH_ID).wait_recv()

    def every_plane(action, planes):
        def at_plane(z, carry):
            each(SIDES, lambda side: action(side, z))
            return carry

        lax.fori_loop(0, planes, at_plane, 0)

    def start_estimate(z, plane):
        out[z] = plane
        for h in range(2):
            half_plane = plane[:, h * 128:(h + 1) * 128]
            est[depth + z, h, pl.ds(8, rows), :] = 0.1 + (
                jnp.maximum(half_plane, 0.0) + jnp.log1p(jnp.exp(-jnp.abs(half_plane))))
        each(SIDES, lambda side: est_copy(side, z).start())

    for zz in range(2):
        start_estimate(2 * kept + zz, r1[kept, zz])
    for zz in range(2):
        long(zz).wait_recv()
        start_estimate(2 * away + zz, r2[zz])
    own_share.wait()
    for share in shares:
        share.wait_recv()

    def early_step(w, carry):
        for z in range(depth):
            total = None
            for t in range(9):
                if z + t not in LATE:
                    term = taps[0, w, t] * est[z + t]
                    total = term if total is None else total + term
            zed[w, z] = total
        return carry

    def view_step(w, carry):
        for z in range(depth):
            total = zed[w, z]
            for plane in LATE:
                if 0 <= plane - z <= 8:
                    total = total + taps[0, w, plane - z] * est[plane]
            zed[w, z] = total
        sides = []
        for h in range(2):
            planes = []
            for z in range(depth):
                total = taps[1, w, 0] * zed[w, z, h, pl.ds(4, rows), :]
                for t in range(1, 9):
                    total = total + taps[1, w, t] * zed[w, z, h, pl.ds(4 + t, rows), :]
                planes.append(total)
            sides.append(jnp.concatenate(planes, axis=0))
        blurred = dot3(jnp.concatenate(sides, axis=1), th[w], tl[w])
        ratio = stacked[w].reshape(depth * rows, width) / blurred
        turned = dot3(ratio, ah[w], al[w])
        for z in range(depth):
            for h in range(2):
                mid[w, z, h, pl.ds(16, rows), :] = turned[z * rows:(z + 1) * rows, h * 128:(h + 1) * 128]
        for z in range(depth):
            for h in range(2):
                total = taps[1, w, 8] * mid[w, z, h, pl.ds(4, frame), :]
                for t in range(1, 9):
                    total = total + taps[1, w, 8 - t] * mid[w, z, h, pl.ds(4 + t, frame), :]
                spread[w, z, h] = total
        return carry

    def gather_planes(planes):
        for zo in planes:
            total = None
            for v in range(views):
                for zs in range(depth):
                    if 0 <= zo - zs <= 8:
                        term = taps[0, v, zo - zs] * spread[v, zs]
                        total = term if total is None else total + term
            acc[zo] = total

    def iteration(step, carry):
        every_plane(est_wait, depth - 1)
        lax.fori_loop(0, views, early_step, 0)
        each(SIDES, lambda side: est_wait(side, depth - 1))
        lax.fori_loop(0, views, view_step, 0, unroll=UNROLL)
        for z in range(depth):
            gather_planes([z, 2 * depth + z, depth + z])
            each(SIDES, lambda side: acc_copy(side, z).start())

        def finish_plane(z, carry):
            each(SIDES, lambda side: acc_wait(side, z))
            each(SIDES, lambda side: est_copy(side, z).wait_send())
            for h in range(2):
                total = acc[depth + z, h, pl.ds(8, rows), :] + (rz[0, z, h] + rz[1, z, h])
                low = rs[SLOT[(-1, 0)], z, h] + (rs[SLOT[(-1, -1)], z, h] + rs[SLOT[(-1, 1)], z, h])
                high = rs[SLOT[(1, 0)], z, h] + (rs[SLOT[(1, -1)], z, h] + rs[SLOT[(1, 1)], z, h])
                total = jnp.concatenate(
                    [total[:8] + low, total[8:rows - 8], total[rows - 8:] + high], axis=0)
                est[depth + z, h, pl.ds(8, rows), :] = (
                    est[depth + z, h, pl.ds(8, rows), :] * (total * (1.0 / views)))

            @pl.when(step < ITERS - 1)
            def _():
                each(SIDES, lambda side: est_copy(side, z).start())
            return carry

        lax.fori_loop(0, depth, finish_plane, 0)
        every_plane(lambda side, z: acc_copy(side, z).wait_send(), depth)
        return carry

    lax.fori_loop(0, ITERS, iteration, 0)
    for h in range(2):
        out2[:, :, h * 128:(h + 1) * 128] = est[pl.ds(depth, depth), h, pl.ds(8, rows), :]

    w_rest.wait_send()
    sent = msg.at[pl.ds(0, 32 * (pencils - 1))]
    remote(sent, sent, 0, (v, mirror)).wait_send()
    pair_sum.wait_send()
    sent_back = gm.at[kept, pl.ds(0, 8 * (pencils - 1))]
    remote(sent_back, sent_back, 4, (v, mirror)).wait_send()
    remote(gm.at[away], gm.at[away], 7, (far, p)).wait_send()
    for zz in range(2):
        near(zz).wait_send()
        long(zz).wait_send()

    @pl.when(jnp.logical_not(own_mirror))
    def _():
        w_first.wait_send()
    for share in shares:
        share.wait_send()


def whole(recorded, weight, taps):
    views, pencils = lax.axis_size("view"), lax.axis_size("pencil")
    n, nx = 4 * pencils, recorded.shape[-1]
    q, depth = n // 4, 4
    frame = q + 16
    vmem, left = pl.BlockSpec(memory_space=pltpu.VMEM), pl.BlockSpec(memory_space=pltpu.HBM)
    tables = [jnp.asarray(t) for t in transform_tables(n, nx)]
    block = pltpu.VMEM((depth, q, nx), F32)
    return pl.pallas_call(
        functools.partial(kernel, views, pencils),
        name="join_and_deconvolve",
        out_shape=(block, block),
        in_specs=[pl.BlockSpec(memory_space=pltpu.SMEM)] + [left] * (2 + len(tables)),
        out_specs=(vmem, vmem),
        scratch_shapes=[
            pltpu.VMEM((4, n, nx), F32),
            pltpu.VMEM((2, n, 4, 128), F32),
            *[pltpu.VMEM(t.shape, t.dtype) for t in tables],
            pltpu.VMEM((4, n, nx), BF16),
            pltpu.VMEM((4, n, nx), BF16),
            pltpu.VMEM((8 * n, 128), F32),
            pltpu.VMEM((pencils, 32, 128), F32),
            pltpu.VMEM((4, n, 128), F32),
            pltpu.VMEM((4, n, 128), F32),
            pltpu.VMEM((4, n, 128), F32),
            pltpu.VMEM((n, 128), F32),
            pltpu.VMEM((2 * n, 2 * n), BF16),
            pltpu.VMEM((2 * n, 2 * n), BF16),
            pltpu.VMEM((4, 2 * n, 128), F32),
            pltpu.VMEM((2, 2 * n, 128), F32),
            pltpu.VMEM((2 * n, 256), BF16),
            pltpu.VMEM((2 * n, 256), BF16),
            pltpu.VMEM((2, 2 * n, 128), F32),
            pltpu.VMEM((2, 8 * pencils, 128), F32),
            pltpu.VMEM((2, 8 * pencils, 128), F32),
            pltpu.VMEM((2, 2, 2, q, nx), F32),
            pltpu.VMEM((2, 2, q, nx), F32),
            pltpu.VMEM((2, q, nx), F32),
            pltpu.VMEM((views, depth, q, nx), F32),
            pltpu.VMEM((3 * depth, 2, frame, 128), F32),
            pltpu.VMEM((views, depth, 2, frame, 128), F32),
            pltpu.VMEM((views, depth, 2, frame + 16, 128), F32),
            pltpu.VMEM((views, depth, 2, frame, 128), F32),
            pltpu.VMEM((3 * depth, 2, frame, 128), F32),
            pltpu.VMEM((2, depth, 2, q, 128), F32),
            pltpu.VMEM((8, depth, 2, 8, 128), F32),
            *[pltpu.VMEM((views, nx, nx), BF16)] * 4,
            pltpu.SemaphoreType.DMA((10,)),
            pltpu.SemaphoreType.DMA((10,)),
            pltpu.SemaphoreType.DMA((4,)),
            pltpu.SemaphoreType.DMA((13,)),
            pltpu.SemaphoreType.DMA((2, 3)),
            pltpu.SemaphoreType.DMA((2, 8, 4)),
            pltpu.SemaphoreType.DMA((2, 8, 4)),
        ],
        compiler_params=pltpu.CompilerParams(collective_id=1, has_side_effects=True,
                                             vmem_limit_bytes=62 * 1024 * 1024),
    )(taps, recorded, weight, *tables)


def store(first, second, first_out, second_out, sem):
    copies = [pltpu.make_async_copy(src, dst, sem.at[k])
              for k, (src, dst) in enumerate(((first, first_out), (second, second_out)))]
    for copy in copies:
        copy.start()
    for copy in copies:
        copy.wait()


def stored(first, second):
    shape = jax.ShapeDtypeStruct(first.shape, F32)
    return pl.pallas_call(
        store,
        name="store",
        out_shape=(shape, shape),
        in_specs=[pl.BlockSpec(memory_space=pl.ANY)] * 2,
        out_specs=(pl.BlockSpec(memory_space=pltpu.HBM),) * 2,
        scratch_shapes=[pltpu.SemaphoreType.DMA((2,))],
        compiler_params=pltpu.CompilerParams(vmem_limit_bytes=2 * 1024 * 1024),
    )(first, second)


def body(recorded, spectral_weight, psf_taps):
    taps = jnp.transpose(psf_taps, (1, 0, 2))
    return stored(*whole(recorded[0], spectral_weight[0], taps))


def solution(mesh):
    return jax.shard_map(
        body,
        mesh=mesh,
        in_specs=(P("view", "pencil", None, None), P("view", None, "pencil", None), P()),
        out_specs=(P("pencil", "view", None), P("pencil", "view", None)),
        check_vma=False,
    )
```

```python
import functools

import jax
import jax.numpy as jnp
import numpy as np
from jax import lax
from jax.experimental import pallas as pl
from jax.experimental.pallas import tpu as pltpu
from jax.sharding import PartitionSpec as P

ITERS = 2
UNROLL = 4
LATE = (3, 7, 11)
MESH_ID = pl.DeviceIdType.MESH
F32 = jnp.float32
BF16 = jnp.bfloat16
SIDES = [(dv, dp) for dp in (-1, 1, 0) for dv in (0, -1, 1) if (dv, dp) != (0, 0)]
SLOT = {side: k for k, side in enumerate(SIDES)}


def halves(value):
    high = value.astype(BF16)
    return high, (value - high.astype(F32)).astype(BF16)


def dot(left, right):
    return jnp.dot(left, right, preferred_element_type=F32)


def two_terms(table):
    high = table.astype(jnp.bfloat16)
    low = (table - high.astype(np.float64)).astype(jnp.bfloat16)
    return [high, low]


def transform_tables(n, nx):
    at = np.arange(n)
    phase = 2.0 * np.pi * (at[:, None] * at[None, :] % n) / n
    cosine, sine = np.cos(phase), np.sin(phase)
    q = n // 4
    rows = np.concatenate([cosine.reshape(4, q, n), sine.reshape(4, q, n)], axis=1)

    x, c = np.arange(nx)[:, None], np.arange(nx // 2)[None, :]
    wave = 2.0 * np.pi * (x * c % nx) / nx
    sign = np.where(x % 2 == 0, 1.0, -1.0)
    columns = np.concatenate([np.cos(wave), np.where(c == 0, sign, -np.sin(wave))], axis=1)
    scale = 1.0 / (float(n) * n * nx)
    back_re = np.where(c == 0, 1.0, 2.0 * np.cos(wave)).T
    back_im = np.where(c == 0, sign, -2.0 * np.sin(wave)).T
    columns_back = np.concatenate([back_re, back_im], axis=0) * scale

    index = np.arange(2 * n)
    part, depth = index % 8 // 4, index // 8 * 4 + index % 4
    c_z, s_z = cosine[:, depth], sine[:, depth]
    depth_table = np.concatenate(
        [np.where(part == 0, c_z, s_z), np.where(part == 0, -s_z, c_z)], axis=0)

    m = np.arange(n // 2)
    back = []
    for core in range(2):
        ky = m // 2 * 4 + 2 * core + m % 2
        back.append(np.concatenate([cosine[:, ky], sine[:, ky]], axis=1))
    return [t for table in (rows, columns, depth_table, np.stack(back), columns_back)
            for t in two_terms(table)]


def right3(high, low, right):
    r_high, r_low = halves(right)
    return dot(high, r_high) + (dot(high, r_low) + dot(low, r_high))


def left3(left, high, low):
    l_high, l_low = halves(left)
    return dot(l_high, high) + (dot(l_high, low) + dot(l_low, high))


def reversal(n):
    total = lax.broadcasted_iota(jnp.int32, (n, n), 0) + lax.broadcasted_iota(jnp.int32, (n, n), 1)
    return jnp.where((total == 0) | (total == n), 1.0, 0.0).astype(BF16)


def moved_right(value, table):
    high, low = halves(value)
    return dot(high, table) + dot(low, table)


def moved_left(table, value):
    high, low = halves(value)
    return dot(table, high) + dot(table, low)


def dot3(left, right_high, right_low):
    high, low = halves(left)
    return dot(high, right_high) + (dot(high, right_low) + dot(low, right_high))


def kernel(views, pencils, taps, slab_ref, weight_ref, *refs):
    table_refs, refs = refs[:10], refs[10:]
    (out, out2, slab, weight, csh, csl, dxh, dxl, mh, ml, cyh, cyl, dih, dil,
     xh, xl, msg, got, wsend, wgot, we, wm, mth, mtl, g, gr, gsh, gsl, fs, gm, fr, pj, r1, r2,
     stacked, est, zed, mid, spread, acc, rz, rs, es, er, cs, strip, th, tl, ah, al,
     ssem, rsem, lsem, load_sem, share_sem, send_sem, recv_sem) = refs
    n = 4 * pencils
    q = n // 4
    half = pencils // 2
    v, p = lax.axis_index("view"), lax.axis_index("pencil")
    core = lax.rem(v, 2)
    mate = v + 1 - 2 * core
    far = lax.rem(v + 2, 4)
    mirror = pencils - 1 - p
    mirror0 = lax.rem(pencils - p, pencils)
    own_mirror = (p == 0) | (p == half)

    tables = [csh, csl, dxh, dxl, mh, ml, cyh, cyl, dih, dil]
    loads = [pltpu.make_async_copy(src, dst, load_sem.at[k])
             for k, (src, dst) in enumerate(zip(table_refs, tables))]
    slab_load = pltpu.make_async_copy(slab_ref, slab, load_sem.at[10])
    weight_loads = [pltpu.make_async_copy(weight_ref.at[:, :, pl.ds(128 * h, 128)], weight.at[h], load_sem.at[11 + h])
                    for h in range(2)]
    slab_load.start()
    for load in loads[2:4] + weight_loads + loads[:2] + loads[4:]:
        load.start()
    flat = [weight.at[h].reshape(4 * n, 128) for h in range(2)]

    def weight_rows(h, j):
        return flat[h][pl.ds(j, n, stride=4), :]

    depth, rows, width = 4, q, slab.shape[-1]
    frame = rows + 16

    def exists(side):
        v1, p1 = v + side[0], p + side[1]
        return (v1 >= 0) & (v1 < views) & (p1 >= 0) & (p1 < pencils)

    def back(side):
        return (-side[0], -side[1])

    def each(sides, action):
        for side in sides:
            @pl.when(exists(side))
            def _(side=side):
                action(side)

    est[...] = jnp.zeros_like(est)
    rz[...] = jnp.zeros_like(rz)
    rs[...] = jnp.zeros_like(rs)

    barrier = pltpu.get_barrier_semaphore()

    def greet(i, carry):
        pl.semaphore_signal(barrier, inc=1, device_id=(v, lax.rem(p + i, pencils)), device_id_type=MESH_ID)
        return carry

    lax.fori_loop(1, pencils, greet, 0, unroll=7)

    def greet_far(i, carry):
        pl.semaphore_signal(barrier, inc=1, device_id=(far, lax.rem(p + i, pencils)), device_id_type=MESH_ID)
        return carry

    lax.fori_loop(0, pencils, greet_far, 0, unroll=8)
    for other in (mate, lax.rem(mate + 2, 4)):
        pl.semaphore_signal(barrier, inc=1, device_id=(other, p), device_id_type=MESH_ID)
    corners = [side for side in SIDES if side[0] != 0 and side[1] != 0]

    def greet_corner(side):
        pl.semaphore_signal(barrier, inc=1, device_id=(v + side[0], p + side[1]), device_id_type=MESH_ID)

    each(corners, greet_corner)
    expected = 2 * pencils + 1 + sum(exists(side).astype(jnp.int32) for side in corners)

    slab_load.wait()
    loads[2].wait()
    loads[3].wait()
    for z in range(4):
        xh[z], xl[z] = halves(left3(slab[z], dxh[...], dxl[...]))
    mid[...] = jnp.zeros_like(mid)
    for load in weight_loads + loads[:2]:
        load.wait()

    def remote(src, dst, k, device):
        return pltpu.make_async_remote_copy(
            src_ref=src, dst_ref=dst, send_sem=ssem.at[k], recv_sem=rsem.at[k],
            device_id=device, device_id_type=MESH_ID)

    lane0 = lax.broadcasted_iota(jnp.int32, (n, 128), 1) == 0

    for j in range(4):
        receiver = mirror0 if j == 0 else mirror
        pick = lane0 & (receiver < half)
        wsend[j] = jnp.where(pick, weight_rows(0, j), weight_rows(1, j))

    pl.semaphore_wait(barrier, expected)
    w_rest = remote(wsend.at[pl.ds(1, 3)], wgot.at[pl.ds(1, 3)], 1, (v, mirror))
    w_first = remote(wsend.at[0], wgot.at[0], 2, (v, mirror0))
    w_local = pltpu.make_async_copy(wsend.at[0], wgot.at[0], lsem.at[0])
    w_rest.start()

    @pl.when(jnp.logical_not(own_mirror))
    def _():
        w_first.start()

    @pl.when(own_mirror)
    def _():
        w_local.start()

    lane_q = lax.broadcasted_iota(jnp.int32, (q, 128), 1) == 0
    row_q = lax.broadcasted_iota(jnp.int32, (q, 128), 0)

    group = pencils // 4
    for step in range(4):
        b = lax.rem(p // group + step, 4)
        first = b < 2
        for z in range(4):
            both = (dot(csh[b], xh[z]) + (dot(csh[b], xl[z]) + dot(csl[b], xh[z])))
            c_re, c_im = both[:q, :128], both[:q, 128:]
            s_re, s_im = both[q:, :128], both[q:, 128:]
            re, im = c_re + s_im, c_im - s_re
            re0 = jnp.where(first, c_re, c_im)
            im0 = jnp.where(first, -s_re, -s_im)
            im0 = jnp.where((row_q == 0) & (b == 0), c_im, im0)
            im0 = jnp.where((row_q == 0) & (b == 2), c_re, im0)
            at = pl.multiple_of(b * (q * 8), q * 8)
            msg[pl.ds(at + z, q, stride=8), :] = jnp.where(lane_q, re0, re)
            msg[pl.ds(at + 4 + z, q, stride=8), :] = jnp.where(lane_q, im0, im)

        def send_chunk(i, carry, b=b):
            peer = b * group + lax.rem(p + i, group)
            at = pl.multiple_of(peer * 32, 32)

            @pl.when(peer != p)
            def _():
                remote(msg.at[pl.ds(at, 32)], got.at[p], 0, (v, peer)).start()
            return carry

        lax.fori_loop(0, group, send_chunk, 0, unroll=2)

    own = pltpu.make_async_copy(msg.at[pl.ds(pl.multiple_of(p * 32, 32), 32)], got.at[p], lsem.at[1])
    own.start()

    def quarter_of(view):
        return slab.at[:, pl.ds(pl.multiple_of(view * q, q), q), :]

    shares = [pltpu.make_async_remote_copy(
        src_ref=quarter_of(lax.rem(v + d, views)), dst_ref=stacked.at[v],
        send_sem=share_sem.at[0, d - 1], recv_sem=share_sem.at[1, d - 1],
        device_id=(lax.rem(v + d, views), p), device_id_type=MESH_ID) for d in range(1, 4)]
    for share in shares:
        share.start()
    own_share = pltpu.make_async_copy(quarter_of(v), stacked.at[v], lsem.at[3])
    own_share.start()

    for load in loads[4:]:
        load.wait()
    mth[...] = mh[...].astype(F32).T.astype(BF16)
    mtl[...] = ml[...].astype(F32).T.astype(BF16)
    def band(v, carry):
        at = (lax.broadcasted_iota(jnp.int32, (width, width), 0)
              - lax.broadcasted_iota(jnp.int32, (width, width), 1))
        table, turned = jnp.zeros((width, width), F32), jnp.zeros((width, width), F32)
        for t in range(9):
            tap = taps[2, v, t]
            table = jnp.where(at == t - 4, tap, table)
            turned = jnp.where(at == 4 - t, tap, turned)
        whole_sum = 1.0
        for axis in range(3):
            axis_sum = taps[axis, v, 0]
            for t in range(1, 9):
                axis_sum = axis_sum + taps[axis, v, t]
            whole_sum = whole_sum * axis_sum
        th[v], tl[v] = halves(table / whole_sum)
        ah[v], al[v] = halves(turned / whole_sum)
        return carry

    lax.fori_loop(0, views, band, 0)

    w_rest.wait_recv()

    @pl.when(jnp.logical_not(own_mirror))
    def _():
        w_first.wait_recv()

    @pl.when(own_mirror)
    def _():
        w_local.wait()

    turn_z, turn_x = reversal(n), reversal(128)
    for j in range(4):
        mine = jnp.where(lane0 & (p >= half), weight_rows(1, j), weight_rows(0, j))
        turned = moved_left(turn_z, moved_right(wgot[(4 - j) % 4], turn_x))
        we[j] = 0.5 * (mine + turned)

    @pl.when(own_mirror)
    def _():
        first = (lax.broadcasted_iota(jnp.int32, (n, 128), 0) * 0 + p) == 0
        other = jnp.where(first, weight_rows(1, 0), weight_rows(0, 0))
        other = 0.5 * (other + moved_left(turn_z, other))
        main = we[0]
        we[0] = jnp.where(lane0, 0.5 * (main + other), main)
        wm[...] = jnp.where(lane0, 0.5 * (main - other), 0.0)

    own.wait()
    remote(got.at[pl.ds(0, pencils - 1)], got.at[pl.ds(0, pencils - 1)], 0, (v, mirror)).wait_recv()

    def pair_spectra(pair):
        block = got[:, pl.ds(pl.multiple_of(16 * pair, 16), 16), :]
        return [block[:, 8 * k:8 * k + 8, :].reshape(2 * n, 128) for k in range(2)]

    def weigh(pair):
        f = right3(mh[...], ml[...], jnp.concatenate(pair_spectra(pair), axis=1))
        for k in range(2):
            j = 2 * pair + k
            for part in range(2):
                g[j, part * n:(part + 1) * n, :] = (
                    f[part * n:(part + 1) * n, 128 * k:128 * k + 128] * we[j])

        @pl.when(own_mirror & (pair == 0))
        def _():
            turned = moved_left(turn_z, jnp.concatenate([f[:n, :128], f[n:, :128]], axis=1))
            g[0, :n, :] = g[0, :n, :] + turned[:, :128] * wm[...]
            g[0, n:, :] = g[0, n:, :] - turned[:, 128:] * wm[...]

    weigh(1 - core)
    pair_sum = remote(g.at[pl.ds(2 - 2 * core, 2)], gr, 3, (mate, p))
    pair_sum.start()
    weigh(core)
    pair_sum.wait_recv()
    gsh[...], gsl[...] = halves(jnp.concatenate(
        [g[2 * core] + gr[0], g[2 * core + 1] + gr[1]], axis=1))

    kept = v // 2
    away = 1 - kept

    def rows_of(peer):
        return pl.ds(pl.multiple_of(peer * 8, 8), 8)

    for step in range(2):
        b = lax.rem(p // half + step, 2)
        at = pl.multiple_of(b * n, n)
        block = pl.ds(at, n)
        f = (dot(mth[block, :], gsh[...])
             + (dot(mth[block, :], gsl[...]) + dot(mtl[block, :], gsh[...])))
        for k in range(2):
            fs[k, block, :] = f[:, 128 * k:128 * k + 128]
        for x in range(2):
            for k in range(2):
                for part in range(2):
                    for zz in range(2):
                        gm[x, pl.ds(at + (4 * k + 2 * part + zz), half, stride=8), :] = (
                            fs[k, pl.ds(at + (4 * part + 2 * x + zz), half, stride=8), :])

        def send_back(i, carry, b=b):
            peer = b * half + lax.rem(p + i, half)

            @pl.when(peer != p)
            def _():
                remote(gm.at[kept, rows_of(peer)], fr.at[kept, rows_of(p)], 4, (v, peer)).start()

            remote(gm.at[away, rows_of(peer)], fr.at[kept, rows_of(p)], 7, (far, peer)).start()
            return carry

        lax.fori_loop(0, half, send_back, 0, unroll=2)

    own_back = pltpu.make_async_copy(gm.at[kept, rows_of(p)], fr.at[kept, rows_of(p)], lsem.at[2])
    own_back.start()
    own_back.wait()
    most = fr.at[kept, pl.ds(0, 8 * (pencils - 1))]
    remote(most, most, 4, (v, mirror)).wait_recv()
    remote(fr.at[away], fr.at[away], 7, (far, p)).wait_recv()

    m = lax.broadcasted_iota(jnp.int32, (n // 2, 128), 0)
    ky = m // 2 * 4 + 2 * core + lax.rem(m, 2)
    lane_m = lax.broadcasted_iota(jnp.int32, (n // 2, 128), 1) == 0
    low, high = (ky > 0) & (ky < n // 2), ky > n // 2
    for zz in range(2):
        re = fr[0, pl.ds(zz, n // 2, stride=4), :] + fr[1, pl.ds(zz, n // 2, stride=4), :]
        im = fr[0, pl.ds(2 + zz, n // 2, stride=4), :] + fr[1, pl.ds(2 + zz, n // 2, stride=4), :]
        zero = jnp.zeros_like(re)
        v1 = jnp.where(low, 2.0 * re, jnp.where(ky == 0, re, jnp.where(ky == n // 2, im, zero)))
        v2 = jnp.where(high, 2.0 * re, jnp.where(ky == 0, im, jnp.where(ky == n // 2, re, zero)))
        b1 = jnp.where(low, -2.0 * im, zero)
        b2 = jnp.where(high, -2.0 * im, zero)
        top = jnp.concatenate([jnp.where(lane_m, v1, re), jnp.where(lane_m, v2, im)], axis=1)
        bottom = jnp.concatenate([jnp.where(lane_m, b1, -im), jnp.where(lane_m, b2, re)], axis=1)
        u = right3(cyh[core], cyl[core], jnp.concatenate([top, bottom], axis=0))
        field = left3(u, dih[...], dil[...])
        for quarter in range(4):
            pj[quarter // 2, quarter % 2, zz] = field[quarter * q:(quarter + 1) * q]
        remote(pj.at[:, 1 - core, zz], r1.at[:, zz], 5 + 3 * zz, (mate, p)).start()

    def near(zz):
        return remote(pj.at[:, 1 - core, zz], r1.at[:, zz], 5 + 3 * zz, (mate, p))

    def long(zz):
        return remote(r1.at[away, zz], r2.at[zz], 6 + 3 * zz, (far, p))

    for zz in range(2):
        near(zz).wait_recv()
        r1[:, zz] = r1[:, zz] + pj[:, core, zz]
        long(zz).start()

    def est_copy(side, z):
        dv, dp = side
        own_rows = pl.ds(8, rows)
        return pltpu.make_async_remote_copy(
            src_ref=es.at[(dv + 1) // 2, z] if dv else est.at[depth + z, :, own_rows, :],
            dst_ref=er.at[SLOT[back(side)], z] if dv else est.at[depth * (1 - dp) + z, :, own_rows, :],
            send_sem=send_sem.at[0, SLOT[side], z],
            recv_sem=recv_sem.at[0, SLOT[back(side)], z],
            device_id=(v + dv, p + dp),
            device_id_type=MESH_ID,
        )

    def acc_copy(side, z):
        dv, dp = side
        slot = SLOT[back(side)]
        landing = rz.at[0 if dp == 1 else 1, z] if dv == 0 else rs.at[slot, z]
        return pltpu.make_async_remote_copy(
            src_ref=cs.at[(dv + 1) // 2, dp + 1, z] if dv else acc.at[depth * (1 + dp) + z, :, pl.ds(8, rows), :],
            dst_ref=landing,
            send_sem=send_sem.at[1, SLOT[side], z],
            recv_sem=recv_sem.at[1, slot, z],
            device_id=(v + dv, p + dp),
            device_id_type=MESH_ID,
        )

    def est_wait(side, z):
        dv, dp = side
        plane = depth * (1 + dp) + z
        landing = er.at[SLOT[side], z] if dv else est.at[plane, :, pl.ds(8, rows), :]
        pltpu.make_async_remote_copy(
            src_ref=landing, dst_ref=landing, send_sem=send_sem.at[0, SLOT[side], z],
            recv_sem=recv_sem.at[0, SLOT[side], z], device_id=(v + dv, p + dp),
            device_id_type=MESH_ID).wait_recv()
        if dv:
            for h in range(2):
                est[plane, h, pl.ds(4 if dv < 0 else rows + 8, 4), :] = er[SLOT[side], z, pl.ds(4 * h, 4), :]

    def acc_wait(side, z):
        dv, dp = side
        landing = rz.at[0 if dp == -1 else 1, z] if dv == 0 else rs.at[SLOT[side], z]
        pltpu.make_async_remote_copy(
            src_ref=landing, dst_ref=landing, send_sem=send_sem.at[1, SLOT[side], z],
            recv_sem=recv_sem.at[1, SLOT[side], z], device_id=(v + dv, p + dp),
            device_id_type=MESH_ID).wait_recv()

    def send_estimate(z):
        for h in range(2):
            es[0, z, pl.ds(4 * h, 4), :] = est[depth + z, h, pl.ds(8, 4), :]
            es[1, z, pl.ds(4 * h, 4), :] = est[depth + z, h, pl.ds(rows + 4, 4), :]
        each(SIDES, lambda side: est_copy(side, z).start())

    def send_correction(z):
        for dp in (-1, 0, 1):
            for h in range(2):
                plane = depth * (1 + dp) + z
                cs[0, dp + 1, z, pl.ds(4 * h, 4), :] = acc[plane, h, pl.ds(4, 4), :]
                cs[1, dp + 1, z, pl.ds(4 * h, 4), :] = acc[plane, h, pl.ds(rows + 8, 4), :]
        each(SIDES, lambda side: acc_copy(side, z).start())

    def every_plane(action, planes):
        def at_plane(z, carry):
            each(SIDES, lambda side: action(side, z))
            return carry

        lax.fori_loop(0, planes, at_plane, 0)

    def start_estimate(z, plane):
        out[z] = plane
        for h in range(2):
            half_plane = plane[:, h * 128:(h + 1) * 128]
            est[depth + z, h, pl.ds(8, rows), :] = 0.1 + (
                jnp.maximum(half_plane, 0.0) + jnp.log1p(jnp.exp(-jnp.abs(half_plane))))
        send_estimate(z)

    for zz in range(2):
        start_estimate(2 * kept + zz, r1[kept, zz])
    for zz in range(2):
        long(zz).wait_recv()
        start_estimate(2 * away + zz, r2[zz])
    own_share.wait()
    for share in shares:
        share.wait_recv()

    def early_step(w, carry):
        for z in range(depth):
            total = None
            for t in range(9):
                if z + t not in LATE:
                    term = taps[0, w, t] * est[z + t]
                    total = term if total is None else total + term
            zed[w, z] = total
        return carry

    def view_step(w, carry):
        for z in range(depth):
            total = zed[w, z]
            for plane in LATE:
                if 0 <= plane - z <= 8:
                    total = total + taps[0, w, plane - z] * est[plane]
            zed[w, z] = total
        sides = []
        for h in range(2):
            planes = []
            for z in range(depth):
                total = taps[1, w, 0] * zed[w, z, h, pl.ds(4, rows), :]
                for t in range(1, 9):
                    total = total + taps[1, w, t] * zed[w, z, h, pl.ds(4 + t, rows), :]
                planes.append(total)
            sides.append(jnp.concatenate(planes, axis=0))
        blurred = dot3(jnp.concatenate(sides, axis=1), th[w], tl[w])
        ratio = stacked[w].reshape(depth * rows, width) / blurred
        turned = dot3(ratio, ah[w], al[w])
        for z in range(depth):
            for h in range(2):
                mid[w, z, h, pl.ds(16, rows), :] = turned[z * rows:(z + 1) * rows, h * 128:(h + 1) * 128]
        for z in range(depth):
            for h in range(2):
                total = taps[1, w, 8] * mid[w, z, h, pl.ds(4, frame), :]
                for t in range(1, 9):
                    total = total + taps[1, w, 8 - t] * mid[w, z, h, pl.ds(4 + t, frame), :]
                spread[w, z, h] = total
        return carry

    def gather_planes(planes):
        for zo in planes:
            total = None
            for v in range(views):
                for zs in range(depth):
                    if 0 <= zo - zs <= 8:
                        term = taps[0, v, zo - zs] * spread[v, zs]
                        total = term if total is None else total + term
            acc[zo] = total

    def iteration(step, carry):
        every_plane(est_wait, depth - 1)
        lax.fori_loop(0, views, early_step, 0)
        each(SIDES, lambda side: est_wait(side, depth - 1))
        lax.fori_loop(0, views, view_step, 0, unroll=UNROLL)
        for z in range(depth):
            gather_planes([z, 2 * depth + z, depth + z])
            send_correction(z)

        def finish_plane(z, carry):
            each(SIDES, lambda side: acc_wait(side, z))
            each(SIDES, lambda side: est_copy(side, z).wait_send())
            for end in (-1, 1):
                strip[...] = rs[SLOT[(end, 0)], z] + (rs[SLOT[(end, -1)], z] + rs[SLOT[(end, 1)], z])
                at = pl.ds(8 if end < 0 else rows + 4, 4)
                for h in range(2):
                    acc[depth + z, h, at, :] = acc[depth + z, h, at, :] + strip[pl.ds(4 * h, 4), :]
            for h in range(2):
                total = acc[depth + z, h, pl.ds(8, rows), :] + (rz[0, z, h] + rz[1, z, h])
                est[depth + z, h, pl.ds(8, rows), :] = (
                    est[depth + z, h, pl.ds(8, rows), :] * (total * (1.0 / views)))

            @pl.when(step < ITERS - 1)
            def _():
                send_estimate(z)
            return carry

        lax.fori_loop(0, depth, finish_plane, 0)
        every_plane(lambda side, z: acc_copy(side, z).wait_send(), depth)
        return carry

    lax.fori_loop(0, ITERS, iteration, 0)
    for h in range(2):
        out2[:, :, h * 128:(h + 1) * 128] = est[pl.ds(depth, depth), h, pl.ds(8, rows), :]

    w_rest.wait_send()
    sent = msg.at[pl.ds(0, 32 * (pencils - 1))]
    remote(sent, sent, 0, (v, mirror)).wait_send()
    pair_sum.wait_send()
    sent_back = gm.at[kept, pl.ds(0, 8 * (pencils - 1))]
    remote(sent_back, sent_back, 4, (v, mirror)).wait_send()
    remote(gm.at[away], gm.at[away], 7, (far, p)).wait_send()
    for zz in range(2):
        near(zz).wait_send()
        long(zz).wait_send()

    @pl.when(jnp.logical_not(own_mirror))
    def _():
        w_first.wait_send()
    for share in shares:
        share.wait_send()


def whole(recorded, weight, taps):
    views, pencils = lax.axis_size("view"), lax.axis_size("pencil")
    n, nx = 4 * pencils, recorded.shape[-1]
    q, depth = n // 4, 4
    frame = q + 16
    vmem, left = pl.BlockSpec(memory_space=pltpu.VMEM), pl.BlockSpec(memory_space=pltpu.HBM)
    tables = [jnp.asarray(t) for t in transform_tables(n, nx)]
    block = pltpu.VMEM((depth, q, nx), F32)
    return pl.pallas_call(
        functools.partial(kernel, views, pencils),
        name="join_and_deconvolve",
        out_shape=(block, block),
        in_specs=[pl.BlockSpec(memory_space=pltpu.SMEM)] + [left] * (2 + len(tables)),
        out_specs=(vmem, vmem),
        scratch_shapes=[
            pltpu.VMEM((4, n, nx), F32),
            pltpu.VMEM((2, n, 4, 128), F32),
            *[pltpu.VMEM(t.shape, t.dtype) for t in tables],
            pltpu.VMEM((4, n, nx), BF16),
            pltpu.VMEM((4, n, nx), BF16),
            pltpu.VMEM((8 * n, 128), F32),
            pltpu.VMEM((pencils, 32, 128), F32),
            pltpu.VMEM((4, n, 128), F32),
            pltpu.VMEM((4, n, 128), F32),
            pltpu.VMEM((4, n, 128), F32),
            pltpu.VMEM((n, 128), F32),
            pltpu.VMEM((2 * n, 2 * n), BF16),
            pltpu.VMEM((2 * n, 2 * n), BF16),
            pltpu.VMEM((4, 2 * n, 128), F32),
            pltpu.VMEM((2, 2 * n, 128), F32),
            pltpu.VMEM((2 * n, 256), BF16),
            pltpu.VMEM((2 * n, 256), BF16),
            pltpu.VMEM((2, 2 * n, 128), F32),
            pltpu.VMEM((2, 8 * pencils, 128), F32),
            pltpu.VMEM((2, 8 * pencils, 128), F32),
            pltpu.VMEM((2, 2, 2, q, nx), F32),
            pltpu.VMEM((2, 2, q, nx), F32),
            pltpu.VMEM((2, q, nx), F32),
            pltpu.VMEM((views, depth, q, nx), F32),
            pltpu.VMEM((3 * depth, 2, frame, 128), F32),
            pltpu.VMEM((views, depth, 2, frame, 128), F32),
            pltpu.VMEM((views, depth, 2, frame + 16, 128), F32),
            pltpu.VMEM((views, depth, 2, frame, 128), F32),
            pltpu.VMEM((3 * depth, 2, frame, 128), F32),
            pltpu.VMEM((2, depth, 2, q, 128), F32),
            pltpu.VMEM((8, depth, 8, 128), F32),
            pltpu.VMEM((2, depth, 8, 128), F32),
            pltpu.VMEM((8, depth, 8, 128), F32),
            pltpu.VMEM((2, 3, depth, 8, 128), F32),
            pltpu.VMEM((8, 128), F32),
            *[pltpu.VMEM((views, nx, nx), BF16)] * 4,
            pltpu.SemaphoreType.DMA((10,)),
            pltpu.SemaphoreType.DMA((10,)),
            pltpu.SemaphoreType.DMA((4,)),
            pltpu.SemaphoreType.DMA((13,)),
            pltpu.SemaphoreType.DMA((2, 3)),
            pltpu.SemaphoreType.DMA((2, 8, 4)),
            pltpu.SemaphoreType.DMA((2, 8, 4)),
        ],
        compiler_params=pltpu.CompilerParams(collective_id=1, has_side_effects=True,
                                             vmem_limit_bytes=62 * 1024 * 1024),
    )(taps, recorded, weight, *tables)


def store(first, second, first_out, second_out, sem):
    copies = [pltpu.make_async_copy(src, dst, sem.at[k])
              for k, (src, dst) in enumerate(((first, first_out), (second, second_out)))]
    for copy in copies:
        copy.start()
    for copy in copies:
        copy.wait()


def stored(first, second):
    shape = jax.ShapeDtypeStruct(first.shape, F32)
    return pl.pallas_call(
        store,
        name="store",
        out_shape=(shape, shape),
        in_specs=[pl.BlockSpec(memory_space=pl.ANY)] * 2,
        out_specs=(pl.BlockSpec(memory_space=pltpu.HBM),) * 2,
        scratch_shapes=[pltpu.SemaphoreType.DMA((2,))],
        compiler_params=pltpu.CompilerParams(vmem_limit_bytes=2 * 1024 * 1024),
    )(first, second)


def body(recorded, spectral_weight, psf_taps):
    taps = jnp.transpose(psf_taps, (1, 0, 2))
    return stored(*whole(recorded[0], spectral_weight[0], taps))


def solution(mesh):
    return jax.shard_map(
        body,
        mesh=mesh,
        in_specs=(P("view", "pencil", None, None), P("view", None, "pencil", None), P()),
        out_specs=(P("pencil", "view", None), P("pencil", "view", None)),
        check_vma=False,
    )
```

```python
import functools

import jax
import jax.numpy as jnp
import numpy as np
from jax import lax
from jax.experimental import pallas as pl
from jax.experimental.pallas import tpu as pltpu
from jax.sharding import PartitionSpec as P

ITERS = 2
UNROLL = 4
LATE = (3, 7, 11)
MESH_ID = pl.DeviceIdType.MESH
F32 = jnp.float32
BF16 = jnp.bfloat16
SIDES = [(dv, dp) for dp in (-1, 1, 0) for dv in (0, -1, 1) if (dv, dp) != (0, 0)]
SLOT = {side: k for k, side in enumerate(SIDES)}


def halves(value):
    high = value.astype(BF16)
    return high, (value - high.astype(F32)).astype(BF16)


def dot(left, right):
    return jnp.dot(left, right, preferred_element_type=F32)


def two_terms(table):
    high = table.astype(jnp.bfloat16)
    low = (table - high.astype(np.float64)).astype(jnp.bfloat16)
    return [high, low]


def transform_tables(n, nx):
    at = np.arange(n)
    phase = 2.0 * np.pi * (at[:, None] * at[None, :] % n) / n
    cosine, sine = np.cos(phase), np.sin(phase)
    q = n // 4
    rows = np.concatenate([cosine.reshape(4, q, n), sine.reshape(4, q, n)], axis=1)

    x, c = np.arange(nx)[:, None], np.arange(nx // 2)[None, :]
    wave = 2.0 * np.pi * (x * c % nx) / nx
    sign = np.where(x % 2 == 0, 1.0, -1.0)
    columns = np.concatenate([np.cos(wave), np.where(c == 0, sign, -np.sin(wave))], axis=1)
    scale = 1.0 / (float(n) * n * nx)
    back_re = np.where(c == 0, 1.0, 2.0 * np.cos(wave)).T
    back_im = np.where(c == 0, sign, -2.0 * np.sin(wave)).T
    columns_back = np.concatenate([back_re, back_im], axis=0) * scale

    index = np.arange(2 * n)
    part, depth = index % 8 // 4, index // 8 * 4 + index % 4
    c_z, s_z = cosine[:, depth], sine[:, depth]
    depth_table = np.concatenate(
        [np.where(part == 0, c_z, s_z), np.where(part == 0, -s_z, c_z)], axis=0)

    m = np.arange(n // 2)
    back = []
    for core in range(2):
        ky = m // 2 * 4 + 2 * core + m % 2
        back.append(np.concatenate([cosine[:, ky], sine[:, ky]], axis=1))
    return [t for table in (rows, columns, depth_table, np.stack(back), columns_back)
            for t in two_terms(table)]


def right3(high, low, right):
    r_high, r_low = halves(right)
    return dot(high, r_high) + (dot(high, r_low) + dot(low, r_high))


def left3(left, high, low):
    l_high, l_low = halves(left)
    return dot(l_high, high) + (dot(l_high, low) + dot(l_low, high))


def reversal(n):
    total = lax.broadcasted_iota(jnp.int32, (n, n), 0) + lax.broadcasted_iota(jnp.int32, (n, n), 1)
    return jnp.where((total == 0) | (total == n), 1.0, 0.0).astype(BF16)


def moved_right(value, table):
    high, low = halves(value)
    return dot(high, table) + dot(low, table)


def moved_left(table, value):
    high, low = halves(value)
    return dot(table, high) + dot(table, low)


def dot3(left, right_high, right_low):
    high, low = halves(left)
    return dot(high, right_high) + (dot(high, right_low) + dot(low, right_high))


def kernel(views, pencils, taps, slab_ref, weight_ref, *refs):
    table_refs, refs = refs[:10], refs[10:]
    (out, out2, slab, weight, csh, csl, dxh, dxl, mh, ml, cyh, cyl, dih, dil,
     xh, xl, msg, got, wsend, wgot, we, wm, mth, mtl, g, gr, gsh, gsl, fs, gm, fr, pj, r1, r2,
     stacked, est, zed, mid, spread, acc, rz, rs, es, er, cs, strip, th, tl, ah, al,
     ssem, rsem, lsem, load_sem, share_sem, send_sem, recv_sem) = refs
    n = 4 * pencils
    q = n // 4
    half = pencils // 2
    v, p = lax.axis_index("view"), lax.axis_index("pencil")
    core = lax.rem(v, 2)
    mate = v + 1 - 2 * core
    far = lax.rem(v + 2, 4)
    mirror = pencils - 1 - p
    mirror0 = lax.rem(pencils - p, pencils)
    own_mirror = (p == 0) | (p == half)

    tables = [csh, csl, dxh, dxl, mh, ml, cyh, cyl, dih, dil]
    loads = [pltpu.make_async_copy(src, dst, load_sem.at[k])
             for k, (src, dst) in enumerate(zip(table_refs, tables))]
    slab_load = pltpu.make_async_copy(slab_ref, slab, load_sem.at[10])
    weight_loads = [pltpu.make_async_copy(weight_ref.at[:, :, pl.ds(128 * h, 128)], weight.at[h], load_sem.at[11 + h])
                    for h in range(2)]
    slab_load.start()
    for load in loads[2:4] + weight_loads + loads[:2] + loads[4:]:
        load.start()
    flat = [weight.at[h].reshape(4 * n, 128) for h in range(2)]

    def weight_rows(h, j):
        return flat[h][pl.ds(j, n, stride=4), :]

    depth, rows, width = 4, q, slab.shape[-1]
    frame = rows + 16

    def exists(side):
        v1, p1 = v + side[0], p + side[1]
        return (v1 >= 0) & (v1 < views) & (p1 >= 0) & (p1 < pencils)

    def back(side):
        return (-side[0], -side[1])

    def each(sides, action):
        for side in sides:
            @pl.when(exists(side))
            def _(side=side):
                action(side)

    est[...] = jnp.zeros_like(est)
    rz[...] = jnp.zeros_like(rz)
    rs[...] = jnp.zeros_like(rs)

    barrier = pltpu.get_barrier_semaphore()

    def greet(i, carry):
        pl.semaphore_signal(barrier, inc=1, device_id=(v, lax.rem(p + i, pencils)), device_id_type=MESH_ID)
        return carry

    lax.fori_loop(1, pencils, greet, 0, unroll=7)

    def greet_far(i, carry):
        pl.semaphore_signal(barrier, inc=1, device_id=(far, lax.rem(p + i, pencils)), device_id_type=MESH_ID)
        return carry

    lax.fori_loop(0, pencils, greet_far, 0, unroll=8)
    for other in (mate, lax.rem(mate + 2, 4)):
        pl.semaphore_signal(barrier, inc=1, device_id=(other, p), device_id_type=MESH_ID)
    corners = [side for side in SIDES if side[0] != 0 and side[1] != 0]

    def greet_corner(side):
        pl.semaphore_signal(barrier, inc=1, device_id=(v + side[0], p + side[1]), device_id_type=MESH_ID)

    each(corners, greet_corner)
    expected = 2 * pencils + 1 + sum(exists(side).astype(jnp.int32) for side in corners)

    slab_load.wait()
    loads[2].wait()
    loads[3].wait()
    for z in range(4):
        xh[z], xl[z] = halves(left3(slab[z], dxh[...], dxl[...]))
    mid[...] = jnp.zeros_like(mid)
    for load in weight_loads + loads[:2]:
        load.wait()

    def remote(src, dst, k, device):
        return pltpu.make_async_remote_copy(
            src_ref=src, dst_ref=dst, send_sem=ssem.at[k], recv_sem=rsem.at[k],
            device_id=device, device_id_type=MESH_ID)

    lane0 = lax.broadcasted_iota(jnp.int32, (n, 128), 1) == 0

    for j in range(4):
        receiver = mirror0 if j == 0 else mirror
        pick = lane0 & (receiver < half)
        wsend[j] = jnp.where(pick, weight_rows(0, j), weight_rows(1, j))

    pl.semaphore_wait(barrier, expected)
    w_rest = remote(wsend.at[pl.ds(1, 3)], wgot.at[pl.ds(1, 3)], 1, (v, mirror))
    w_first = remote(wsend.at[0], wgot.at[0], 2, (v, mirror0))
    w_local = pltpu.make_async_copy(wsend.at[0], wgot.at[0], lsem.at[0])
    w_rest.start()

    @pl.when(jnp.logical_not(own_mirror))
    def _():
        w_first.start()

    @pl.when(own_mirror)
    def _():
        w_local.start()

    lane_q = lax.broadcasted_iota(jnp.int32, (q, 128), 1) == 0
    row_q = lax.broadcasted_iota(jnp.int32, (q, 128), 0)

    group = pencils // 4
    for step in range(4):
        b = lax.rem(p // group + step, 4)
        first = b < 2
        for z in range(4):
            both = (dot(csh[b], xh[z]) + (dot(csh[b], xl[z]) + dot(csl[b], xh[z])))
            c_re, c_im = both[:q, :128], both[:q, 128:]
            s_re, s_im = both[q:, :128], both[q:, 128:]
            re, im = c_re + s_im, c_im - s_re
            re0 = jnp.where(first, c_re, c_im)
            im0 = jnp.where(first, -s_re, -s_im)
            im0 = jnp.where((row_q == 0) & (b == 0), c_im, im0)
            im0 = jnp.where((row_q == 0) & (b == 2), c_re, im0)
            at = pl.multiple_of(b * (q * 8), q * 8)
            msg[pl.ds(at + z, q, stride=8), :] = jnp.where(lane_q, re0, re)
            msg[pl.ds(at + 4 + z, q, stride=8), :] = jnp.where(lane_q, im0, im)

        def send_chunk(i, carry, b=b):
            peer = b * group + lax.rem(p + i, group)
            at = pl.multiple_of(peer * 32, 32)

            @pl.when(peer != p)
            def _():
                remote(msg.at[pl.ds(at, 32)], got.at[p], 0, (v, peer)).start()
            return carry

        lax.fori_loop(0, group, send_chunk, 0, unroll=2)

    own = pltpu.make_async_copy(msg.at[pl.ds(pl.multiple_of(p * 32, 32), 32)], got.at[p], lsem.at[1])
    own.start()

    def quarter_of(view):
        return slab.at[:, pl.ds(pl.multiple_of(view * q, q), q), :]

    shares = [pltpu.make_async_remote_copy(
        src_ref=quarter_of(lax.rem(v + d, views)), dst_ref=stacked.at[v],
        send_sem=share_sem.at[0, d - 1], recv_sem=share_sem.at[1, d - 1],
        device_id=(lax.rem(v + d, views), p), device_id_type=MESH_ID) for d in range(1, 4)]
    for share in shares:
        share.start()
    own_share = pltpu.make_async_copy(quarter_of(v), stacked.at[v], lsem.at[3])
    own_share.start()

    for load in loads[4:]:
        load.wait()
    mth[...] = mh[...].astype(F32).T.astype(BF16)
    mtl[...] = ml[...].astype(F32).T.astype(BF16)
    def band(v, carry):
        at = (lax.broadcasted_iota(jnp.int32, (width, width), 0)
              - lax.broadcasted_iota(jnp.int32, (width, width), 1))
        table, turned = jnp.zeros((width, width), F32), jnp.zeros((width, width), F32)
        for t in range(9):
            tap = taps[2, v, t]
            table = jnp.where(at == t - 4, tap, table)
            turned = jnp.where(at == 4 - t, tap, turned)
        whole_sum = 1.0
        for axis in range(3):
            axis_sum = taps[axis, v, 0]
            for t in range(1, 9):
                axis_sum = axis_sum + taps[axis, v, t]
            whole_sum = whole_sum * axis_sum
        th[v], tl[v] = halves(table / whole_sum)
        ah[v], al[v] = halves(turned / whole_sum)
        return carry

    lax.fori_loop(0, views, band, 0)

    w_rest.wait_recv()

    @pl.when(jnp.logical_not(own_mirror))
    def _():
        w_first.wait_recv()

    @pl.when(own_mirror)
    def _():
        w_local.wait()

    turn_z, turn_x = reversal(n), reversal(128)
    for j in range(4):
        mine = jnp.where(lane0 & (p >= half), weight_rows(1, j), weight_rows(0, j))
        turned = moved_left(turn_z, moved_right(wgot[(4 - j) % 4], turn_x))
        we[j] = 0.5 * (mine + turned)

    @pl.when(own_mirror)
    def _():
        first = (lax.broadcasted_iota(jnp.int32, (n, 128), 0) * 0 + p) == 0
        other = jnp.where(first, weight_rows(1, 0), weight_rows(0, 0))
        other = 0.5 * (other + moved_left(turn_z, other))
        main = we[0]
        we[0] = jnp.where(lane0, 0.5 * (main + other), main)
        wm[...] = jnp.where(lane0, 0.5 * (main - other), 0.0)

    own.wait()
    remote(got.at[pl.ds(0, pencils - 1)], got.at[pl.ds(0, pencils - 1)], 0, (v, mirror)).wait_recv()

    def pair_spectra(pair):
        block = got[:, pl.ds(pl.multiple_of(16 * pair, 16), 16), :]
        return [block[:, 8 * k:8 * k + 8, :].reshape(2 * n, 128) for k in range(2)]

    def weigh(pair):
        f = right3(mh[...], ml[...], jnp.concatenate(pair_spectra(pair), axis=1))
        for k in range(2):
            j = 2 * pair + k
            for part in range(2):
                g[j, part * n:(part + 1) * n, :] = (
                    f[part * n:(part + 1) * n, 128 * k:128 * k + 128] * we[j])

        @pl.when(own_mirror & (pair == 0))
        def _():
            turned = moved_left(turn_z, jnp.concatenate([f[:n, :128], f[n:, :128]], axis=1))
            g[0, :n, :] = g[0, :n, :] + turned[:, :128] * wm[...]
            g[0, n:, :] = g[0, n:, :] - turned[:, 128:] * wm[...]

    weigh(1 - core)
    pair_sum = remote(g.at[pl.ds(2 - 2 * core, 2)], gr, 3, (mate, p))
    pair_sum.start()
    weigh(core)
    pair_sum.wait_recv()
    gsh[...], gsl[...] = halves(jnp.concatenate(
        [g[2 * core] + gr[0], g[2 * core + 1] + gr[1]], axis=1))

    kept = v // 2
    away = 1 - kept

    def rows_of(peer):
        return pl.ds(pl.multiple_of(peer * 8, 8), 8)

    for step in range(2):
        b = lax.rem(p // half + step, 2)
        at = pl.multiple_of(b * n, n)
        block = pl.ds(at, n)
        f = (dot(mth[block, :], gsh[...])
             + (dot(mth[block, :], gsl[...]) + dot(mtl[block, :], gsh[...])))
        for k in range(2):
            fs[k, block, :] = f[:, 128 * k:128 * k + 128]
        for x in range(2):
            for k in range(2):
                for part in range(2):
                    for zz in range(2):
                        gm[x, pl.ds(at + (4 * k + 2 * part + zz), half, stride=8), :] = (
                            fs[k, pl.ds(at + (4 * part + 2 * x + zz), half, stride=8), :])

        def send_back(i, carry, b=b):
            peer = b * half + lax.rem(p + i, half)

            @pl.when(peer != p)
            def _():
                remote(gm.at[kept, rows_of(peer)], fr.at[kept, rows_of(p)], 4, (v, peer)).start()

            remote(gm.at[away, rows_of(peer)], fr.at[kept, rows_of(p)], 7, (far, peer)).start()
            return carry

        lax.fori_loop(0, half, send_back, 0, unroll=2)

    own_back = pltpu.make_async_copy(gm.at[kept, rows_of(p)], fr.at[kept, rows_of(p)], lsem.at[2])
    own_back.start()
    own_back.wait()
    most = fr.at[kept, pl.ds(0, 8 * (pencils - 1))]
    remote(most, most, 4, (v, mirror)).wait_recv()
    remote(fr.at[away], fr.at[away], 7, (far, p)).wait_recv()

    m = lax.broadcasted_iota(jnp.int32, (n // 2, 128), 0)
    ky = m // 2 * 4 + 2 * core + lax.rem(m, 2)
    lane_m = lax.broadcasted_iota(jnp.int32, (n // 2, 128), 1) == 0
    low, high = (ky > 0) & (ky < n // 2), ky > n // 2
    for zz in range(2):
        re = fr[0, pl.ds(zz, n // 2, stride=4), :] + fr[1, pl.ds(zz, n // 2, stride=4), :]
        im = fr[0, pl.ds(2 + zz, n // 2, stride=4), :] + fr[1, pl.ds(2 + zz, n // 2, stride=4), :]
        zero = jnp.zeros_like(re)
        v1 = jnp.where(low, 2.0 * re, jnp.where(ky == 0, re, jnp.where(ky == n // 2, im, zero)))
        v2 = jnp.where(high, 2.0 * re, jnp.where(ky == 0, im, jnp.where(ky == n // 2, re, zero)))
        b1 = jnp.where(low, -2.0 * im, zero)
        b2 = jnp.where(high, -2.0 * im, zero)
        top = jnp.concatenate([jnp.where(lane_m, v1, re), jnp.where(lane_m, v2, im)], axis=1)
        bottom = jnp.concatenate([jnp.where(lane_m, b1, -im), jnp.where(lane_m, b2, re)], axis=1)
        u = right3(cyh[core], cyl[core], jnp.concatenate([top, bottom], axis=0))
        field = left3(u, dih[...], dil[...])
        for quarter in range(4):
            pj[quarter // 2, quarter % 2, zz] = field[quarter * q:(quarter + 1) * q]
        remote(pj.at[:, 1 - core, zz], r1.at[:, zz], 5 + 3 * zz, (mate, p)).start()

    def near(zz):
        return remote(pj.at[:, 1 - core, zz], r1.at[:, zz], 5 + 3 * zz, (mate, p))

    def long(zz):
        return remote(r1.at[away, zz], r2.at[zz], 6 + 3 * zz, (far, p))

    for zz in range(2):
        near(zz).wait_recv()
        r1[:, zz] = r1[:, zz] + pj[:, core, zz]
        long(zz).start()

    def est_copy(side, z):
        dv, dp = side
        own_rows = pl.ds(8, rows)
        return pltpu.make_async_remote_copy(
            src_ref=es.at[(dv + 1) // 2, z] if dv else est.at[depth + z, :, own_rows, :],
            dst_ref=er.at[SLOT[back(side)], z] if dv else est.at[depth * (1 - dp) + z, :, own_rows, :],
            send_sem=send_sem.at[0, SLOT[side], z],
            recv_sem=recv_sem.at[0, SLOT[back(side)], z],
            device_id=(v + dv, p + dp),
            device_id_type=MESH_ID,
        )

    def acc_copy(side, z):
        dv, dp = side
        slot = SLOT[back(side)]
        landing = rz.at[0 if dp == 1 else 1, z] if dv == 0 else rs.at[slot, z]
        return pltpu.make_async_remote_copy(
            src_ref=cs.at[(dv + 1) // 2, dp + 1, z] if dv else acc.at[depth * (1 + dp) + z, :, pl.ds(8, rows), :],
            dst_ref=landing,
            send_sem=send_sem.at[1, SLOT[side], z],
            recv_sem=recv_sem.at[1, slot, z],
            device_id=(v + dv, p + dp),
            device_id_type=MESH_ID,
        )

    def est_wait(side, z):
        dv, dp = side
        plane = depth * (1 + dp) + z
        landing = er.at[SLOT[side], z] if dv else est.at[plane, :, pl.ds(8, rows), :]
        pltpu.make_async_remote_copy(
            src_ref=landing, dst_ref=landing, send_sem=send_sem.at[0, SLOT[side], z],
            recv_sem=recv_sem.at[0, SLOT[side], z], device_id=(v + dv, p + dp),
            device_id_type=MESH_ID).wait_recv()
        if dv:
            for h in range(2):
                est[plane, h, pl.ds(4 if dv < 0 else rows + 8, 4), :] = er[SLOT[side], z, pl.ds(4 * h, 4), :]

    def acc_wait(side, z):
        dv, dp = side
        landing = rz.at[0 if dp == -1 else 1, z] if dv == 0 else rs.at[SLOT[side], z]
        pltpu.make_async_remote_copy(
            src_ref=landing, dst_ref=landing, send_sem=send_sem.at[1, SLOT[side], z],
            recv_sem=recv_sem.at[1, SLOT[side], z], device_id=(v + dv, p + dp),
            device_id_type=MESH_ID).wait_recv()

    def send_estimate(z):
        for h in range(2):
            es[0, z, pl.ds(4 * h, 4), :] = est[depth + z, h, pl.ds(8, 4), :]
            es[1, z, pl.ds(4 * h, 4), :] = est[depth + z, h, pl.ds(rows + 4, 4), :]
        each(SIDES, lambda side: est_copy(side, z).start())

    def send_correction(z):
        for dp in (-1, 0, 1):
            for h in range(2):
                plane = depth * (1 + dp) + z
                cs[0, dp + 1, z, pl.ds(4 * h, 4), :] = acc[plane, h, pl.ds(4, 4), :]
                cs[1, dp + 1, z, pl.ds(4 * h, 4), :] = acc[plane, h, pl.ds(rows + 8, 4), :]
        each(SIDES, lambda side: acc_copy(side, z).start())

    def every_plane(action, planes):
        def at_plane(z, carry):
            each(SIDES, lambda side: action(side, z))
            return carry

        lax.fori_loop(0, planes, at_plane, 0, unroll=True)

    def start_estimate(z, plane):
        out[z] = plane
        for h in range(2):
            half_plane = plane[:, h * 128:(h + 1) * 128]
            est[depth + z, h, pl.ds(8, rows), :] = 0.1 + (
                jnp.maximum(half_plane, 0.0) + jnp.log1p(jnp.exp(-jnp.abs(half_plane))))
        send_estimate(z)

    for zz in range(2):
        start_estimate(2 * kept + zz, r1[kept, zz])
    for zz in range(2):
        long(zz).wait_recv()
        start_estimate(2 * away + zz, r2[zz])
    own_share.wait()
    for share in shares:
        share.wait_recv()

    def early_step(w, carry):
        for z in range(depth):
            total = None
            for t in range(9):
                if z + t not in LATE:
                    term = taps[0, w, t] * est[z + t]
                    total = term if total is None else total + term
            zed[w, z] = total
        return carry

    def view_step(w, carry):
        for z in range(depth):
            total = zed[w, z]
            for plane in LATE:
                if 0 <= plane - z <= 8:
                    total = total + taps[0, w, plane - z] * est[plane]
            zed[w, z] = total
        sides = []
        for h in range(2):
            planes = []
            for z in range(depth):
                total = taps[1, w, 0] * zed[w, z, h, pl.ds(4, rows), :]
                for t in range(1, 9):
                    total = total + taps[1, w, t] * zed[w, z, h, pl.ds(4 + t, rows), :]
                planes.append(total)
            sides.append(jnp.concatenate(planes, axis=0))
        blurred = dot3(jnp.concatenate(sides, axis=1), th[w], tl[w])
        ratio = stacked[w].reshape(depth * rows, width) / blurred
        turned = dot3(ratio, ah[w], al[w])
        for z in range(depth):
            for h in range(2):
                mid[w, z, h, pl.ds(16, rows), :] = turned[z * rows:(z + 1) * rows, h * 128:(h + 1) * 128]
        for z in range(depth):
            for h in range(2):
                total = taps[1, w, 8] * mid[w, z, h, pl.ds(4, frame), :]
                for t in range(1, 9):
                    total = total + taps[1, w, 8 - t] * mid[w, z, h, pl.ds(4 + t, frame), :]
                spread[w, z, h] = total
        return carry

    def gather_planes(planes):
        for zo in planes:
            total = None
            for v in range(views):
                for zs in range(depth):
                    if 0 <= zo - zs <= 8:
                        term = taps[0, v, zo - zs] * spread[v, zs]
                        total = term if total is None else total + term
            acc[zo] = total

    def iteration(step, carry):
        every_plane(est_wait, depth - 1)
        lax.fori_loop(0, views, early_step, 0)
        each(SIDES, lambda side: est_wait(side, depth - 1))
        lax.fori_loop(0, views, view_step, 0, unroll=UNROLL)
        for z in range(depth):
            gather_planes([z, 2 * depth + z, depth + z])
            send_correction(z)

        def finish_plane(z, carry):
            each(SIDES, lambda side: acc_wait(side, z))
            each(SIDES, lambda side: est_copy(side, z).wait_send())
            for end in (-1, 1):
                strip[...] = rs[SLOT[(end, 0)], z] + (rs[SLOT[(end, -1)], z] + rs[SLOT[(end, 1)], z])
                at = pl.ds(8 if end < 0 else rows + 4, 4)
                for h in range(2):
                    acc[depth + z, h, at, :] = acc[depth + z, h, at, :] + strip[pl.ds(4 * h, 4), :]
            for h in range(2):
                total = acc[depth + z, h, pl.ds(8, rows), :] + (rz[0, z, h] + rz[1, z, h])
                est[depth + z, h, pl.ds(8, rows), :] = (
                    est[depth + z, h, pl.ds(8, rows), :] * (total * (1.0 / views)))

            @pl.when(step < ITERS - 1)
            def _():
                send_estimate(z)
            return carry

        lax.fori_loop(0, depth, finish_plane, 0, unroll=True)
        every_plane(lambda side, z: acc_copy(side, z).wait_send(), depth)
        return carry

    lax.fori_loop(0, ITERS, iteration, 0)
    for h in range(2):
        out2[:, :, h * 128:(h + 1) * 128] = est[pl.ds(depth, depth), h, pl.ds(8, rows), :]

    w_rest.wait_send()
    sent = msg.at[pl.ds(0, 32 * (pencils - 1))]
    remote(sent, sent, 0, (v, mirror)).wait_send()
    pair_sum.wait_send()
    sent_back = gm.at[kept, pl.ds(0, 8 * (pencils - 1))]
    remote(sent_back, sent_back, 4, (v, mirror)).wait_send()
    remote(gm.at[away], gm.at[away], 7, (far, p)).wait_send()
    for zz in range(2):
        near(zz).wait_send()
        long(zz).wait_send()

    @pl.when(jnp.logical_not(own_mirror))
    def _():
        w_first.wait_send()
    for share in shares:
        share.wait_send()


def whole(recorded, weight, taps):
    views, pencils = lax.axis_size("view"), lax.axis_size("pencil")
    n, nx = 4 * pencils, recorded.shape[-1]
    q, depth = n // 4, 4
    frame = q + 16
    vmem, left = pl.BlockSpec(memory_space=pltpu.VMEM), pl.BlockSpec(memory_space=pltpu.HBM)
    tables = [jnp.asarray(t) for t in transform_tables(n, nx)]
    block = pltpu.VMEM((depth, q, nx), F32)
    return pl.pallas_call(
        functools.partial(kernel, views, pencils),
        name="join_and_deconvolve",
        out_shape=(block, block),
        in_specs=[pl.BlockSpec(memory_space=pltpu.SMEM)] + [left] * (2 + len(tables)),
        out_specs=(vmem, vmem),
        scratch_shapes=[
            pltpu.VMEM((4, n, nx), F32),
            pltpu.VMEM((2, n, 4, 128), F32),
            *[pltpu.VMEM(t.shape, t.dtype) for t in tables],
            pltpu.VMEM((4, n, nx), BF16),
            pltpu.VMEM((4, n, nx), BF16),
            pltpu.VMEM((8 * n, 128), F32),
            pltpu.VMEM((pencils, 32, 128), F32),
            pltpu.VMEM((4, n, 128), F32),
            pltpu.VMEM((4, n, 128), F32),
            pltpu.VMEM((4, n, 128), F32),
            pltpu.VMEM((n, 128), F32),
            pltpu.VMEM((2 * n, 2 * n), BF16),
            pltpu.VMEM((2 * n, 2 * n), BF16),
            pltpu.VMEM((4, 2 * n, 128), F32),
            pltpu.VMEM((2, 2 * n, 128), F32),
            pltpu.VMEM((2 * n, 256), BF16),
            pltpu.VMEM((2 * n, 256), BF16),
            pltpu.VMEM((2, 2 * n, 128), F32),
            pltpu.VMEM((2, 8 * pencils, 128), F32),
            pltpu.VMEM((2, 8 * pencils, 128), F32),
            pltpu.VMEM((2, 2, 2, q, nx), F32),
            pltpu.VMEM((2, 2, q, nx), F32),
            pltpu.VMEM((2, q, nx), F32),
            pltpu.VMEM((views, depth, q, nx), F32),
            pltpu.VMEM((3 * depth, 2, frame, 128), F32),
            pltpu.VMEM((views, depth, 2, frame, 128), F32),
            pltpu.VMEM((views, depth, 2, frame + 16, 128), F32),
            pltpu.VMEM((views, depth, 2, frame, 128), F32),
            pltpu.VMEM((3 * depth, 2, frame, 128), F32),
            pltpu.VMEM((2, depth, 2, q, 128), F32),
            pltpu.VMEM((8, depth, 8, 128), F32),
            pltpu.VMEM((2, depth, 8, 128), F32),
            pltpu.VMEM((8, depth, 8, 128), F32),
            pltpu.VMEM((2, 3, depth, 8, 128), F32),
            pltpu.VMEM((8, 128), F32),
            *[pltpu.VMEM((views, nx, nx), BF16)] * 4,
            pltpu.SemaphoreType.DMA((10,)),
            pltpu.SemaphoreType.DMA((10,)),
            pltpu.SemaphoreType.DMA((4,)),
            pltpu.SemaphoreType.DMA((13,)),
            pltpu.SemaphoreType.DMA((2, 3)),
            pltpu.SemaphoreType.DMA((2, 8, 4)),
            pltpu.SemaphoreType.DMA((2, 8, 4)),
        ],
        compiler_params=pltpu.CompilerParams(collective_id=1, has_side_effects=True,
                                             vmem_limit_bytes=62 * 1024 * 1024),
    )(taps, recorded, weight, *tables)


def store(first, second, first_out, second_out, sem):
    copies = [pltpu.make_async_copy(src, dst, sem.at[k])
              for k, (src, dst) in enumerate(((first, first_out), (second, second_out)))]
    for copy in copies:
        copy.start()
    for copy in copies:
        copy.wait()


def stored(first, second):
    shape = jax.ShapeDtypeStruct(first.shape, F32)
    return pl.pallas_call(
        store,
        name="store",
        out_shape=(shape, shape),
        in_specs=[pl.BlockSpec(memory_space=pl.ANY)] * 2,
        out_specs=(pl.BlockSpec(memory_space=pltpu.HBM),) * 2,
        scratch_shapes=[pltpu.SemaphoreType.DMA((2,))],
        compiler_params=pltpu.CompilerParams(vmem_limit_bytes=2 * 1024 * 1024),
    )(first, second)


def body(recorded, spectral_weight, psf_taps):
    taps = jnp.transpose(psf_taps, (1, 0, 2))
    return stored(*whole(recorded[0], spectral_weight[0], taps))


def solution(mesh):
    return jax.shard_map(
        body,
        mesh=mesh,
        in_specs=(P("view", "pencil", None, None), P("view", None, "pencil", None), P()),
        out_specs=(P("pencil", "view", None), P("pencil", "view", None)),
        check_vma=False,
    )
```
